32 devices in a mesh: gz: 4 (over y, x), gx: 8 (over z, core).
Axes of the slice: x: 2, y: 2, z: 4, core: 2. Of those that a mesh axis runs over, the one named last changes fastest.
Arguments:
- substrate: float32 [64, 256, 1024], P('gz', 'gx'), may hold values from 0 to 1
- catalyst: float32 [64, 256, 1024], P('gz', 'gx'), may hold values from 0 to 1
- extinction: float32 [2], replicated, may hold values from 0.25 to 1
- emission: float32 [3, 2], replicated, may hold values from 0.5 to 2
Outputs:
- substrate_next: float32 [64, 256, 1024], P('gz', 'gx')
- catalyst_next: float32 [64, 256, 1024], P('gz', 'gx')
- image: float32 [4, 256, 1024], P(None, 'gx', 'gz')
The draws below stay inside these ranges and needn't reach their ends.
All inputs are finite; a program needn't handle non-finite values.
Results may differ from the reference program's by a relative error of at most 0.00004.
Values sent between devices are 32-bit elements; how exact they have to be, the bound alone decides.
No kernel may reach another device: no remote copies, remote signals or barrier semaphores. Data moves between devices by JAX's collectives and lax.ppermute only.
A program may use at most 64 MiB of HBM per device.

```python
import math
import jax
import jax.numpy as jnp

NY = 1024
STEPS = 2
NZ = 64
NX = 256


def shard_levels(rng, dims, shards, low, top_value):
    level, own = 1.0, jax.random.fold_in(rng, 6)
    for axis_at, shards_of in shards:
        steps = jnp.exp(jax.random.uniform(jax.random.fold_in(own, axis_at), (shards_of,), jnp.float32, low / len(shards), top_value / len(shards)))
        level = level * jnp.repeat(steps, dims[axis_at] // shards_of).reshape([-1 if axis == axis_at else 1 for axis in range(len(dims))])
    return level


def setup_inputs(seed: int = 0) -> dict:
    arg_keys = jax.random.split(jax.random.key(seed), 5)
    return {
        "substrate": jnp.clip(1.0 * jax.random.uniform(arg_keys[0], (NZ, NX, NY), jnp.float32) ** shard_levels(arg_keys[0], (NZ, NX, NY), ((0, 4), (1, 8)), -0.2, 0.2), 0.0, 1.0),
        "catalyst": jnp.clip(1.0 * jax.random.uniform(arg_keys[1], (NZ, NX, NY), jnp.float32) ** shard_levels(arg_keys[1], (NZ, NX, NY), ((0, 4), (1, 8)), -0.2, 0.2), 0.0, 1.0),
        "extinction": jnp.clip(jnp.exp(jax.random.uniform(arg_keys[2], (2,), jnp.float32, math.log(0.25), math.log(1.0))), 0.25, 1.0),
        "emission": jnp.clip(jnp.exp(jax.random.uniform(arg_keys[3], (3, 2), jnp.float32, math.log(0.5), math.log(2.0))), 0.5, 2.0),
    }


diffusion_rates = (0.16, 0.08)
feed_rate = 0.037
kill_rate = 0.06
optical_scale = 4.0


def laplace_of(fields):
    padded = jnp.pad(fields, ((0, 0), (1, 1), (1, 1), (0, 0)), mode="wrap")
    centre = padded[:, 1:-1, 1:-1]
    result = padded[:, 2:, 1:-1] + padded[:, :-2, 1:-1]
    result = result + padded[:, 1:-1, 2:] + padded[:, 1:-1, :-2]
    result = result + jnp.roll(centre, 1, axis=3) + jnp.roll(centre, -1, axis=3)
    return result - 6.0 * centre


def react(fields):
    laplace = laplace_of(fields)
    sub_old = fields[0]
    cat_old = fields[1]
    growth = sub_old * cat_old * cat_old
    sub_new = sub_old + diffusion_rates[0] * laplace[0] - growth + feed_rate * (1.0 - sub_old)
    cat_new = cat_old + diffusion_rates[1] * laplace[1] + growth - (feed_rate + kill_rate) * cat_old
    return jnp.stack([sub_new, cat_new])


def reference(substrate, catalyst, extinction, emission):
    fields = jnp.stack([substrate, catalyst])
    for step in range(STEPS):
        fields = react(fields)
    sub_final = fields[0]
    cat_final = fields[1]
    optical = (extinction[0] * sub_final + extinction[1] * cat_final) * (optical_scale / NZ)
    opacity = 1.0 - jnp.exp(-optical)
    before = jnp.cumsum(optical, axis=0) - optical
    weight = jnp.exp(-before) * opacity
    seen_sub = jnp.sum(weight * sub_final, axis=0)
    seen_cat = jnp.sum(weight * cat_final, axis=0)
    colour = emission[:, 0, None, None] * seen_sub[None] + emission[:, 1, None, None] * seen_cat[None]
    alpha_total = 1.0 - jnp.exp(-jnp.sum(optical, axis=0))
    image = jnp.concatenate([colour, alpha_total[None]], axis=0)
    return sub_final, cat_final, image
```

```python
import functools

import jax
import jax.numpy as jnp
from jax import lax
from jax.experimental import pallas as pl
from jax.experimental.pallas import tpu as pltpu
from jax.sharding import PartitionSpec as P


RATES = (0.16, 0.08)
FEED = 0.037
KILL = 0.06
OPTICAL = 4.0
ROWS = 8

ANY = pl.BlockSpec(memory_space=pl.ANY)
VMEM = pl.BlockSpec(memory_space=pltpu.VMEM)
SMEM = pl.BlockSpec(memory_space=pltpu.SMEM)


def f32(*shape):
    return jax.ShapeDtypeStruct(shape, jnp.float32)


def lanes(x):
    return pltpu.roll(x, 1, axis=x.ndim - 1) + pltpu.roll(x, x.shape[-1] - 1, axis=x.ndim - 1)


def react(sub, cat, around_sub, around_cat):
    growth = sub * cat * cat
    sub_new = (1.0 - 6.0 * RATES[0] - FEED) * sub + RATES[0] * around_sub - growth + FEED
    cat_new = (1.0 - 6.0 * RATES[1] - FEED - KILL) * cat + RATES[1] * around_cat + growth
    return sub_new, cat_new


def plane_step(load, low_rows, high_rows, across, store):
    count = 4
    first = low_rows[0].shape[-1]
    index = lax.broadcasted_iota(jnp.int32, (ROWS, first), 0)
    top, bottom = index == 0, index == ROWS - 1
    for tile in range(load.tiles):
        sums, olds = [], []
        for s in range(2):
            old = load(s, tile)
            above = low_rows[s] if tile == 0 else load(s, tile - 1)[ROWS - 1 :]
            below = high_rows[s] if tile == load.tiles - 1 else load(s, tile + 1)[:1]
            up = jnp.where(top, jnp.broadcast_to(above, old.shape), pltpu.roll(old, 1, axis=0))
            down = jnp.where(bottom, jnp.broadcast_to(below, old.shape), pltpu.roll(old, ROWS - 1, axis=0))
            around = lanes(old) + (up + down)
            beside = across(s, tile)
            sums.append(around if beside is None else around + beside)
            olds.append(old)
        store(tile, *react(olds[0], olds[1], sums[0], sums[1]))


class Tiles:
    def __init__(self, sub, cat):
        self.refs = (sub, cat)
        self.tiles = sub.shape[0] // ROWS

    def __call__(self, s, tile):
        return self.refs[s][pl.ds(tile * ROWS, ROWS), :]


def edge_kernel(front, back, second, penult, from_low, from_high, q_low, q_high):
    depth = from_low.shape[2]
    for plane, outer, inner, out in ((0, front, second, q_low), (depth - 1, back, penult, q_high)):
        load = Tiles(outer.at[0], outer.at[1])
        inside = Tiles(inner.at[0], inner.at[1])

        def store(tile, sub, cat, out=out):
            out[0, pl.ds(tile * ROWS, ROWS), :] = sub
            out[1, pl.ds(tile * ROWS, ROWS), :] = cat

        plane_step(
            load,
            [from_low[s, 1, plane : plane + 1] for s in range(2)],
            [from_high[s, 0, plane : plane + 1] for s in range(2)],
            inside,
            store,
        )


def composite(sub, cat, scale_sub, scale_cat, clear):
    keep = jnp.exp(-(scale_sub * sub + scale_cat * cat))
    weight = clear * (1.0 - keep)
    return weight * sub, weight * cat, clear * keep


def inner_kernel(
    scale, sub_hbm, cat_hbm, from_low, from_high, own_low, own_high,
    sub_out, cat_out, seen, near, far, rows_low, rows_high,
    old, mid, new, sem_in, sem_out,
):
    depth, rows, columns = sub_hbm.shape
    chunk = 2
    chunks = depth // chunk
    inputs = (sub_hbm, cat_hbm)
    outputs = (sub_out, cat_out)

    def fetch(s, c):
        return pltpu.make_async_copy(
            inputs[s].at[pl.ds(c * chunk, chunk)], old.at[s, pl.ds(c * chunk, chunk)], sem_in.at[s, c]
        )

    def put(s, c):
        return pltpu.make_async_copy(
            new.at[s, pl.ds(c * chunk, chunk)], outputs[s].at[pl.ds(c * chunk, chunk)], sem_out.at[s, c]
        )

    for c in range(chunks):
        for s in range(2):
            fetch(s, c).start()

    which = lax.broadcasted_iota(jnp.int32, (depth, columns), 0)
    for got, at, own, at_own, out in (
        (from_low, 1, own_low, 0, rows_low),
        (from_high, 0, own_high, 1, rows_high),
    ):
        sums, olds = [], []
        for s in range(2):
            here = got[s, at]
            ahead = jnp.where(which == 0, 0.0, pltpu.roll(here, 1, axis=0))
            behind = jnp.where(which == depth - 1, 0.0, pltpu.roll(here, depth - 1, axis=0))
            sums.append(lanes(here) + (got[s, 1 - at] + own[s, at_own]) + (ahead + behind))
            olds.append(here)
        sub, cat = react(olds[0], olds[1], sums[0], sums[1])
        out[0] = sub
        out[1] = cat

    def first(k):
        def store(tile, sub, cat):
            mid[0, k, pl.ds(tile * ROWS, ROWS), :] = sub
            mid[1, k, pl.ds(tile * ROWS, ROWS), :] = cat

        def across(s, tile):
            span = pl.ds(tile * ROWS, ROWS)
            return old[s, k - 1, span, :] + old[s, k + 1, span, :]

        plane_step(
            Tiles(old.at[0, k], old.at[1, k]),
            [from_low[s, 1, pl.ds(k, 1)] for s in range(2)],
            [from_high[s, 0, pl.ds(k, 1)] for s in range(2)],
            across,
            store,
        )

    scale_sub, scale_cat = scale[0], scale[1]
    seen[0] = jnp.zeros((rows, columns), jnp.float32)
    seen[1] = jnp.zeros((rows, columns), jnp.float32)
    seen[2] = jnp.ones((rows, columns), jnp.float32)

    def second(k):
        def store(tile, sub, cat):
            span = pl.ds(tile * ROWS, ROWS)
            new[0, k, span, :] = sub
            new[1, k, span, :] = cat
            one, two, clear = composite(sub, cat, scale_sub, scale_cat, seen[2, span, :])
            seen[0, span, :] += one
            seen[1, span, :] += two
            seen[2, span, :] = clear

        def across(s, tile):
            span = pl.ds(tile * ROWS, ROWS)
            return mid[s, k - 1, span, :] + mid[s, k + 1, span, :]

        plane_step(
            Tiles(mid.at[0, k], mid.at[1, k]),
            [rows_low[s, pl.ds(k, 1)] for s in range(2)],
            [rows_high[s, pl.ds(k, 1)] for s in range(2)],
            across,
            store,
        )

    for s in range(2):
        fetch(s, 0).wait()

    @pl.loop(1, chunks)
    def _(c):
        for s in range(2):
            fetch(s, c).wait()
        for j in range(chunk):
            first(c * chunk + j - 1)

    @pl.loop(1, chunks - 1)
    def _(c):
        for j in range(chunk):
            second(c * chunk + j)
        for s in range(2):
            put(s, c).start()

    for s in range(2):
        for j in range(2):
            near[s, j] = mid[s, 1 + j]
            far[s, j] = mid[s, depth - 3 + j]

    @pl.loop(1, chunks - 1)
    def _(c):
        for s in range(2):
            put(s, c).wait()


def rim_kernel(
    scale, q_low, q_high, p_low, p_high, front, back, near, far, rows_low, rows_high, corner_low, corner_high, inner,
    ring, known, seen, mid,
):
    depth = rows_low.shape[1]
    rows, columns = q_low.shape[1:]
    scale_sub, scale_cat = scale[0], scale[1]
    for side, q, p, own, inside in ((0, q_low, p_low, front, near), (1, q_high, p_high, back, far)):
        outer = 0 if side == 0 else depth - 1
        inner_plane = 1 if side == 0 else depth - 2
        one, two = (0, 1) if side == 0 else (1, 0)
        for s in range(2):
            mid[side, s] = q[s] + RATES[s] * p[s]

        def store_known(tile, sub, cat, side=side, own=own):
            span = pl.ds(tile * ROWS, ROWS)
            known[side, 0, span, :] = sub + (RATES[0] * RATES[0]) * own[0, span, :]
            known[side, 1, span, :] = cat + (RATES[1] * RATES[1]) * own[1, span, :]

        def across_known(s, tile, inside=inside, one=one):
            return inside[s, one, pl.ds(tile * ROWS, ROWS), :]

        plane_step(
            Tiles(mid.at[side, 0], mid.at[side, 1]),
            [rows_low[s, outer : outer + 1] + RATES[s] * corner_low[side, s : s + 1] for s in range(2)],
            [rows_high[s, outer : outer + 1] + RATES[s] * corner_high[side, s : s + 1] for s in range(2)],
            across_known,
            store_known,
        )

        def store_ring(tile, sub, cat, side=side):
            span = pl.ds(tile * ROWS, ROWS)
            ring[0, side, span, :] = sub
            ring[1, side, span, :] = cat

        def across_ring(s, tile, side=side, inside=inside, two=two):
            span = pl.ds(tile * ROWS, ROWS)
            return inside[s, two, span, :] + mid[side, s, span, :]

        plane_step(
            Tiles(inside.at[0, one], inside.at[1, one]),
            [rows_low[s, inner_plane : inner_plane + 1] for s in range(2)],
            [rows_high[s, inner_plane : inner_plane + 1] for s in range(2)],
            across_ring,
            store_ring,
        )

    for tile in range(rows // ROWS):
        span = pl.ds(tile * ROWS, ROWS)
        one, two, clear = composite(ring[0, 0, span, :], ring[1, 0, span, :], scale_sub, scale_cat, 1.0)
        sub = one + clear * inner[0, span, :]
        cat = two + clear * inner[1, span, :]
        clear = clear * inner[2, span, :]
        one, two, clear = composite(ring[0, 1, span, :], ring[1, 1, span, :], scale_sub, scale_cat, clear)
        seen[0, span, :] = sub + one
        seen[1, span, :] = cat + two
        seen[2, span, :] = clear


def last_kernel(scale, me, known, q_low, q_high, seen, *outs_and_scratch):
    *pieces, outer, whole = outs_and_scratch
    rows, columns = seen.shape[1:]
    count = len(pieces)
    wide = columns // count
    scale_sub, scale_cat = scale[0], scale[1]
    for tile in range(rows // ROWS):
        span = pl.ds(tile * ROWS, ROWS)
        low = [known[0, s, span, :] + RATES[s] * q_low[s, span, :] for s in range(2)]
        high = [known[1, s, span, :] + RATES[s] * q_high[s, span, :] for s in range(2)]
        for s in range(2):
            outer[s, 0, span, :] = low[s]
            outer[s, 1, span, :] = high[s]
        one, two, clear = composite(low[0], low[1], scale_sub, scale_cat, 1.0)
        sub = one + clear * seen[0, span, :]
        cat = two + clear * seen[1, span, :]
        clear = clear * seen[2, span, :]
        one, two, clear = composite(high[0], high[1], scale_sub, scale_cat, clear)
        whole[0, span, :] = sub + one
        whole[1, span, :] = cat + two
        whole[2, span, :] = clear
    for shift, piece in enumerate(pieces):
        target = lax.rem(me[0] + shift, count)
        if wide % 128 == 0:
            piece[...] = whole[:, :, pl.ds(pl.multiple_of(target * wide, 128), wide)]
        else:
            for other in range(count):

                @pl.when(target == other)
                def _(piece=piece, other=other):
                    piece[...] = whole[:, :, other * wide : (other + 1) * wide]


def shade_kernel(emission, me, *pieces_and_rest):
    *pieces, image, slabs = pieces_and_rest
    count = len(pieces)
    for shift, piece in enumerate(pieces):
        slabs[lax.rem(me[0] + count - shift, count)] = piece[...]
    sub, cat, clear = slabs[0, 0], slabs[0, 1], slabs[0, 2]
    for slab in range(1, count):
        sub = sub + clear * slabs[slab, 0]
        cat = cat + clear * slabs[slab, 1]
        clear = clear * slabs[slab, 2]
    for channel in range(3):
        image[channel] = emission[channel, 0] * sub + emission[channel, 1] * cat
    image[3] = 1.0 - clear


def place_kernel(ring, outer, sub_in, cat_in, sub_out, cat_out, sems):
    del sub_in, cat_in
    depth = sub_out.shape[0]
    outputs = (sub_out, cat_out)
    copies = []
    for s in range(2):
        for side in range(2):
            for at, source in ((side * (depth - 1), outer), (1 + side * (depth - 3), ring)):
                copies.append(pltpu.make_async_copy(source.at[s, side], outputs[s].at[at], sems.at[len(copies)]))
    for copy in copies:
        copy.start()
    for copy in copies:
        copy.wait()


def call(kernel, flops, **kwargs):
    return pl.pallas_call(
        kernel, cost_estimate=pl.CostEstimate(flops=flops, bytes_accessed=1 << 16, transcendentals=0), **kwargs
    )


def body(substrate, catalyst, extinction, emission):
    depth, rows, columns = substrate.shape
    count = lax.axis_size("gz")
    across = lax.axis_size("gx")
    wide = columns // count
    me = lax.axis_index("gz").astype(jnp.int32)[None]
    scale = extinction * (OPTICAL / (depth * count))

    def ring(size, shift):
        return [(i, (i + shift) % size) for i in range(size)]

    def up(x, axis):
        return lax.ppermute(x, axis, ring(lax.axis_size(axis), 1))

    def down(x, axis):
        return lax.ppermute(x, axis, ring(lax.axis_size(axis), -1))

    both = (substrate, catalyst)
    front = jnp.stack([f[0] for f in both])
    back = jnp.stack([f[depth - 1] for f in both])
    second = jnp.stack([f[1] for f in both])
    penult = jnp.stack([f[depth - 2] for f in both])
    own_low = jnp.stack([jnp.stack([f[:, 0], f[:, 1]]) for f in both])
    own_high = jnp.stack([jnp.stack([f[:, rows - 2], f[:, rows - 1]]) for f in both])

    p_low = up(back, "gz")
    p_high = down(front, "gz")
    from_low = up(own_high, "gx")
    from_high = down(own_low, "gx")

    q_low, q_high = call(
        edge_kernel,
        1 << 22,
        name="edge",
        out_shape=(f32(2, rows, columns), f32(2, rows, columns)),
        in_specs=[VMEM] * 6,
        out_specs=(VMEM, VMEM),
    )(front, back, second, penult, from_low, from_high)
    q_from_low = up(q_high, "gz")
    q_from_high = down(q_low, "gz")

    sub_part, cat_part, inner, near, far, rows_low, rows_high = call(
        inner_kernel,
        1 << 26,
        name="inner",
        out_shape=(
            f32(depth, rows, columns),
            f32(depth, rows, columns),
            f32(3, rows, columns),
            f32(2, 2, rows, columns),
            f32(2, 2, rows, columns),
            f32(2, depth, columns),
            f32(2, depth, columns),
        ),
        in_specs=[SMEM, ANY, ANY, VMEM, VMEM, VMEM, VMEM],
        out_specs=(ANY, ANY, VMEM, VMEM, VMEM, VMEM, VMEM),
        scratch_shapes=[
            pltpu.VMEM((2, depth, rows, columns), jnp.float32),
            pltpu.VMEM((2, depth, rows, columns), jnp.float32),
            pltpu.VMEM((2, depth, rows, columns), jnp.float32),
            pltpu.SemaphoreType.DMA((2, depth // 2)),
            pltpu.SemaphoreType.DMA((2, depth // 2)),
        ],
    )(scale, substrate, catalyst, from_low, from_high, own_low, own_high)

    corner_low = up(jnp.stack([p_low[:, rows - 1], p_high[:, rows - 1]]), "gx")
    corner_high = down(jnp.stack([p_low[:, 0], p_high[:, 0]]), "gx")

    ring_planes, known, seen = call(
        rim_kernel,
        1 << 23,
        name="rim",
        out_shape=(f32(2, 2, rows, columns), f32(2, 2, rows, columns), f32(3, rows, columns)),
        in_specs=[SMEM] + [VMEM] * 13,
        out_specs=(VMEM, VMEM, VMEM),
        scratch_shapes=[pltpu.VMEM((2, 2, rows, columns), jnp.float32)],
    )(
        scale, q_low, q_high, p_low, p_high, front, back, near, far, rows_low, rows_high, corner_low, corner_high, inner
    )

    *pieces, outer = call(
        last_kernel,
        1 << 22,
        name="last",
        out_shape=(*[f32(3, rows, wide)] * count, f32(2, 2, rows, columns)),
        in_specs=[SMEM, SMEM] + [VMEM] * 4,
        out_specs=tuple([VMEM] * (count + 1)),
        scratch_shapes=[pltpu.VMEM((3, rows, columns), jnp.float32)],
    )(scale, me, known, q_from_low, q_from_high, seen)

    received = [pieces[0]]
    for shift in range(1, count):
        received.append(lax.ppermute(pieces[shift], "gz", ring(count, shift)))

    sub_final, cat_final = call(
        place_kernel,
        1 << 22,
        name="place",
        out_shape=(f32(depth, rows, columns), f32(depth, rows, columns)),
        in_specs=[VMEM, VMEM, ANY, ANY],
        out_specs=(ANY, ANY),
        input_output_aliases={2: 0, 3: 1},
        scratch_shapes=[pltpu.SemaphoreType.DMA((8,))],
    )(ring_planes, outer, sub_part, cat_part)

    image = call(
        shade_kernel,
        1 << 20,
        name="shade",
        out_shape=f32(4, rows, wide),
        in_specs=[SMEM, SMEM] + [VMEM] * count,
        out_specs=VMEM,
        scratch_shapes=[pltpu.VMEM((count, 3, rows, wide), jnp.float32)],
    )(emission, me, *received)
    return sub_final, cat_final, image


def solution(mesh):
    placed = (P("gz", "gx", None), P("gz", "gx", None), P(), P())
    return jax.shard_map(
        body,
        mesh=mesh,
        in_specs=placed,
        out_specs=(P("gz", "gx", None), P("gz", "gx", None), P(None, "gx", "gz")),
        check_vma=False,
    )
```

```python
import functools

import jax
import jax.numpy as jnp
from jax import lax
from jax.experimental import pallas as pl
from jax.experimental.pallas import tpu as pltpu
from jax.sharding import PartitionSpec as P


RATES = (0.16, 0.08)
FEED = 0.037
KILL = 0.06
OPTICAL = 4.0
ROWS = 8

HBM = pl.BlockSpec(memory_space=pltpu.HBM)
VMEM = pl.BlockSpec(memory_space=pltpu.VMEM)
SMEM = pl.BlockSpec(memory_space=pltpu.SMEM)


def f32(*shape):
    return jax.ShapeDtypeStruct(shape, jnp.float32)


def hbm(x):
    return pltpu.with_memory_space_constraint(x, pltpu.HBM)


def lanes(x):
    return pltpu.roll(x, 1, axis=x.ndim - 1) + pltpu.roll(x, x.shape[-1] - 1, axis=x.ndim - 1)


def react(sub, cat, around_sub, around_cat):
    growth = sub * cat * cat
    sub_new = (1.0 - 6.0 * RATES[0] - FEED) * sub + RATES[0] * around_sub - growth + FEED
    cat_new = (1.0 - 6.0 * RATES[1] - FEED - KILL) * cat + RATES[1] * around_cat + growth
    return sub_new, cat_new


def plane_step(load, low_rows, high_rows, across, store):
    first = low_rows[0].shape[-1]
    index = lax.broadcasted_iota(jnp.int32, (ROWS, first), 0)
    top, bottom = index == 0, index == ROWS - 1
    for tile in range(load.tiles):
        sums, olds = [], []
        for s in range(2):
            old = load(s, tile)
            above = low_rows[s] if tile == 0 else load(s, tile - 1)[ROWS - 1 :]
            below = high_rows[s] if tile == load.tiles - 1 else load(s, tile + 1)[:1]
            up = jnp.where(top, jnp.broadcast_to(above, old.shape), pltpu.roll(old, 1, axis=0))
            down = jnp.where(bottom, jnp.broadcast_to(below, old.shape), pltpu.roll(old, ROWS - 1, axis=0))
            around = lanes(old) + (up + down)
            beside = across(s, tile)
            sums.append(around if beside is None else around + beside)
            olds.append(old)
        store(tile, *react(olds[0], olds[1], sums[0], sums[1]))


class Tiles:
    def __init__(self, sub, cat):
        self.refs = (sub, cat)
        self.tiles = sub.shape[0] // ROWS

    def __call__(self, s, tile):
        return self.refs[s][pl.ds(tile * ROWS, ROWS), :]


def planes_kernel(sub, cat, front, back, sems):
    depth = sub.shape[0]
    copies = []
    for s, field in enumerate((sub, cat)):
        for plane, out in ((0, front), (depth - 1, back)):
            copies.append(pltpu.make_async_copy(field.at[plane], out.at[s], sems.at[len(copies)]))
    for copy in copies:
        copy.start()
    for copy in copies:
        copy.wait()


def rows_kernel(sub, cat, low, high, second, penult, heads, tails, sems):
    depth, rows, _ = sub.shape
    copies = []
    for s, field in enumerate((sub, cat)):
        for source, out in (
            (field.at[:, :ROWS], heads.at[s]),
            (field.at[:, rows - ROWS :], tails.at[s]),
            (field.at[1], second.at[s]),
            (field.at[depth - 2], penult.at[s]),
        ):
            copies.append(pltpu.make_async_copy(source, out, sems.at[len(copies)]))
    for copy in copies:
        copy.start()
    for copy in copies:
        copy.wait()
    for s in range(2):
        for row in range(2):
            for plane in range(depth):
                low[s, row, plane : plane + 1] = heads[s, plane, row : row + 1]
                high[s, row, plane : plane + 1] = tails[s, plane, ROWS - 2 + row : ROWS - 1 + row]


def edge_kernel(front, back, second, penult, from_low, from_high, q_low, q_high):
    depth = from_low.shape[2]
    for plane, outer, inner, out in ((0, front, second, q_low), (depth - 1, back, penult, q_high)):
        load = Tiles(outer.at[0], outer.at[1])
        inside = Tiles(inner.at[0], inner.at[1])

        def store(tile, sub, cat, out=out):
            out[0, pl.ds(tile * ROWS, ROWS), :] = sub
            out[1, pl.ds(tile * ROWS, ROWS), :] = cat

        plane_step(
            load,
            [from_low[s, 1, plane : plane + 1] for s in range(2)],
            [from_high[s, 0, plane : plane + 1] for s in range(2)],
            inside,
            store,
        )


def composite(sub, cat, scale_sub, scale_cat, clear):
    keep = jnp.exp(-(scale_sub * sub + scale_cat * cat))
    weight = clear * (1.0 - keep)
    return weight * sub, weight * cat, clear * keep


def inner_kernel(
    share, scale, emission, me, sub_hbm, cat_hbm, from_low, from_high, own_low, own_high,
    sub_out, cat_out, seen, near, far, rows_low, rows_high,
    old, mid, new, sem_in, sem_out,
):
    del emission, me
    depth, rows, columns = sub_hbm.shape
    chunk = 2
    chunks = depth // chunk
    inputs = (sub_hbm, cat_hbm)
    outputs = (sub_out, cat_out)

    def fetch(s, c):
        return pltpu.make_async_copy(
            inputs[s].at[pl.ds(c * chunk, chunk)], old.at[s, pl.ds(c * chunk, chunk)], sem_in.at[s, c]
        )

    def put(s, c):
        return pltpu.make_async_copy(
            new.at[s, pl.ds(c * chunk, chunk)], outputs[s].at[pl.ds(c * chunk, chunk)], sem_out.at[s, c]
        )

    for c in range(chunks):
        for s in range(2):
            fetch(s, c).start()

    which = lax.broadcasted_iota(jnp.int32, (depth, columns), 0)
    for got, at, own, at_own, out in (
        (from_low, 1, own_low, 0, rows_low),
        (from_high, 0, own_high, 1, rows_high),
    ):
        sums, olds = [], []
        for s in range(2):
            here = got[s, at]
            ahead = jnp.where(which == 0, 0.0, pltpu.roll(here, 1, axis=0))
            behind = jnp.where(which == depth - 1, 0.0, pltpu.roll(here, depth - 1, axis=0))
            sums.append(lanes(here) + (got[s, 1 - at] + own[s, at_own]) + (ahead + behind))
            olds.append(here)
        sub, cat = react(olds[0], olds[1], sums[0], sums[1])
        out[0] = sub
        out[1] = cat

    def first(k):
        def store(tile, sub, cat):
            mid[0, k, pl.ds(tile * ROWS, ROWS), :] = sub
            mid[1, k, pl.ds(tile * ROWS, ROWS), :] = cat

        def across(s, tile):
            span = pl.ds(tile * ROWS, ROWS)
            return old[s, k - 1, span, :] + old[s, k + 1, span, :]

        plane_step(
            Tiles(old.at[0, k], old.at[1, k]),
            [from_low[s, 1, pl.ds(k, 1)] for s in range(2)],
            [from_high[s, 0, pl.ds(k, 1)] for s in range(2)],
            across,
            store,
        )

    scale_sub, scale_cat = scale[0] * share, scale[1] * share
    seen[0] = jnp.zeros((rows, columns), jnp.float32)
    seen[1] = jnp.zeros((rows, columns), jnp.float32)
    seen[2] = jnp.ones((rows, columns), jnp.float32)

    def second(k):
        def store(tile, sub, cat):
            span = pl.ds(tile * ROWS, ROWS)
            new[0, k, span, :] = sub
            new[1, k, span, :] = cat
            one, two, clear = composite(sub, cat, scale_sub, scale_cat, seen[2, span, :])
            seen[0, span, :] += one
            seen[1, span, :] += two
            seen[2, span, :] = clear

        def across(s, tile):
            span = pl.ds(tile * ROWS, ROWS)
            return mid[s, k - 1, span, :] + mid[s, k + 1, span, :]

        plane_step(
            Tiles(mid.at[0, k], mid.at[1, k]),
            [rows_low[s, pl.ds(k, 1)] for s in range(2)],
            [rows_high[s, pl.ds(k, 1)] for s in range(2)],
            across,
            store,
        )

    for s in range(2):
        fetch(s, 0).wait()

    @pl.loop(1, chunks)
    def _(c):
        for s in range(2):
            fetch(s, c).wait()
        for j in range(chunk):
            first(c * chunk + j - 1)

    @pl.loop(1, chunks - 1)
    def _(c):
        for j in range(chunk):
            second(c * chunk + j)
        for s in range(2):
            put(s, c).start()

    for s in range(2):
        for j in range(2):
            near[s, j] = mid[s, 1 + j]
            far[s, j] = mid[s, depth - 3 + j]

    @pl.loop(1, chunks - 1)
    def _(c):
        for s in range(2):
            put(s, c).wait()


def corner_kernel(p_low, p_high, first, last):
    rows = p_low.shape[1]
    for side, p in enumerate((p_low, p_high)):
        for s in range(2):
            first[side, s : s + 1] = p[s, :1]
            last[side, s : s + 1] = p[s, rows - 1 :]


def rim_kernel(
    share, scale, q_low, q_high, p_low, p_high, front, back, near, far, rows_low, rows_high, corner_low, corner_high, inner,
    ring, known, seen, mid,
):
    depth = rows_low.shape[1]
    rows, _ = q_low.shape[1:]
    scale_sub, scale_cat = scale[0] * share, scale[1] * share
    for side, q, p, own, inside in ((0, q_low, p_low, front, near), (1, q_high, p_high, back, far)):
        outer = 0 if side == 0 else depth - 1
        inner_plane = 1 if side == 0 else depth - 2
        one, two = (0, 1) if side == 0 else (1, 0)
        for s in range(2):
            mid[side, s] = q[s] + RATES[s] * p[s]

        def store_known(tile, sub, cat, side=side, own=own):
            span = pl.ds(tile * ROWS, ROWS)
            known[side, 0, span, :] = sub + (RATES[0] * RATES[0]) * own[0, span, :]
            known[side, 1, span, :] = cat + (RATES[1] * RATES[1]) * own[1, span, :]

        def across_known(s, tile, inside=inside, one=one):
            return inside[s, one, pl.ds(tile * ROWS, ROWS), :]

        plane_step(
            Tiles(mid.at[side, 0], mid.at[side, 1]),
            [rows_low[s, outer : outer + 1] + RATES[s] * corner_low[side, s : s + 1] for s in range(2)],
            [rows_high[s, outer : outer + 1] + RATES[s] * corner_high[side, s : s + 1] for s in range(2)],
            across_known,
            store_known,
        )

        def store_ring(tile, sub, cat, side=side):
            span = pl.ds(tile * ROWS, ROWS)
            ring[0, side, span, :] = sub
            ring[1, side, span, :] = cat

        def across_ring(s, tile, side=side, inside=inside, two=two):
            span = pl.ds(tile * ROWS, ROWS)
            return inside[s, two, span, :] + mid[side, s, span, :]

        plane_step(
            Tiles(inside.at[0, one], inside.at[1, one]),
            [rows_low[s, inner_plane : inner_plane + 1] for s in range(2)],
            [rows_high[s, inner_plane : inner_plane + 1] for s in range(2)],
            across_ring,
            store_ring,
        )

    for tile in range(rows // ROWS):
        span = pl.ds(tile * ROWS, ROWS)
        one, two, clear = composite(ring[0, 0, span, :], ring[1, 0, span, :], scale_sub, scale_cat, 1.0)
        sub = one + clear * inner[0, span, :]
        cat = two + clear * inner[1, span, :]
        clear = clear * inner[2, span, :]
        one, two, clear = composite(ring[0, 1, span, :], ring[1, 1, span, :], scale_sub, scale_cat, clear)
        seen[0, span, :] = sub + one
        seen[1, span, :] = cat + two
        seen[2, span, :] = clear


def last_kernel(share, scale, me, known, q_low, q_high, seen, *outs_and_scratch):
    *pieces, outer, whole = outs_and_scratch
    rows, columns = seen.shape[1:]
    count = len(pieces)
    wide = columns // count
    scale_sub, scale_cat = scale[0] * share, scale[1] * share
    for tile in range(rows // ROWS):
        span = pl.ds(tile * ROWS, ROWS)
        low = [known[0, s, span, :] + RATES[s] * q_low[s, span, :] for s in range(2)]
        high = [known[1, s, span, :] + RATES[s] * q_high[s, span, :] for s in range(2)]
        for s in range(2):
            outer[s, 0, span, :] = low[s]
            outer[s, 1, span, :] = high[s]
        one, two, clear = composite(low[0], low[1], scale_sub, scale_cat, 1.0)
        sub = one + clear * seen[0, span, :]
        cat = two + clear * seen[1, span, :]
        clear = clear * seen[2, span, :]
        one, two, clear = composite(high[0], high[1], scale_sub, scale_cat, clear)
        whole[0, span, :] = sub + one
        whole[1, span, :] = cat + two
        whole[2, span, :] = clear
    for shift, piece in enumerate(pieces):
        target = lax.rem(me[0] + shift, count)
        if wide % 128 == 0:
            piece[...] = whole[:, :, pl.ds(pl.multiple_of(target * wide, 128), wide)]
        else:
            for other in range(count):

                @pl.when(target == other)
                def _(piece=piece, other=other):
                    piece[...] = whole[:, :, other * wide : (other + 1) * wide]


def shade_kernel(emission, me, *pieces_and_rest):
    *pieces, image, slabs = pieces_and_rest
    count = len(pieces)
    for shift, piece in enumerate(pieces):
        slabs[lax.rem(me[0] + count - shift, count)] = piece[...]
    sub, cat, clear = slabs[0, 0], slabs[0, 1], slabs[0, 2]
    for slab in range(1, count):
        sub = sub + clear * slabs[slab, 0]
        cat = cat + clear * slabs[slab, 1]
        clear = clear * slabs[slab, 2]
    for channel in range(3):
        image[channel] = emission[channel, 0] * sub + emission[channel, 1] * cat
    image[3] = 1.0 - clear


def place_kernel(ring, outer, sub_in, cat_in, sub_out, cat_out, sems):
    del sub_in, cat_in
    depth = sub_out.shape[0]
    outputs = (sub_out, cat_out)
    copies = []
    for s in range(2):
        for side in range(2):
            for at, source in ((side * (depth - 1), outer), (1 + side * (depth - 3), ring)):
                copies.append(pltpu.make_async_copy(source.at[s, side], outputs[s].at[at], sems.at[len(copies)]))
    for copy in copies:
        copy.start()
    for copy in copies:
        copy.wait()


def call(kernel, flops, room, **kwargs):
    return pl.pallas_call(
        kernel,
        cost_estimate=pl.CostEstimate(flops=flops, bytes_accessed=1 << 16, transcendentals=0),
        compiler_params=pltpu.CompilerParams(vmem_limit_bytes=room << 20),
        **kwargs,
    )


def body(substrate, catalyst, extinction, emission):
    depth, rows, columns = substrate.shape
    count = lax.axis_size("gz")
    wide = columns // count
    me = lax.axis_index("gz").astype(jnp.int32)[None]
    share = OPTICAL / (depth * count)

    def ring(size, shift):
        return [(i, (i + shift) % size) for i in range(size)]

    def up(x, axis):
        return lax.ppermute(x, axis, ring(lax.axis_size(axis), 1))

    def down(x, axis):
        return lax.ppermute(x, axis, ring(lax.axis_size(axis), -1))

    front, back = call(
        planes_kernel,
        1 << 20,
        2,
        name="planes",
        out_shape=(f32(2, rows, columns), f32(2, rows, columns)),
        in_specs=[HBM, HBM],
        out_specs=(VMEM, VMEM),
        scratch_shapes=[pltpu.SemaphoreType.DMA((4,))],
    )(hbm(substrate), hbm(catalyst))
    p_low = up(back, "gz")
    p_high = down(front, "gz")
    own_low, own_high, second, penult = call(
        rows_kernel,
        1 << 20,
        8,
        name="rows",
        out_shape=(
            f32(2, 2, depth, columns),
            f32(2, 2, depth, columns),
            f32(2, rows, columns),
            f32(2, rows, columns),
        ),
        in_specs=[HBM, HBM],
        out_specs=(VMEM, VMEM, VMEM, VMEM),
        scratch_shapes=[
            pltpu.VMEM((2, depth, ROWS, columns), jnp.float32),
            pltpu.VMEM((2, depth, ROWS, columns), jnp.float32),
            pltpu.SemaphoreType.DMA((8,)),
        ],
    )(hbm(substrate), hbm(catalyst))
    from_low = up(own_high, "gx")
    from_high = down(own_low, "gx")

    q_low, q_high = call(
        edge_kernel,
        1 << 22,
        8,
        name="edge",
        out_shape=(f32(2, rows, columns), f32(2, rows, columns)),
        in_specs=[VMEM] * 6,
        out_specs=(VMEM, VMEM),
    )(front, back, second, penult, from_low, from_high)
    q_from_low = up(q_high, "gz")
    q_from_high = down(q_low, "gz")

    sub_part, cat_part, inner, near, far, rows_low, rows_high = call(
        functools.partial(inner_kernel, share),
        1 << 26,
        24,
        name="inner",
        out_shape=(
            f32(depth, rows, columns),
            f32(depth, rows, columns),
            f32(3, rows, columns),
            f32(2, 2, rows, columns),
            f32(2, 2, rows, columns),
            f32(2, depth, columns),
            f32(2, depth, columns),
        ),
        in_specs=[SMEM, SMEM, SMEM, HBM, HBM, VMEM, VMEM, VMEM, VMEM],
        out_specs=(HBM, HBM, VMEM, VMEM, VMEM, VMEM, VMEM),
        scratch_shapes=[
            pltpu.VMEM((2, depth, rows, columns), jnp.float32),
            pltpu.VMEM((2, depth, rows, columns), jnp.float32),
            pltpu.VMEM((2, depth, rows, columns), jnp.float32),
            pltpu.SemaphoreType.DMA((2, depth // 2)),
            pltpu.SemaphoreType.DMA((2, depth // 2)),
        ],
    )(extinction, emission, me, hbm(substrate), hbm(catalyst), from_low, from_high, own_low, own_high)

    p_low, p_high, inner = lax.optimization_barrier((p_low, p_high, inner))
    first_rows, last_rows = call(
        corner_kernel,
        1 << 18,
        2,
        name="corner",
        out_shape=(f32(2, 2, columns), f32(2, 2, columns)),
        in_specs=[VMEM, VMEM],
        out_specs=(VMEM, VMEM),
    )(p_low, p_high)
    corner_low = up(last_rows, "gx")
    corner_high = down(first_rows, "gx")

    ring_planes, known, seen = call(
        functools.partial(rim_kernel, share),
        1 << 23,
        12,
        name="rim",
        out_shape=(f32(2, 2, rows, columns), f32(2, 2, rows, columns), f32(3, rows, columns)),
        in_specs=[SMEM] + [VMEM] * 13,
        out_specs=(VMEM, VMEM, VMEM),
        scratch_shapes=[pltpu.VMEM((2, 2, rows, columns), jnp.float32)],
    )(
        extinction, q_low, q_high, p_low, p_high, front, back, near, far, rows_low, rows_high, corner_low, corner_high, inner
    )

    *pieces, outer = call(
        functools.partial(last_kernel, share),
        1 << 22,
        8,
        name="last",
        out_shape=(*[f32(3, rows, wide)] * count, f32(2, 2, rows, columns)),
        in_specs=[SMEM, SMEM] + [VMEM] * 4,
        out_specs=tuple([VMEM] * (count + 1)),
        scratch_shapes=[pltpu.VMEM((3, rows, columns), jnp.float32)],
    )(extinction, me, known, q_from_low, q_from_high, seen)

    received = [pieces[0]]
    for shift in range(1, count):
        received.append(lax.ppermute(pieces[shift], "gz", ring(count, shift)))

    sub_final, cat_final = call(
        place_kernel,
        1 << 22,
        4,
        name="place",
        out_shape=(f32(depth, rows, columns), f32(depth, rows, columns)),
        in_specs=[VMEM, VMEM, HBM, HBM],
        out_specs=(HBM, HBM),
        input_output_aliases={2: 0, 3: 1},
        scratch_shapes=[pltpu.SemaphoreType.DMA((8,))],
    )(ring_planes, outer, sub_part, cat_part)

    image = call(
        shade_kernel,
        1 << 20,
        8,
        name="shade",
        out_shape=f32(4, rows, wide),
        in_specs=[SMEM, SMEM] + [VMEM] * count,
        out_specs=VMEM,
        scratch_shapes=[pltpu.VMEM((count, 3, rows, wide), jnp.float32)],
    )(emission, me, *received)
    return sub_final, cat_final, image


def solution(mesh):
    placed = (P("gz", "gx", None), P("gz", "gx", None), P(), P())

    return jax.shard_map(
        body,
        mesh=mesh,
        in_specs=placed,
        out_specs=(P("gz", "gx", None), P("gz", "gx", None), P(None, "gx", "gz")),
        check_vma=False,
    )
```

```python
import functools

import jax
import jax.numpy as jnp
from jax import lax
from jax.experimental import pallas as pl
from jax.experimental.pallas import tpu as pltpu
from jax.sharding import PartitionSpec as P


RATES = (0.16, 0.08)
FEED = 0.037
KILL = 0.06
OPTICAL = 4.0
ROWS = 8

HBM = pl.BlockSpec(memory_space=pltpu.HBM)
VMEM = pl.BlockSpec(memory_space=pltpu.VMEM)
SMEM = pl.BlockSpec(memory_space=pltpu.SMEM)


def f32(*shape):
    return jax.ShapeDtypeStruct(shape, jnp.float32)


def hbm(x):
    return pltpu.with_memory_space_constraint(x, pltpu.HBM)


def lanes(x):
    return pltpu.roll(x, 1, axis=x.ndim - 1) + pltpu.roll(x, x.shape[-1] - 1, axis=x.ndim - 1)


def react(sub, cat, around_sub, around_cat):
    growth = sub * cat * cat
    sub_new = (1.0 - 6.0 * RATES[0] - FEED) * sub + RATES[0] * around_sub - growth + FEED
    cat_new = (1.0 - 6.0 * RATES[1] - FEED - KILL) * cat + RATES[1] * around_cat + growth
    return sub_new, cat_new


def plane_step(load, tiles, low_rows, high_rows, across, store):
    for tile in range(tiles):
        sums, olds = [], []
        for s in range(2):
            old = load(s, tile)
            index = lax.broadcasted_iota(jnp.int32, old.shape, 0)
            above = load(s, tile - 1)[ROWS - 1 :] if tile else low_rows and low_rows[s]
            below = load(s, tile + 1)[:1] if tile < tiles - 1 else high_rows and high_rows[s]
            above = 0.0 if above is None else jnp.broadcast_to(above, old.shape)
            below = 0.0 if below is None else jnp.broadcast_to(below, old.shape)
            up = jnp.where(index == 0, above, pltpu.roll(old, 1, axis=0))
            down = jnp.where(index == ROWS - 1, below, pltpu.roll(old, ROWS - 1, axis=0))
            sums.append(lanes(old) + (up + down) + across(s, tile))
            olds.append(old)
        store(tile, *react(olds[0], olds[1], sums[0], sums[1]))


def span(tile):
    return pl.ds(tile * ROWS, ROWS)


def planes_kernel(sub, cat, front, back, sems):
    depth = sub.shape[0]
    copies = []
    for s, field in enumerate((sub, cat)):
        for plane, out in ((0, front), (depth - 1, back)):
            copies.append(pltpu.make_async_copy(field.at[plane], out.at[s], sems.at[len(copies)]))
    for copy in copies:
        copy.start()
    for copy in copies:
        copy.wait()


def prepare_kernel(sub, cat, front, back, low, high, q_low, q_high, heads, tails, second, penult, sems):
    depth, rows, _ = sub.shape
    copies = []
    for s, field in enumerate((sub, cat)):
        for source, out in (
            (field.at[1], second.at[s]),
            (field.at[depth - 2], penult.at[s]),
            (field.at[:, :ROWS], heads.at[s]),
            (field.at[:, rows - ROWS :], tails.at[s]),
        ):
            copies.append(pltpu.make_async_copy(source, out, sems.at[len(copies)]))
    for copy in copies:
        copy.start()
    for at in (0, 1, 4, 5):
        copies[at].wait()
    for outer, inner, out in ((front, second, q_low), (back, penult, q_high)):

        def store(tile, sub, cat, out=out):
            out[0, span(tile), :] = sub
            out[1, span(tile), :] = cat

        plane_step(
            lambda s, tile, outer=outer: outer[s, span(tile), :],
            rows // ROWS,
            None,
            None,
            lambda s, tile, inner=inner: inner[s, span(tile), :],
            store,
        )
    for at in (2, 3, 6, 7):
        copies[at].wait()
    for s in range(2):
        for row in range(2):
            for plane in range(depth):
                low[s, row, plane : plane + 1] = heads[s, plane, row : row + 1]
                high[s, row, plane : plane + 1] = tails[s, plane, ROWS - 2 + row : ROWS - 1 + row]


def composite(sub, cat, scale_sub, scale_cat, clear):
    keep = jnp.exp(-(scale_sub * sub + scale_cat * cat))
    weight = clear * (1.0 - keep)
    return weight * sub, weight * cat, clear * keep


def first_kernel(emission, me, sub, cat, mid, old, sems):
    del emission, me
    depth, rows, _ = sub.shape
    fields = (sub, cat)

    def fetch(s, k):
        return pltpu.make_async_copy(fields[s].at[k], old.at[s, k], sems.at[s, k])

    for k in range(depth):
        for s in range(2):
            fetch(s, k).start()
    for k in range(2):
        for s in range(2):
            fetch(s, k).wait()

    @pl.loop(1, depth - 1)
    def _(k):
        for s in range(2):
            fetch(s, k + 1).wait()

        def store(tile, sub_new, cat_new):
            mid[0, k, span(tile), :] = sub_new
            mid[1, k, span(tile), :] = cat_new

        plane_step(
            lambda s, tile: old[s, k, span(tile), :],
            rows // ROWS,
            None,
            None,
            lambda s, tile: old[s, k - 1, span(tile), :] + old[s, k + 1, span(tile), :],
            store,
        )


def second_kernel(
    share, scale, mid, q_low, q_high, from_low, from_high, own_low, own_high,
    sub_out, cat_out, seen, near, far, rows_low, rows_high,
    heads, tails, new, sem_out,
):
    depth, rows, columns = sub_out.shape
    outputs = (sub_out, cat_out)
    tiles = rows // ROWS
    scale_sub, scale_cat = scale[0] * share, scale[1] * share

    def put(s, k):
        return pltpu.make_async_copy(new.at[s, k], outputs[s].at[k], sem_out.at[s, k])

    which = lax.broadcasted_iota(jnp.int32, (depth, columns), 0)
    for got, at, own, at_own, out in (
        (from_low, 1, own_low, 0, rows_low),
        (from_high, 0, own_high, 1, rows_high),
    ):
        sums, olds = [], []
        for s in range(2):
            here = got[s, at]
            ahead = jnp.where(which == 0, 0.0, pltpu.roll(here, 1, axis=0))
            behind = jnp.where(which == depth - 1, 0.0, pltpu.roll(here, depth - 1, axis=0))
            sums.append(lanes(here) + (got[s, 1 - at] + own[s, at_own]) + (ahead + behind))
            olds.append(here)
        sub, cat = react(olds[0], olds[1], sums[0], sums[1])
        out[0] = sub
        out[1] = cat

    index = lax.broadcasted_iota(jnp.int32, (ROWS, columns), 0)

    def with_low(s, k, tile):
        row = jnp.broadcast_to(from_low[s, 1, pl.ds(k, 1)], tile.shape)
        return tile + jnp.where(index == 0, RATES[s] * row, 0.0)

    def with_high(s, k, tile):
        row = jnp.broadcast_to(from_high[s, 0, pl.ds(k, 1)], tile.shape)
        return tile + jnp.where(index == ROWS - 1, RATES[s] * row, 0.0)

    @pl.loop(1, depth - 1)
    def _(k):
        for s in range(2):
            heads[s, k] = with_low(s, k, mid[s, k, span(0), :])
            tails[s, k] = with_high(s, k, mid[s, k, span(tiles - 1), :])

    def load(s, k, tile):
        if tile == 0:
            return heads[s, k]
        if tile == tiles - 1:
            return tails[s, k]
        return mid[s, k, span(tile), :]

    for s in range(2):
        for tile in range(tiles):
            first, last = q_low[s, span(tile), :], q_high[s, span(tile), :]
            if tile == 0:
                first, last = with_low(s, 0, first), with_low(s, depth - 1, last)
            if tile == tiles - 1:
                first, last = with_high(s, 0, first), with_high(s, depth - 1, last)
            near[s, 0, span(tile), :] = first
            far[s, 2, span(tile), :] = last
            for j in range(2):
                near[s, 1 + j, span(tile), :] = load(s, 1 + j, tile)
                far[s, j, span(tile), :] = load(s, depth - 3 + j, tile)

    seen[0] = jnp.zeros((rows, columns), jnp.float32)
    seen[1] = jnp.zeros((rows, columns), jnp.float32)
    seen[2] = jnp.ones((rows, columns), jnp.float32)

    @pl.loop(2, depth - 2)
    def _(k):
        def store(tile, sub, cat):
            at = span(tile)
            new[0, k, at, :] = sub
            new[1, k, at, :] = cat
            one, two, clear = composite(sub, cat, scale_sub, scale_cat, seen[2, at, :])
            seen[0, at, :] += one
            seen[1, at, :] += two
            seen[2, at, :] = clear

        plane_step(
            lambda s, tile: load(s, k, tile),
            tiles,
            [rows_low[s, pl.ds(k, 1)] for s in range(2)],
            [rows_high[s, pl.ds(k, 1)] for s in range(2)],
            lambda s, tile: load(s, k - 1, tile) + load(s, k + 1, tile),
            store,
        )
        for s in range(2):
            put(s, k).start()

    @pl.loop(2, depth - 2)
    def _(k):
        for s in range(2):
            put(s, k).wait()


def corner_kernel(p_low, p_high, first, last):
    rows = p_low.shape[1]
    for side, p in enumerate((p_low, p_high)):
        for s in range(2):
            first[side, s : s + 1] = p[s, :1]
            last[side, s : s + 1] = p[s, rows - 1 :]


def rim_kernel(
    share, scale, p_low, p_high, front, back, near, far, rows_low, rows_high, inner,
    ring, known, seen, mid,
):
    depth = rows_low.shape[1]
    rows = p_low.shape[1]
    tiles = rows // ROWS
    scale_sub, scale_cat = scale[0] * share, scale[1] * share
    for side, p, own, inside in ((0, p_low, front, near), (1, p_high, back, far)):
        zero, one, two = (0, 1, 2) if side == 0 else (2, 1, 0)
        outer, beside = (0, 1) if side == 0 else (depth - 1, depth - 2)
        for s in range(2):
            mid[side, s] = inside[s, zero] + RATES[s] * p[s]

        def store_known(tile, sub, cat, side=side, own=own):
            at = span(tile)
            known[side, 0, at, :] = sub + (RATES[0] * RATES[0]) * own[0, at, :]
            known[side, 1, at, :] = cat + (RATES[1] * RATES[1]) * own[1, at, :]

        plane_step(
            lambda s, tile, side=side: mid[side, s, span(tile), :],
            tiles,
            [rows_low[s, outer : outer + 1] for s in range(2)],
            [rows_high[s, outer : outer + 1] for s in range(2)],
            lambda s, tile, inside=inside, one=one: inside[s, one, span(tile), :],
            store_known,
        )

        def store_ring(tile, sub, cat, side=side):
            ring[0, side, span(tile), :] = sub
            ring[1, side, span(tile), :] = cat

        plane_step(
            lambda s, tile, inside=inside, one=one: inside[s, one, span(tile), :],
            tiles,
            [rows_low[s, beside : beside + 1] for s in range(2)],
            [rows_high[s, beside : beside + 1] for s in range(2)],
            lambda s, tile, inside=inside, two=two, side=side: inside[s, two, span(tile), :]
            + mid[side, s, span(tile), :],
            store_ring,
        )

    for tile in range(tiles):
        at = span(tile)
        one, two, clear = composite(ring[0, 0, at, :], ring[1, 0, at, :], scale_sub, scale_cat, 1.0)
        sub = one + clear * inner[0, at, :]
        cat = two + clear * inner[1, at, :]
        clear = clear * inner[2, at, :]
        one, two, clear = composite(ring[0, 1, at, :], ring[1, 1, at, :], scale_sub, scale_cat, clear)
        seen[0, at, :] = sub + one
        seen[1, at, :] = cat + two
        seen[2, at, :] = clear


def last_kernel(share, scale, me, known, q_low, q_high, seen, corner_low, corner_high, *outs_and_scratch):
    *pieces, outer, whole = outs_and_scratch
    rows, columns = seen.shape[1:]
    count = len(pieces)
    wide = columns // count
    tiles = rows // ROWS
    scale_sub, scale_cat = scale[0] * share, scale[1] * share
    index = lax.broadcasted_iota(jnp.int32, (ROWS, columns), 0)
    for tile in range(tiles):
        at = span(tile)
        planes = []
        for side, q in enumerate((q_low, q_high)):
            for s in range(2):
                value = known[side, s, at, :] + RATES[s] * q[s, at, :]
                twice = 2.0 * RATES[s] * RATES[s]
                if tile == 0:
                    row = jnp.broadcast_to(corner_low[side, s : s + 1], value.shape)
                    value = value + jnp.where(index == 0, twice * row, 0.0)
                if tile == tiles - 1:
                    row = jnp.broadcast_to(corner_high[side, s : s + 1], value.shape)
                    value = value + jnp.where(index == ROWS - 1, twice * row, 0.0)
                outer[s, side, at, :] = value
                planes.append(value)
        one, two, clear = composite(planes[0], planes[1], scale_sub, scale_cat, 1.0)
        sub = one + clear * seen[0, at, :]
        cat = two + clear * seen[1, at, :]
        clear = clear * seen[2, at, :]
        one, two, clear = composite(planes[2], planes[3], scale_sub, scale_cat, clear)
        whole[0, at, :] = sub + one
        whole[1, at, :] = cat + two
        whole[2, at, :] = clear
    for shift, piece in enumerate(pieces):
        target = lax.rem(me[0] + shift, count)
        if wide % 128 == 0:
            piece[...] = whole[:, :, pl.ds(pl.multiple_of(target * wide, 128), wide)]
        else:
            for other in range(count):

                @pl.when(target == other)
                def _(piece=piece, other=other):
                    piece[...] = whole[:, :, other * wide : (other + 1) * wide]


def shade_kernel(emission, me, *pieces_and_rest):
    *pieces, image, slabs = pieces_and_rest
    count = len(pieces)
    for shift, piece in enumerate(pieces):
        slabs[lax.rem(me[0] + count - shift, count)] = piece[...]
    sub, cat, clear = slabs[0, 0], slabs[0, 1], slabs[0, 2]
    for slab in range(1, count):
        sub = sub + clear * slabs[slab, 0]
        cat = cat + clear * slabs[slab, 1]
        clear = clear * slabs[slab, 2]
    for channel in range(3):
        image[channel] = emission[channel, 0] * sub + emission[channel, 1] * cat
    image[3] = 1.0 - clear


def place_kernel(ring, outer, sub_in, cat_in, sub_out, cat_out, sems):
    del sub_in, cat_in
    depth = sub_out.shape[0]
    outputs = (sub_out, cat_out)
    copies = []
    for s in range(2):
        for side in range(2):
            for at, source in ((side * (depth - 1), outer), (1 + side * (depth - 3), ring)):
                copies.append(pltpu.make_async_copy(source.at[s, side], outputs[s].at[at], sems.at[len(copies)]))
    for copy in copies:
        copy.start()
    for copy in copies:
        copy.wait()


def call(kernel, flops, room, **kwargs):
    return pl.pallas_call(
        kernel,
        cost_estimate=pl.CostEstimate(flops=flops, bytes_accessed=1 << 16, transcendentals=0),
        compiler_params=pltpu.CompilerParams(vmem_limit_bytes=room << 20),
        **kwargs,
    )


def body(substrate, catalyst, extinction, emission):
    depth, rows, columns = substrate.shape
    count = lax.axis_size("gz")
    wide = columns // count
    me = lax.axis_index("gz").astype(jnp.int32)[None]
    share = OPTICAL / (depth * count)

    def ring(size, shift):
        return [(i, (i + shift) % size) for i in range(size)]

    def up(x, axis):
        return lax.ppermute(x, axis, ring(lax.axis_size(axis), 1))

    def down(x, axis):
        return lax.ppermute(x, axis, ring(lax.axis_size(axis), -1))

    front, back = call(
        planes_kernel,
        1 << 20,
        2,
        name="planes",
        out_shape=(f32(2, rows, columns), f32(2, rows, columns)),
        in_specs=[HBM, HBM],
        out_specs=(VMEM, VMEM),
        scratch_shapes=[pltpu.SemaphoreType.DMA((4,))],
    )(hbm(substrate), hbm(catalyst))
    p_low = up(back, "gz")
    p_high = down(front, "gz")
    p_low = up(back, "gz")
    p_high = down(front, "gz")

    own_low, own_high, q_low, q_high = call(
        prepare_kernel,
        1 << 22,
        8,
        name="prepare",
        out_shape=(
            f32(2, 2, depth, columns),
            f32(2, 2, depth, columns),
            f32(2, rows, columns),
            f32(2, rows, columns),
        ),
        in_specs=[HBM, HBM, VMEM, VMEM],
        out_specs=(VMEM, VMEM, VMEM, VMEM),
        scratch_shapes=[
            pltpu.VMEM((2, depth, ROWS, columns), jnp.float32),
            pltpu.VMEM((2, depth, ROWS, columns), jnp.float32),
            pltpu.VMEM((2, rows, columns), jnp.float32),
            pltpu.VMEM((2, rows, columns), jnp.float32),
            pltpu.SemaphoreType.DMA((8,)),
        ],
    )(hbm(substrate), hbm(catalyst), front, back)
    from_low = up(own_high, "gx")
    from_high = down(own_low, "gx")
    q_from_low = up(q_high, "gz")
    q_from_high = down(q_low, "gz")

    mid = call(
        first_kernel,
        1 << 24,
        12,
        name="first",
        out_shape=f32(2, depth, rows, columns),
        in_specs=[SMEM, SMEM, HBM, HBM],
        out_specs=VMEM,
        scratch_shapes=[
            pltpu.VMEM((2, depth, rows, columns), jnp.float32),
            pltpu.SemaphoreType.DMA((2, depth)),
        ],
    )(emission, me, hbm(substrate), hbm(catalyst))

    sub_part, cat_part, inner, near, far, rows_low, rows_high = call(
        functools.partial(second_kernel, share),
        1 << 25,
        20,
        name="second",
        out_shape=(
            f32(depth, rows, columns),
            f32(depth, rows, columns),
            f32(3, rows, columns),
            f32(2, 3, rows, columns),
            f32(2, 3, rows, columns),
            f32(2, depth, columns),
            f32(2, depth, columns),
        ),
        in_specs=[SMEM] + [VMEM] * 7,
        out_specs=(HBM, HBM, VMEM, VMEM, VMEM, VMEM, VMEM),
        scratch_shapes=[
            pltpu.VMEM((2, depth, ROWS, columns), jnp.float32),
            pltpu.VMEM((2, depth, ROWS, columns), jnp.float32),
            pltpu.VMEM((2, depth, rows, columns), jnp.float32),
            pltpu.SemaphoreType.DMA((2, depth)),
        ],
    )(extinction, mid, q_low, q_high, from_low, from_high, own_low, own_high)

    p_low, p_high, inner = lax.optimization_barrier((p_low, p_high, inner))
    first_rows, last_rows = call(
        corner_kernel,
        1 << 18,
        2,
        name="corner",
        out_shape=(f32(2, 2, columns), f32(2, 2, columns)),
        in_specs=[VMEM, VMEM],
        out_specs=(VMEM, VMEM),
    )(p_low, p_high)
    corner_low = up(last_rows, "gx")
    corner_high = down(first_rows, "gx")

    ring_planes, known, seen = call(
        functools.partial(rim_kernel, share),
        1 << 23,
        12,
        name="rim",
        out_shape=(f32(2, 2, rows, columns), f32(2, 2, rows, columns), f32(3, rows, columns)),
        in_specs=[SMEM] + [VMEM] * 9,
        out_specs=(VMEM, VMEM, VMEM),
        scratch_shapes=[pltpu.VMEM((2, 2, rows, columns), jnp.float32)],
    )(extinction, p_low, p_high, front, back, near, far, rows_low, rows_high, inner)

    *pieces, outer = call(
        functools.partial(last_kernel, share),
        1 << 22,
        8,
        name="last",
        out_shape=(*[f32(3, rows, wide)] * count, f32(2, 2, rows, columns)),
        in_specs=[SMEM, SMEM] + [VMEM] * 6,
        out_specs=tuple([VMEM] * (count + 1)),
        scratch_shapes=[pltpu.VMEM((3, rows, columns), jnp.float32)],
    )(extinction, me, known, q_from_low, q_from_high, seen, corner_low, corner_high)

    received = [pieces[0]]
    for shift in range(1, count):
        received.append(lax.ppermute(pieces[shift], "gz", ring(count, shift)))

    sub_final, cat_final = call(
        place_kernel,
        1 << 22,
        4,
        name="place",
        out_shape=(f32(depth, rows, columns), f32(depth, rows, columns)),
        in_specs=[VMEM, VMEM, HBM, HBM],
        out_specs=(HBM, HBM),
        input_output_aliases={2: 0, 3: 1},
        scratch_shapes=[pltpu.SemaphoreType.DMA((8,))],
    )(ring_planes, outer, sub_part, cat_part)

    image = call(
        shade_kernel,
        1 << 20,
        8,
        name="shade",
        out_shape=f32(4, rows, wide),
        in_specs=[SMEM, SMEM] + [VMEM] * count,
        out_specs=VMEM,
        scratch_shapes=[pltpu.VMEM((count, 3, rows, wide), jnp.float32)],
    )(emission, me, *received)
    return sub_final, cat_final, image


def solution(mesh):
    placed = (P("gz", "gx", None), P("gz", "gx", None), P(), P())

    return jax.shard_map(
        body,
        mesh=mesh,
        in_specs=placed,
        out_specs=(P("gz", "gx", None), P("gz", "gx", None), P(None, "gx", "gz")),
        check_vma=False,
    )
```

```python
import functools

import jax
import jax.numpy as jnp
from jax import lax
from jax.experimental import pallas as pl
from jax.experimental.pallas import tpu as pltpu
from jax.sharding import PartitionSpec as P


RATES = (0.16, 0.08)
FEED = 0.037
KILL = 0.06
OPTICAL = 4.0
ROWS, LANES = 8, 128

HBM = pl.BlockSpec(memory_space=pltpu.HBM)
VMEM = pl.BlockSpec(memory_space=pltpu.VMEM)
SMEM = pl.BlockSpec(memory_space=pltpu.SMEM)


def f32(*shape):
    return jax.ShapeDtypeStruct(shape, jnp.float32)


def hbm(x):
    return pltpu.with_memory_space_constraint(x, pltpu.HBM)


def lanes(x):
    return pltpu.roll(x, 1, axis=x.ndim - 1) + pltpu.roll(x, x.shape[-1] - 1, axis=x.ndim - 1)


def react(sub, cat, around_sub, around_cat):
    growth = sub * cat * cat
    sub_new = (1.0 - 6.0 * RATES[0] - FEED) * sub + RATES[0] * around_sub - growth + FEED
    cat_new = (1.0 - 6.0 * RATES[1] - FEED - KILL) * cat + RATES[1] * around_cat + growth
    return sub_new, cat_new


def plane_step(load, tiles, low_rows, high_rows, across, store, only=None):
    for tile in range(tiles) if only is None else only:
        sums, olds = [], []
        for s in range(2):
            old = load(s, tile)
            index = lax.broadcasted_iota(jnp.int32, old.shape, 0)
            above = load(s, tile - 1)[ROWS - 1 :] if tile else low_rows and low_rows[s]
            below = load(s, tile + 1)[:1] if tile < tiles - 1 else high_rows and high_rows[s]
            above = 0.0 if above is None else jnp.broadcast_to(above, old.shape)
            below = 0.0 if below is None else jnp.broadcast_to(below, old.shape)
            up = jnp.where(index == 0, above, pltpu.roll(old, 1, axis=0))
            down = jnp.where(index == ROWS - 1, below, pltpu.roll(old, ROWS - 1, axis=0))
            sums.append(lanes(old) + (up + down) + across(s, tile))
            olds.append(old)
        store(tile, *react(olds[0], olds[1], sums[0], sums[1]))


def span(tile):
    return pl.ds(tile * ROWS, ROWS)


def across_columns(tile, columns):
    return tile[:, :columns] if columns <= LANES else jnp.concatenate([tile] * (columns // LANES), axis=1)


def outer_step(outer, inner, rows, only, store):
    plane_step(
        lambda s, tile: outer[s, span(tile), :],
        rows // ROWS,
        None,
        None,
        lambda s, tile: inner[s, span(tile), :],
        store,
        only,
    )


def planes_kernel(sub, cat, up, down, second, penult, sems):
    depth, rows, _ = sub.shape
    copies = []
    for s, field in enumerate((sub, cat)):
        for plane, out in (
            (depth - 1, up.at[s, pl.ds(0, rows)]),
            (depth - 2, penult.at[s]),
            (0, down.at[s, pl.ds(0, rows)]),
            (1, second.at[s]),
        ):
            copies.append(pltpu.make_async_copy(field.at[plane], out, sems.at[len(copies)]))
    for copy in copies:
        copy.start()
    for copy in copies:
        copy.wait()
    for outer, inner in ((up, penult), (down, second)):

        def store(tile, sub_new, cat_new, outer=outer):
            at = pl.ds(rows + (tile - 1) * ROWS, ROWS)
            outer[0, at, :] = sub_new
            outer[1, at, :] = cat_new

        outer_step(outer, inner, rows, range(1, rows // ROWS - 1), store)


def prepare_kernel(
    share, scale, emission, sub, cat, up, down, second, penult,
    old, low, high, q_up, q_down, values, sems,
):
    depth, rows, _ = sub.shape
    copies = []
    for plane in range(depth):
        for s, field in enumerate((sub, cat)):
            copies.append(pltpu.make_async_copy(field.at[plane], old.at[s, plane], sems.at[s, plane]))
    for copy in copies:
        copy.start()
    shape = values.shape[1:]
    for s in range(2):
        values[s] = jnp.full(shape, scale[s] * share, jnp.float32)
        for channel in range(3):
            values[2 + channel * 2 + s] = jnp.full(shape, emission[channel, s], jnp.float32)
    for outer, inner, out in ((up, penult, q_up), (down, second, q_down)):

        def store(tile, sub_new, cat_new, out=out):
            at = span(0 if tile == 0 else 1)
            out[0, at, :] = sub_new
            out[1, at, :] = cat_new

        outer_step(outer, inner, rows, (0, rows // ROWS - 1), store)
    for copy in copies:
        copy.wait()
    for s in range(2):
        for row in range(2):
            for plane in range(depth):
                low[s, row, plane : plane + 1] = old[s, plane, row : row + 1]
                high[s, row, plane : plane + 1] = old[s, plane, rows - 2 + row : rows - 1 + row]


def composite(sub, cat, scale_sub, scale_cat, clear):
    keep = jnp.exp(-(scale_sub * sub + scale_cat * cat))
    weight = clear * (1.0 - keep)
    return weight * sub, weight * cat, clear * keep


def first_kernel(old, mid):
    depth, rows, _ = old.shape[1:]

    @pl.loop(1, depth - 1)
    def _(k):
        def store(tile, sub, cat):
            mid[0, k, span(tile), :] = sub
            mid[1, k, span(tile), :] = cat

        plane_step(
            lambda s, tile: old[s, k, span(tile), :],
            rows // ROWS,
            None,
            None,
            lambda s, tile: old[s, k - 1, span(tile), :] + old[s, k + 1, span(tile), :],
            store,
        )


def second_kernel(
    values, mid, up, down, q_up, q_down, from_low, from_high, own_low, own_high,
    sub_out, cat_out, seen, near, far, rows_low, rows_high,
    heads, tails, new, sem_out,
):
    depth, rows, columns = sub_out.shape
    outputs = (sub_out, cat_out)
    tiles = rows // ROWS
    scale_sub, scale_cat = across_columns(values[0], columns), across_columns(values[1], columns)

    def put(s, k):
        return pltpu.make_async_copy(new.at[s, k], outputs[s].at[k], sem_out.at[s, k])

    which = lax.broadcasted_iota(jnp.int32, (depth, columns), 0)
    for got, at, own, at_own, out in (
        (from_low, 1, own_low, 0, rows_low),
        (from_high, 0, own_high, 1, rows_high),
    ):
        sums, olds = [], []
        for s in range(2):
            here = got[s, at]
            ahead = jnp.where(which == 0, 0.0, pltpu.roll(here, 1, axis=0))
            behind = jnp.where(which == depth - 1, 0.0, pltpu.roll(here, depth - 1, axis=0))
            sums.append(lanes(here) + (got[s, 1 - at] + own[s, at_own]) + (ahead + behind))
            olds.append(here)
        sub, cat = react(olds[0], olds[1], sums[0], sums[1])
        out[0] = sub
        out[1] = cat

    index = lax.broadcasted_iota(jnp.int32, (ROWS, columns), 0)

    def with_low(s, k, tile):
        row = jnp.broadcast_to(from_low[s, 1, pl.ds(k, 1)], tile.shape)
        return tile + jnp.where(index == 0, RATES[s] * row, 0.0)

    def with_high(s, k, tile):
        row = jnp.broadcast_to(from_high[s, 0, pl.ds(k, 1)], tile.shape)
        return tile + jnp.where(index == ROWS - 1, RATES[s] * row, 0.0)

    @pl.loop(1, depth - 1)
    def _(k):
        for s in range(2):
            heads[s, k] = with_low(s, k, mid[s, k, span(0), :])
            tails[s, k] = with_high(s, k, mid[s, k, span(tiles - 1), :])

    def load(s, k, tile):
        if tile == 0:
            return heads[s, k]
        if tile == tiles - 1:
            return tails[s, k]
        return mid[s, k, span(tile), :]

    for s in range(2):
        for tile in range(tiles):
            if 0 < tile < tiles - 1:
                at = pl.ds(rows + (tile - 1) * ROWS, ROWS)
                first, last = down[s, at, :], up[s, at, :]
            else:
                first, last = q_down[s, span(1 if tile else 0), :], q_up[s, span(1 if tile else 0), :]
            if tile == 0:
                first, last = with_low(s, 0, first), with_low(s, depth - 1, last)
            if tile == tiles - 1:
                first, last = with_high(s, 0, first), with_high(s, depth - 1, last)
            near[s, 0, span(tile), :] = first
            far[s, 2, span(tile), :] = last
            for j in range(2):
                near[s, 1 + j, span(tile), :] = load(s, 1 + j, tile)
                far[s, j, span(tile), :] = load(s, depth - 3 + j, tile)

    seen[0] = jnp.zeros((rows, columns), jnp.float32)
    seen[1] = jnp.zeros((rows, columns), jnp.float32)
    seen[2] = jnp.ones((rows, columns), jnp.float32)

    @pl.loop(2, depth - 2)
    def _(k):
        def store(tile, sub, cat):
            at = span(tile)
            new[0, k, at, :] = sub
            new[1, k, at, :] = cat
            one, two, clear = composite(sub, cat, scale_sub, scale_cat, seen[2, at, :])
            seen[0, at, :] += one
            seen[1, at, :] += two
            seen[2, at, :] = clear

        plane_step(
            lambda s, tile: load(s, k, tile),
            tiles,
            [rows_low[s, pl.ds(k, 1)] for s in range(2)],
            [rows_high[s, pl.ds(k, 1)] for s in range(2)],
            lambda s, tile: load(s, k - 1, tile) + load(s, k + 1, tile),
            store,
        )
        for s in range(2):
            put(s, k).start()

    @pl.loop(2, depth - 2)
    def _(k):
        for s in range(2):
            put(s, k).wait()


def corner_kernel(rows, p_low, p_high, first, last):
    for side, p in enumerate((p_low, p_high)):
        for s in range(2):
            first[side, s : s + 1] = p[s, :1]
            last[side, s : s + 1] = p[s, rows - 1 : rows]


def rim_kernel(
    values, p_low, p_high, down, up, near, far, rows_low, rows_high, inner,
    ring, known, seen, mid,
):
    depth = rows_low.shape[1]
    rows, columns = inner.shape[1:]
    tiles = rows // ROWS
    scale_sub, scale_cat = across_columns(values[0], columns), across_columns(values[1], columns)
    for side, p, own, inside in ((0, p_low, down, near), (1, p_high, up, far)):
        zero, one, two = (0, 1, 2) if side == 0 else (2, 1, 0)
        outer, beside = (0, 1) if side == 0 else (depth - 1, depth - 2)
        for s in range(2):
            mid[side, s] = inside[s, zero] + RATES[s] * p[s, :rows]

        def store_known(tile, sub, cat, side=side, own=own):
            at = span(tile)
            known[side, 0, at, :] = sub + (RATES[0] * RATES[0]) * own[0, at, :]
            known[side, 1, at, :] = cat + (RATES[1] * RATES[1]) * own[1, at, :]

        plane_step(
            lambda s, tile, side=side: mid[side, s, span(tile), :],
            tiles,
            [rows_low[s, outer : outer + 1] for s in range(2)],
            [rows_high[s, outer : outer + 1] for s in range(2)],
            lambda s, tile, inside=inside, one=one: inside[s, one, span(tile), :],
            store_known,
        )

        def store_ring(tile, sub, cat, side=side):
            ring[0, side, span(tile), :] = sub
            ring[1, side, span(tile), :] = cat

        plane_step(
            lambda s, tile, inside=inside, one=one: inside[s, one, span(tile), :],
            tiles,
            [rows_low[s, beside : beside + 1] for s in range(2)],
            [rows_high[s, beside : beside + 1] for s in range(2)],
            lambda s, tile, inside=inside, two=two, side=side: inside[s, two, span(tile), :]
            + mid[side, s, span(tile), :],
            store_ring,
        )

    for tile in range(tiles):
        at = span(tile)
        one, two, clear = composite(ring[0, 0, at, :], ring[1, 0, at, :], scale_sub, scale_cat, 1.0)
        sub = one + clear * inner[0, at, :]
        cat = two + clear * inner[1, at, :]
        clear = clear * inner[2, at, :]
        one, two, clear = composite(ring[0, 1, at, :], ring[1, 1, at, :], scale_sub, scale_cat, clear)
        seen[0, at, :] = sub + one
        seen[1, at, :] = cat + two
        seen[2, at, :] = clear


def last_kernel(corners, values, known, q_low, q_high, seen, *rest):
    if corners:
        corner_low, corner_high, *rest = rest
    *pieces, outer, whole = rest
    rows, columns = seen.shape[1:]
    count = len(pieces)
    wide = columns // count
    tiles = rows // ROWS
    scale_sub, scale_cat = across_columns(values[0], columns), across_columns(values[1], columns)
    index = lax.broadcasted_iota(jnp.int32, (ROWS, columns), 0)
    for place, tile in enumerate((0, tiles - 1) if corners else range(1, tiles - 1)):
        at, to = span(tile), span(place)
        source = to if corners else pl.ds(rows + place * ROWS, ROWS)
        planes = []
        for side, q in enumerate((q_low, q_high)):
            for s in range(2):
                value = known[side, s, at, :] + RATES[s] * q[s, source, :]
                if corners:
                    corner, edge = (corner_low, 0) if tile == 0 else (corner_high, ROWS - 1)
                    row = jnp.broadcast_to(corner[side, s : s + 1], value.shape)
                    value = value + jnp.where(index == edge, (2.0 * RATES[s] * RATES[s]) * row, 0.0)
                outer[s, side, to, :] = value
                planes.append(value)
        one, two, clear = composite(planes[0], planes[1], scale_sub, scale_cat, 1.0)
        sub = one + clear * seen[0, at, :]
        cat = two + clear * seen[1, at, :]
        clear = clear * seen[2, at, :]
        one, two, clear = composite(planes[2], planes[3], scale_sub, scale_cat, clear)
        whole[0, to, :] = sub + one
        whole[1, to, :] = cat + two
        whole[2, to, :] = clear
    me = lax.axis_index("gz")
    for shift, piece in enumerate(pieces):
        target = lax.rem(me + shift, count)
        if wide % LANES == 0:
            piece[...] = whole[:, :, pl.ds(pl.multiple_of(target * wide, LANES), wide)]
        else:
            for other in range(count):

                @pl.when(target == other)
                def _(piece=piece, other=other):
                    piece[...] = whole[:, :, other * wide : (other + 1) * wide]


def shade_kernel(values, *pieces_and_rest):
    *pieces, image, slabs = pieces_and_rest
    count = len(pieces) // 2
    rows, wide = image.shape[1:]
    me = lax.axis_index("gz")
    for shift in range(count):
        slab = lax.rem(me + count - shift, count)
        inner, outer = pieces[shift], pieces[count + shift]
        slabs[slab, :, pl.ds(ROWS, rows - 2 * ROWS), :] = inner[...]
        slabs[slab, :, pl.ds(0, ROWS), :] = outer[:, :ROWS]
        slabs[slab, :, pl.ds(rows - ROWS, ROWS), :] = outer[:, ROWS:]
    for tile in range(rows // ROWS):
        at = span(tile)
        sub, cat, clear = slabs[0, 0, at, :], slabs[0, 1, at, :], slabs[0, 2, at, :]
        for slab in range(1, count):
            sub = sub + clear * slabs[slab, 0, at, :]
            cat = cat + clear * slabs[slab, 1, at, :]
            clear = clear * slabs[slab, 2, at, :]
        for channel in range(3):
            of_sub = across_columns(values[2 + channel * 2], wide)
            of_cat = across_columns(values[3 + channel * 2], wide)
            image[channel, at, :] = of_sub * sub + of_cat * cat
        image[3, at, :] = 1.0 - clear


def place_kernel(ring, inner, outer, sub_in, cat_in, sub_out, cat_out, sems):
    del sub_in, cat_in
    depth, rows, _ = sub_out.shape
    copies = []
    for s, out in enumerate((sub_out, cat_out)):
        for side in range(2):
            plane = side * (depth - 1)
            for source, target in (
                (ring.at[s, side], out.at[1 + side * (depth - 3)]),
                (inner.at[s, side], out.at[plane, pl.ds(ROWS, rows - 2 * ROWS)]),
                (outer.at[s, side, pl.ds(0, ROWS)], out.at[plane, pl.ds(0, ROWS)]),
                (outer.at[s, side, pl.ds(ROWS, ROWS)], out.at[plane, pl.ds(rows - ROWS, ROWS)]),
            ):
                copies.append(pltpu.make_async_copy(source, target, sems.at[len(copies)]))
    for copy in copies:
        copy.start()
    for copy in copies:
        copy.wait()


def call(kernel, flops, room, **kwargs):
    return pl.pallas_call(
        kernel,
        cost_estimate=pl.CostEstimate(flops=flops, bytes_accessed=1 << 16, transcendentals=0),
        compiler_params=pltpu.CompilerParams(vmem_limit_bytes=room << 20),
        **kwargs,
    )


def body(substrate, catalyst, extinction, emission):
    depth, rows, columns = substrate.shape
    count = lax.axis_size("gz")
    wide = columns // count
    share = OPTICAL / (depth * count)
    middle = rows - 2 * ROWS
    outers = 2 * ROWS

    def ring(size, shift):
        return [(i, (i + shift) % size) for i in range(size)]

    def shifted(x, axis, shift):
        return lax.ppermute(x, axis, ring(lax.axis_size(axis), shift))

    up, down, second, penult = call(
        planes_kernel,
        1 << 20,
        2,
        name="planes",
        out_shape=(f32(2, rows + middle, columns),) * 2 + (f32(2, rows, columns),) * 2,
        in_specs=[HBM, HBM],
        out_specs=(VMEM,) * 4,
        scratch_shapes=[pltpu.SemaphoreType.DMA((8,))],
    )(hbm(substrate), hbm(catalyst))
    p_low = shifted(up, "gz", 1)
    p_high = shifted(down, "gz", -1)

    old, own_low, own_high, q_up, q_down, values = call(
        functools.partial(prepare_kernel, share),
        1 << 22,
        2,
        name="prepare",
        out_shape=(
            f32(2, depth, rows, columns),
            f32(2, 2, depth, columns),
            f32(2, 2, depth, columns),
            f32(2, outers, columns),
            f32(2, outers, columns),
            f32(8, ROWS, LANES),
        ),
        in_specs=[SMEM, SMEM, HBM, HBM, VMEM, VMEM, VMEM, VMEM],
        out_specs=(VMEM,) * 6,
        scratch_shapes=[pltpu.SemaphoreType.DMA((2, depth))],
    )(extinction, emission, hbm(substrate), hbm(catalyst), up, down, second, penult)
    from_low = shifted(own_high, "gx", 1)
    from_high = shifted(own_low, "gx", -1)
    q_low = shifted(q_up, "gz", 1)
    q_high = shifted(q_down, "gz", -1)

    mid = call(
        first_kernel,
        1 << 24,
        2,
        name="first",
        out_shape=f32(2, depth, rows, columns),
        in_specs=[VMEM],
        out_specs=VMEM,
    )(old)

    sub_part, cat_part, inner, near, far, rows_low, rows_high = call(
        second_kernel,
        1 << 25,
        10,
        name="second",
        out_shape=(
            f32(depth, rows, columns),
            f32(depth, rows, columns),
            f32(3, rows, columns),
            f32(2, 3, rows, columns),
            f32(2, 3, rows, columns),
            f32(2, depth, columns),
            f32(2, depth, columns),
        ),
        in_specs=[VMEM] * 10,
        out_specs=(HBM, HBM) + (VMEM,) * 5,
        scratch_shapes=[
            pltpu.VMEM((2, depth, ROWS, columns), jnp.float32),
            pltpu.VMEM((2, depth, ROWS, columns), jnp.float32),
            pltpu.VMEM((2, depth, rows, columns), jnp.float32),
            pltpu.SemaphoreType.DMA((2, depth)),
        ],
    )(values, mid, up, down, q_up, q_down, from_low, from_high, own_low, own_high)

    p_low, p_high, inner = lax.optimization_barrier((p_low, p_high, inner))
    ring_planes, known, seen = call(
        rim_kernel,
        1 << 23,
        4,
        name="rim",
        out_shape=(f32(2, 2, rows, columns), f32(2, 2, rows, columns), f32(3, rows, columns)),
        in_specs=[VMEM] * 10,
        out_specs=(VMEM,) * 3,
        scratch_shapes=[pltpu.VMEM((2, 2, rows, columns), jnp.float32)],
    )(values, p_low, p_high, down, up, near, far, rows_low, rows_high, inner)

    def finish(corners, high, *args):
        *pieces, outer = call(
            functools.partial(last_kernel, corners),
            1 << 22,
            4,
            name="last" if corners else "most",
            out_shape=(f32(3, high, wide),) * count + (f32(2, 2, high, columns),),
            in_specs=[VMEM] * len(args),
            out_specs=(VMEM,) * (count + 1),
            scratch_shapes=[pltpu.VMEM((3, high, columns), jnp.float32)],
        )(*args)
        return [pieces[0]] + [shifted(pieces[i], "gz", i) for i in range(1, count)], outer

    inner_pieces, inner_rows = finish(False, middle, values, known, p_low, p_high, seen)

    first_rows, last_rows = call(
        functools.partial(corner_kernel, rows),
        1 << 18,
        2,
        name="corner",
        out_shape=(f32(2, 2, columns), f32(2, 2, columns)),
        in_specs=[VMEM, VMEM],
        out_specs=(VMEM, VMEM),
    )(p_low, p_high)
    corner_low = shifted(last_rows, "gx", 1)
    corner_high = shifted(first_rows, "gx", -1)

    outer_pieces, outer_rows = finish(True, outers, values, known, q_low, q_high, seen, corner_low, corner_high)

    sub_final, cat_final = call(
        place_kernel,
        1 << 22,
        2,
        name="place",
        out_shape=(f32(depth, rows, columns), f32(depth, rows, columns)),
        in_specs=[VMEM, VMEM, VMEM, HBM, HBM],
        out_specs=(HBM, HBM),
        input_output_aliases={3: 0, 4: 1},
        scratch_shapes=[pltpu.SemaphoreType.DMA((16,))],
    )(ring_planes, inner_rows, outer_rows, sub_part, cat_part)

    image = call(
        shade_kernel,
        1 << 20,
        4,
        name="shade",
        out_shape=f32(4, rows, wide),
        in_specs=[VMEM] * (1 + 2 * count),
        out_specs=VMEM,
        scratch_shapes=[pltpu.VMEM((count, 3, rows, wide), jnp.float32)],
    )(values, *inner_pieces, *outer_pieces)
    return sub_final, cat_final, image


def solution(mesh):
    placed = (P("gz", "gx", None), P("gz", "gx", None), P(), P())

    return jax.shard_map(
        body,
        mesh=mesh,
        in_specs=placed,
        out_specs=(P("gz", "gx", None), P("gz", "gx", None), P(None, "gx", "gz")),
        check_vma=False,
    )
```

```python
import functools

import jax
import jax.numpy as jnp
from jax import lax
from jax.experimental import pallas as pl
from jax.experimental.pallas import tpu as pltpu
from jax.sharding import PartitionSpec as P


RATES = (0.16, 0.08)
FEED = 0.037
KILL = 0.06
OPTICAL = 4.0
ROWS, LANES = 8, 128

HBM = pl.BlockSpec(memory_space=pltpu.HBM)
VMEM = pl.BlockSpec(memory_space=pltpu.VMEM)
SMEM = pl.BlockSpec(memory_space=pltpu.SMEM)


def f32(*shape):
    return jax.ShapeDtypeStruct(shape, jnp.float32)


def hbm(x):
    return pltpu.with_memory_space_constraint(x, pltpu.HBM)


def lanes(x):
    return pltpu.roll(x, 1, axis=x.ndim - 1) + pltpu.roll(x, x.shape[-1] - 1, axis=x.ndim - 1)


def react(sub, cat, around_sub, around_cat):
    growth = sub * cat * cat
    sub_new = (1.0 - 6.0 * RATES[0] - FEED) * sub + RATES[0] * around_sub - growth + FEED
    cat_new = (1.0 - 6.0 * RATES[1] - FEED - KILL) * cat + RATES[1] * around_cat + growth
    return sub_new, cat_new


def plane_step(load, tiles, low_rows, high_rows, across, store, only=None):
    for tile in range(tiles) if only is None else only:
        sums, olds = [], []
        for s in range(2):
            old = load(s, tile)
            index = lax.broadcasted_iota(jnp.int32, old.shape, 0)
            above = load(s, tile - 1)[ROWS - 1 :] if tile else low_rows and low_rows[s]
            below = load(s, tile + 1)[:1] if tile < tiles - 1 else high_rows and high_rows[s]
            above = 0.0 if above is None else jnp.broadcast_to(above, old.shape)
            below = 0.0 if below is None else jnp.broadcast_to(below, old.shape)
            up = jnp.where(index == 0, above, pltpu.roll(old, 1, axis=0))
            down = jnp.where(index == ROWS - 1, below, pltpu.roll(old, ROWS - 1, axis=0))
            sums.append(lanes(old) + (up + down) + across(s, tile))
            olds.append(old)
        store(tile, *react(olds[0], olds[1], sums[0], sums[1]))


def span(tile):
    return pl.ds(tile * ROWS, ROWS)


def across_columns(tile, columns):
    return tile[:, :columns] if columns <= LANES else jnp.concatenate([tile] * (columns // LANES), axis=1)


def outer_step(outer, inner, rows, only, store):
    plane_step(
        lambda s, tile: outer[s, span(tile), :],
        rows // ROWS,
        None,
        None,
        lambda s, tile: inner[s, span(tile), :],
        store,
        only,
    )


def planes_kernel(sub, cat, up, down, second, penult, sems):
    depth, rows, _ = sub.shape
    copies = []
    for s, field in enumerate((sub, cat)):
        for plane, out in (
            (depth - 1, up.at[s, pl.ds(0, rows)]),
            (depth - 2, penult.at[s]),
            (0, down.at[s, pl.ds(0, rows)]),
            (1, second.at[s]),
        ):
            copies.append(pltpu.make_async_copy(field.at[plane], out, sems.at[len(copies)]))
    for copy in copies:
        copy.start()
    for copy in copies:
        copy.wait()
    for outer, inner in ((up, penult), (down, second)):

        def store(tile, sub_new, cat_new, outer=outer):
            at = pl.ds(rows + (tile - 1) * ROWS, ROWS)
            outer[0, at, :] = sub_new
            outer[1, at, :] = cat_new

        outer_step(outer, inner, rows, range(1, rows // ROWS - 1), store)


def prepare_kernel(sub, cat, up, down, second, penult, old, low, high, q_up, q_down, sems):
    depth, rows, _ = sub.shape
    copies = []
    for plane in range(depth):
        for s, field in enumerate((sub, cat)):
            copies.append(pltpu.make_async_copy(field.at[plane], old.at[s, plane], sems.at[s, plane]))
    for copy in copies:
        copy.start()
    for outer, inner, out in ((up, penult, q_up), (down, second, q_down)):

        def store(tile, sub_new, cat_new, out=out):
            at = span(0 if tile == 0 else 1)
            out[0, at, :] = sub_new
            out[1, at, :] = cat_new

        outer_step(outer, inner, rows, (0, rows // ROWS - 1), store)
    for plane in range(depth):
        for s in range(2):
            copies[2 * plane + s].wait()
            for row in range(2):
                low[s, row, plane : plane + 1] = old[s, plane, row : row + 1]
                high[s, row, plane : plane + 1] = old[s, plane, rows - 2 + row : rows - 1 + row]


def composite(sub, cat, scale_sub, scale_cat, clear):
    keep = jnp.exp(-(scale_sub * sub + scale_cat * cat))
    weight = clear * (1.0 - keep)
    return weight * sub, weight * cat, clear * keep


def scalars_kernel(share, scale, emission, values):
    shape = values.shape[1:]
    for s in range(2):
        values[s] = jnp.full(shape, scale[s] * share, jnp.float32)
        for channel in range(3):
            values[2 + channel * 2 + s] = jnp.full(shape, emission[s, channel], jnp.float32)


def first_kernel(old, mid):
    depth, rows, _ = old.shape[1:]

    @pl.loop(1, depth - 1)
    def _(k):
        def store(tile, sub, cat):
            mid[0, k, span(tile), :] = sub
            mid[1, k, span(tile), :] = cat

        plane_step(
            lambda s, tile: old[s, k, span(tile), :],
            rows // ROWS,
            None,
            None,
            lambda s, tile: old[s, k - 1, span(tile), :] + old[s, k + 1, span(tile), :],
            store,
        )


def second_kernel(
    values, mid, up, down, q_up, q_down, from_low, from_high, own_low, own_high,
    sub_out, cat_out, seen, near, far, rows_low, rows_high,
    heads, tails, new, sem_out,
):
    depth, rows, columns = sub_out.shape
    outputs = (sub_out, cat_out)
    tiles = rows // ROWS
    scale_sub, scale_cat = across_columns(values[0], columns), across_columns(values[1], columns)

    def put(s, k):
        return pltpu.make_async_copy(new.at[s, k], outputs[s].at[k], sem_out.at[s, k])

    which = lax.broadcasted_iota(jnp.int32, (depth, columns), 0)
    for got, at, own, at_own, out in (
        (from_low, 1, own_low, 0, rows_low),
        (from_high, 0, own_high, 1, rows_high),
    ):
        sums, olds = [], []
        for s in range(2):
            here = got[s, at]
            ahead = jnp.where(which == 0, 0.0, pltpu.roll(here, 1, axis=0))
            behind = jnp.where(which == depth - 1, 0.0, pltpu.roll(here, depth - 1, axis=0))
            sums.append(lanes(here) + (got[s, 1 - at] + own[s, at_own]) + (ahead + behind))
            olds.append(here)
        sub, cat = react(olds[0], olds[1], sums[0], sums[1])
        out[0] = sub
        out[1] = cat

    index = lax.broadcasted_iota(jnp.int32, (ROWS, columns), 0)

    def with_low(s, k, tile):
        row = jnp.broadcast_to(from_low[s, 1, pl.ds(k, 1)], tile.shape)
        return tile + jnp.where(index == 0, RATES[s] * row, 0.0)

    def with_high(s, k, tile):
        row = jnp.broadcast_to(from_high[s, 0, pl.ds(k, 1)], tile.shape)
        return tile + jnp.where(index == ROWS - 1, RATES[s] * row, 0.0)

    @pl.loop(1, depth - 1)
    def _(k):
        for s in range(2):
            heads[s, k] = with_low(s, k, mid[s, k, span(0), :])
            tails[s, k] = with_high(s, k, mid[s, k, span(tiles - 1), :])

    def load(s, k, tile):
        if tile == 0:
            return heads[s, k]
        if tile == tiles - 1:
            return tails[s, k]
        return mid[s, k, span(tile), :]

    for s in range(2):
        for tile in range(tiles):
            if 0 < tile < tiles - 1:
                at = pl.ds(rows + (tile - 1) * ROWS, ROWS)
                first, last = down[s, at, :], up[s, at, :]
            else:
                first, last = q_down[s, span(1 if tile else 0), :], q_up[s, span(1 if tile else 0), :]
            if tile == 0:
                first, last = with_low(s, 0, first), with_low(s, depth - 1, last)
            if tile == tiles - 1:
                first, last = with_high(s, 0, first), with_high(s, depth - 1, last)
            near[s, 0, span(tile), :] = first
            far[s, 2, span(tile), :] = last
            for j in range(2):
                near[s, 1 + j, span(tile), :] = load(s, 1 + j, tile)
                far[s, j, span(tile), :] = load(s, depth - 3 + j, tile)

    seen[0] = jnp.zeros((rows, columns), jnp.float32)
    seen[1] = jnp.zeros((rows, columns), jnp.float32)
    seen[2] = jnp.ones((rows, columns), jnp.float32)

    @pl.loop(2, depth - 2)
    def _(k):
        def store(tile, sub, cat):
            at = span(tile)
            new[0, k, at, :] = sub
            new[1, k, at, :] = cat
            one, two, clear = composite(sub, cat, scale_sub, scale_cat, seen[2, at, :])
            seen[0, at, :] += one
            seen[1, at, :] += two
            seen[2, at, :] = clear

        plane_step(
            lambda s, tile: load(s, k, tile),
            tiles,
            [rows_low[s, pl.ds(k, 1)] for s in range(2)],
            [rows_high[s, pl.ds(k, 1)] for s in range(2)],
            lambda s, tile: load(s, k - 1, tile) + load(s, k + 1, tile),
            store,
        )
        for s in range(2):
            put(s, k).start()

    @pl.loop(2, depth - 2)
    def _(k):
        for s in range(2):
            put(s, k).wait()


def rows_kernel(q_up, q_down, from_low, from_high, up, down):
    depth = from_low.shape[2]
    for plane, q, out in ((depth - 1, q_up, up), (0, q_down, down)):
        for place, edge, source in ((0, 0, from_low.at[:, 1]), (1, ROWS - 1, from_high.at[:, 0])):
            for s in range(2):
                tile = q[s, span(place), :]
                index = lax.broadcasted_iota(jnp.int32, tile.shape, 0)
                row = jnp.broadcast_to(source[s, plane : plane + 1], tile.shape)
                out[s, span(place), :] = tile + jnp.where(index == edge, (2.0 * RATES[s]) * row, 0.0)


def rim_kernel(
    values, p_low, p_high, down, up, near, far, rows_low, rows_high, inner,
    ring, known, seen, mid,
):
    depth = rows_low.shape[1]
    rows, columns = inner.shape[1:]
    tiles = rows // ROWS
    scale_sub, scale_cat = across_columns(values[0], columns), across_columns(values[1], columns)
    for side, p, own, inside in ((0, p_low, down, near), (1, p_high, up, far)):
        zero, one, two = (0, 1, 2) if side == 0 else (2, 1, 0)
        outer, beside = (0, 1) if side == 0 else (depth - 1, depth - 2)
        for s in range(2):
            mid[side, s] = inside[s, zero] + RATES[s] * p[s, :rows]

        def store_known(tile, sub, cat, side=side, own=own):
            at = span(tile)
            known[side, 0, at, :] = sub + (RATES[0] * RATES[0]) * own[0, at, :]
            known[side, 1, at, :] = cat + (RATES[1] * RATES[1]) * own[1, at, :]

        plane_step(
            lambda s, tile, side=side: mid[side, s, span(tile), :],
            tiles,
            [rows_low[s, outer : outer + 1] for s in range(2)],
            [rows_high[s, outer : outer + 1] for s in range(2)],
            lambda s, tile, inside=inside, one=one: inside[s, one, span(tile), :],
            store_known,
        )

        def store_ring(tile, sub, cat, side=side):
            ring[0, side, span(tile), :] = sub
            ring[1, side, span(tile), :] = cat

        plane_step(
            lambda s, tile, inside=inside, one=one: inside[s, one, span(tile), :],
            tiles,
            [rows_low[s, beside : beside + 1] for s in range(2)],
            [rows_high[s, beside : beside + 1] for s in range(2)],
            lambda s, tile, inside=inside, two=two, side=side: inside[s, two, span(tile), :]
            + mid[side, s, span(tile), :],
            store_ring,
        )

    for tile in range(tiles):
        at = span(tile)
        one, two, clear = composite(ring[0, 0, at, :], ring[1, 0, at, :], scale_sub, scale_cat, 1.0)
        sub = one + clear * inner[0, at, :]
        cat = two + clear * inner[1, at, :]
        clear = clear * inner[2, at, :]
        one, two, clear = composite(ring[0, 1, at, :], ring[1, 1, at, :], scale_sub, scale_cat, clear)
        seen[0, at, :] = sub + one
        seen[1, at, :] = cat + two
        seen[2, at, :] = clear


def last_kernel(outermost, values, known, q_low, q_high, seen, *rest):
    *pieces, outer, whole = rest
    rows, columns = seen.shape[1:]
    count = len(pieces)
    wide = columns // count
    tiles = rows // ROWS
    scale_sub, scale_cat = across_columns(values[0], columns), across_columns(values[1], columns)
    for place, tile in enumerate((0, tiles - 1) if outermost else range(1, tiles - 1)):
        at, to = span(tile), span(place)
        source = to if outermost else pl.ds(rows + place * ROWS, ROWS)
        planes = []
        for side, q in enumerate((q_low, q_high)):
            for s in range(2):
                value = known[side, s, at, :] + RATES[s] * q[s, source, :]
                outer[s, side, to, :] = value
                planes.append(value)
        one, two, clear = composite(planes[0], planes[1], scale_sub, scale_cat, 1.0)
        sub = one + clear * seen[0, at, :]
        cat = two + clear * seen[1, at, :]
        clear = clear * seen[2, at, :]
        one, two, clear = composite(planes[2], planes[3], scale_sub, scale_cat, clear)
        whole[0, to, :] = sub + one
        whole[1, to, :] = cat + two
        whole[2, to, :] = clear
    me = lax.axis_index("gz")
    for shift, piece in enumerate(pieces):
        target = lax.rem(me + shift, count)
        if wide % LANES == 0:
            piece[...] = whole[:, :, pl.ds(pl.multiple_of(target * wide, LANES), wide)]
        else:
            for other in range(count):

                @pl.when(target == other)
                def _(piece=piece, other=other):
                    piece[...] = whole[:, :, other * wide : (other + 1) * wide]


def shade_kernel(values, *pieces_and_rest):
    *pieces, image, slabs = pieces_and_rest
    count = len(pieces) // 2
    rows, wide = image.shape[1:]
    me = lax.axis_index("gz")
    for shift in range(count):
        slab = lax.rem(me + count - shift, count)
        inner, outer = pieces[shift], pieces[count + shift]
        slabs[slab, :, pl.ds(ROWS, rows - 2 * ROWS), :] = inner[...]
        slabs[slab, :, pl.ds(0, ROWS), :] = outer[:, :ROWS]
        slabs[slab, :, pl.ds(rows - ROWS, ROWS), :] = outer[:, ROWS:]
    for tile in range(rows // ROWS):
        at = span(tile)
        sub, cat, clear = slabs[0, 0, at, :], slabs[0, 1, at, :], slabs[0, 2, at, :]
        for slab in range(1, count):
            sub = sub + clear * slabs[slab, 0, at, :]
            cat = cat + clear * slabs[slab, 1, at, :]
            clear = clear * slabs[slab, 2, at, :]
        for channel in range(3):
            of_sub = across_columns(values[2 + channel * 2], wide)
            of_cat = across_columns(values[3 + channel * 2], wide)
            image[channel, at, :] = of_sub * sub + of_cat * cat
        image[3, at, :] = 1.0 - clear


def place_kernel(ring, inner, outer, sub_in, cat_in, sub_out, cat_out, sems):
    del sub_in, cat_in
    depth, rows, _ = sub_out.shape
    copies = []
    for s, out in enumerate((sub_out, cat_out)):
        for side in range(2):
            plane = side * (depth - 1)
            for source, target in (
                (ring.at[s, side], out.at[1 + side * (depth - 3)]),
                (inner.at[s, side], out.at[plane, pl.ds(ROWS, rows - 2 * ROWS)]),
                (outer.at[s, side, pl.ds(0, ROWS)], out.at[plane, pl.ds(0, ROWS)]),
                (outer.at[s, side, pl.ds(ROWS, ROWS)], out.at[plane, pl.ds(rows - ROWS, ROWS)]),
            ):
                copies.append(pltpu.make_async_copy(source, target, sems.at[len(copies)]))
    for copy in copies:
        copy.start()
    for copy in copies:
        copy.wait()


def call(kernel, flops, room, **kwargs):
    return pl.pallas_call(
        kernel,
        cost_estimate=pl.CostEstimate(flops=flops, bytes_accessed=1 << 16, transcendentals=0),
        compiler_params=pltpu.CompilerParams(vmem_limit_bytes=room << 20),
        **kwargs,
    )


def body(substrate, catalyst, extinction, emission):
    depth, rows, columns = substrate.shape
    count = lax.axis_size("gz")
    wide = columns // count
    share = OPTICAL / (depth * count)
    middle = rows - 2 * ROWS
    outers = 2 * ROWS

    def ring(size, shift):
        return [(i, (i + shift) % size) for i in range(size)]

    def shifted(x, axis, shift):
        return lax.ppermute(x, axis, ring(lax.axis_size(axis), shift))

    up, down, second, penult = call(
        planes_kernel,
        1 << 20,
        2,
        name="planes",
        out_shape=(f32(2, rows + middle, columns),) * 2 + (f32(2, rows, columns),) * 2,
        in_specs=[HBM, HBM],
        out_specs=(VMEM,) * 4,
        scratch_shapes=[pltpu.SemaphoreType.DMA((8,))],
    )(hbm(substrate), hbm(catalyst))
    p_low = shifted(up, "gz", 1)
    p_high = shifted(down, "gz", -1)

    old, own_low, own_high, q_up, q_down = call(
        prepare_kernel,
        1 << 22,
        2,
        name="prepare",
        out_shape=(
            f32(2, depth, rows, columns),
            f32(2, 2, depth, columns),
            f32(2, 2, depth, columns),
            f32(2, outers, columns),
            f32(2, outers, columns),
        ),
        in_specs=[HBM, HBM, VMEM, VMEM, VMEM, VMEM],
        out_specs=(VMEM,) * 5,
        scratch_shapes=[pltpu.SemaphoreType.DMA((2, depth))],
    )(hbm(substrate), hbm(catalyst), up, down, second, penult)
    from_low = shifted(own_high, "gx", 1)
    from_high = shifted(own_low, "gx", -1)

    mid = call(
        first_kernel,
        1 << 24,
        2,
        name="first",
        out_shape=f32(2, depth, rows, columns),
        in_specs=[VMEM],
        out_specs=VMEM,
    )(old)
    values = call(
        functools.partial(scalars_kernel, share),
        1 << 18,
        2,
        name="scalars",
        out_shape=f32(8, ROWS, LANES),
        in_specs=[SMEM, SMEM],
        out_specs=VMEM,
    )(extinction, emission.T)

    m_up, m_down = call(
        rows_kernel,
        1 << 18,
        2,
        name="rows",
        out_shape=(f32(2, outers, columns),) * 2,
        in_specs=[VMEM] * 4,
        out_specs=(VMEM,) * 2,
    )(q_up, q_down, from_low, from_high)
    q_low = shifted(m_up, "gz", 1)
    q_high = shifted(m_down, "gz", -1)

    sub_part, cat_part, inner, near, far, rows_low, rows_high = call(
        second_kernel,
        1 << 25,
        10,
        name="second",
        out_shape=(
            f32(depth, rows, columns),
            f32(depth, rows, columns),
            f32(3, rows, columns),
            f32(2, 3, rows, columns),
            f32(2, 3, rows, columns),
            f32(2, depth, columns),
            f32(2, depth, columns),
        ),
        in_specs=[VMEM] * 10,
        out_specs=(HBM, HBM) + (VMEM,) * 5,
        scratch_shapes=[
            pltpu.VMEM((2, depth, ROWS, columns), jnp.float32),
            pltpu.VMEM((2, depth, ROWS, columns), jnp.float32),
            pltpu.VMEM((2, depth, rows, columns), jnp.float32),
            pltpu.SemaphoreType.DMA((2, depth)),
        ],
    )(values, mid, up, down, q_up, q_down, from_low, from_high, own_low, own_high)

    p_low, p_high, inner = lax.optimization_barrier((p_low, p_high, inner))
    ring_planes, known, seen = call(
        rim_kernel,
        1 << 23,
        4,
        name="rim",
        out_shape=(f32(2, 2, rows, columns), f32(2, 2, rows, columns), f32(3, rows, columns)),
        in_specs=[VMEM] * 10,
        out_specs=(VMEM,) * 3,
        scratch_shapes=[pltpu.VMEM((2, 2, rows, columns), jnp.float32)],
    )(values, p_low, p_high, down, up, near, far, rows_low, rows_high, inner)

    def finish(outermost, high, *args):
        *pieces, outer = call(
            functools.partial(last_kernel, outermost),
            1 << 22,
            4,
            name="last" if outermost else "most",
            out_shape=(f32(3, high, wide),) * count + (f32(2, 2, high, columns),),
            in_specs=[VMEM] * len(args),
            out_specs=(VMEM,) * (count + 1),
            scratch_shapes=[pltpu.VMEM((3, high, columns), jnp.float32)],
        )(*args)
        received = [pieces[0]]
        for shift in range(1, count):
            received.append(shifted(pieces[shift], "gz", shift))
        return received, outer

    inner_pieces, inner_rows = finish(False, middle, values, known, p_low, p_high, seen)

    outer_pieces, outer_rows = finish(True, outers, values, known, q_low, q_high, seen)

    sub_final, cat_final = call(
        place_kernel,
        1 << 22,
        2,
        name="place",
        out_shape=(f32(depth, rows, columns), f32(depth, rows, columns)),
        in_specs=[VMEM, VMEM, VMEM, HBM, HBM],
        out_specs=(HBM, HBM),
        input_output_aliases={3: 0, 4: 1},
        scratch_shapes=[pltpu.SemaphoreType.DMA((16,))],
    )(ring_planes, inner_rows, outer_rows, sub_part, cat_part)

    image = call(
        shade_kernel,
        1 << 20,
        4,
        name="shade",
        out_shape=f32(4, rows, wide),
        in_specs=[VMEM] * (1 + 2 * count),
        out_specs=VMEM,
        scratch_shapes=[pltpu.VMEM((count, 3, rows, wide), jnp.float32)],
    )(values, *inner_pieces, *outer_pieces)
    return sub_final, cat_final, image


def solution(mesh):
    placed = (P("gz", "gx", None), P("gz", "gx", None), P(), P())

    return jax.shard_map(
        body,
        mesh=mesh,
        in_specs=placed,
        out_specs=(P("gz", "gx", None), P("gz", "gx", None), P(None, "gx", "gz")),
        check_vma=False,
    )
```

```python
import functools

import jax
import jax.numpy as jnp
from jax import lax
from jax.experimental import pallas as pl
from jax.experimental.pallas import tpu as pltpu
from jax.sharding import PartitionSpec as P


RATES = (0.16, 0.08)
FEED = 0.037
KILL = 0.06
OPTICAL = 4.0
ROWS, LANES = 8, 128

HBM = pl.BlockSpec(memory_space=pltpu.HBM)
VMEM = pl.BlockSpec(memory_space=pltpu.VMEM)
SMEM = pl.BlockSpec(memory_space=pltpu.SMEM)


def f32(*shape):
    return jax.ShapeDtypeStruct(shape, jnp.float32)


def hbm(x):
    return pltpu.with_memory_space_constraint(x, pltpu.HBM)


def lanes(x):
    return pltpu.roll(x, 1, axis=x.ndim - 1) + pltpu.roll(x, x.shape[-1] - 1, axis=x.ndim - 1)


def react(sub, cat, around_sub, around_cat):
    growth = sub * cat * cat
    sub_new = (1.0 - 6.0 * RATES[0] - FEED) * sub + RATES[0] * around_sub - growth + FEED
    cat_new = (1.0 - 6.0 * RATES[1] - FEED - KILL) * cat + RATES[1] * around_cat + growth
    return sub_new, cat_new


def plane_step(load, tiles, low_rows, high_rows, across, store, only=None):
    for tile in range(tiles) if only is None else only:
        sums, olds = [], []
        for s in range(2):
            old = load(s, tile)
            index = lax.broadcasted_iota(jnp.int32, old.shape, 0)
            above = load(s, tile - 1)[ROWS - 1 :] if tile else low_rows and low_rows[s]
            below = load(s, tile + 1)[:1] if tile < tiles - 1 else high_rows and high_rows[s]
            above = 0.0 if above is None else jnp.broadcast_to(above, old.shape)
            below = 0.0 if below is None else jnp.broadcast_to(below, old.shape)
            up = jnp.where(index == 0, above, pltpu.roll(old, 1, axis=0))
            down = jnp.where(index == ROWS - 1, below, pltpu.roll(old, ROWS - 1, axis=0))
            sums.append(lanes(old) + (up + down) + across(s, tile))
            olds.append(old)
        store(tile, *react(olds[0], olds[1], sums[0], sums[1]))


def span(tile):
    return pl.ds(tile * ROWS, ROWS)


def across_columns(tile, columns):
    return tile[:, :columns] if columns <= LANES else jnp.concatenate([tile] * (columns // LANES), axis=1)


def outer_step(outer, inner, rows, only, store):
    plane_step(
        lambda s, tile: outer[s, span(tile), :],
        rows // ROWS,
        None,
        None,
        lambda s, tile: inner[s, span(tile), :],
        store,
        only,
    )


def planes_kernel(sub, cat, up, down, second, penult, sems):
    depth, rows, _ = sub.shape
    copies = []
    for s, field in enumerate((sub, cat)):
        for plane, out in (
            (depth - 1, up.at[s, pl.ds(0, rows)]),
            (depth - 2, penult.at[s]),
            (0, down.at[s, pl.ds(0, rows)]),
            (1, second.at[s]),
        ):
            copies.append(pltpu.make_async_copy(field.at[plane], out, sems.at[len(copies)]))
    for copy in copies:
        copy.start()
    for copy in copies:
        copy.wait()
    for outer, inner in ((up, penult), (down, second)):

        def store(tile, sub_new, cat_new, outer=outer):
            at = pl.ds(rows + (tile - 1) * ROWS, ROWS)
            outer[0, at, :] = sub_new
            outer[1, at, :] = cat_new

        outer_step(outer, inner, rows, range(1, rows // ROWS - 1), store)


def prepare_kernel(sub, cat, up, down, second, penult, low, high, q_up, q_down):
    depth, rows, _ = sub.shape
    for s, field in enumerate((sub, cat)):
        for plane in range(depth):
            for row in range(2):
                low[s, row, plane : plane + 1] = field[plane, row : row + 1]
                high[s, row, plane : plane + 1] = field[plane, rows - 2 + row : rows - 1 + row]
    for outer, inner, out in ((up, penult, q_up), (down, second, q_down)):

        def store(tile, sub_new, cat_new, out=out):
            at = span(0 if tile == 0 else 1)
            out[0, at, :] = sub_new
            out[1, at, :] = cat_new

        outer_step(outer, inner, rows, (0, rows // ROWS - 1), store)


def composite(sub, cat, scale_sub, scale_cat, clear):
    keep = jnp.exp(-(scale_sub * sub + scale_cat * cat))
    weight = clear * (1.0 - keep)
    return weight * sub, weight * cat, clear * keep


def scalars_kernel(share, scale, emission, values):
    shape = values.shape[1:]
    for s in range(2):
        values[s] = jnp.full(shape, scale[s] * share, jnp.float32)
        for channel in range(3):
            values[2 + channel * 2 + s] = jnp.full(shape, emission[s, channel], jnp.float32)


def first_kernel(sub, cat, mid):
    depth, rows, _ = sub.shape
    old = (sub, cat)

    @pl.loop(1, depth - 1)
    def _(k):
        def store(tile, sub_new, cat_new):
            mid[0, k, span(tile), :] = sub_new
            mid[1, k, span(tile), :] = cat_new

        plane_step(
            lambda s, tile: old[s][k, span(tile), :],
            rows // ROWS,
            None,
            None,
            lambda s, tile: old[s][k - 1, span(tile), :] + old[s][k + 1, span(tile), :],
            store,
        )


def image_step(k, load, tiles, only, low_rows, high_rows, scales, seen, keep):
    def store(tile, sub, cat):
        at = span(tile)
        keep(tile, sub, cat)
        one, two, clear = composite(sub, cat, *scales, seen[2, at, :])
        seen[0, at, :] += one
        seen[1, at, :] += two
        seen[2, at, :] = clear

    plane_step(
        lambda s, tile: load(s, k, tile),
        tiles,
        low_rows,
        high_rows,
        lambda s, tile: load(s, k - 1, tile) + load(s, k + 1, tile),
        store,
        only,
    )


def clear_image(seen):
    seen[0] = jnp.zeros(seen.shape[1:], jnp.float32)
    seen[1] = jnp.zeros(seen.shape[1:], jnp.float32)
    seen[2] = jnp.ones(seen.shape[1:], jnp.float32)


def center_kernel(values, mid, sub_out, cat_out, seen, new, sem_out):
    depth, rows, columns = sub_out.shape
    outputs = (sub_out, cat_out)
    tiles = rows // ROWS
    scales = across_columns(values[0], columns), across_columns(values[1], columns)
    inside = pl.ds(ROWS, rows - 2 * ROWS)

    def put(s, k):
        return pltpu.make_async_copy(new.at[s, k], outputs[s].at[k, inside], sem_out.at[s, k])

    clear_image(seen)

    @pl.loop(2, depth - 2)
    def _(k):
        def keep(tile, sub, cat):
            new[0, k, span(tile - 1), :] = sub
            new[1, k, span(tile - 1), :] = cat

        image_step(
            k, lambda s, k, tile: mid[s, k, span(tile), :], tiles, range(1, tiles - 1), None, None, scales, seen, keep
        )
        for s in range(2):
            put(s, k).start()

    @pl.loop(2, depth - 2)
    def _(k):
        for s in range(2):
            put(s, k).wait()


def second_kernel(
    values, mid, up, down, q_up, q_down, from_low, from_high, own_low, own_high, center, sub_in, cat_in,
    sub_out, cat_out, seen, near, far, rows_low, rows_high,
    heads, tails, new, sem_out,
):
    del sub_in, cat_in
    depth, rows, columns = sub_out.shape
    outputs = (sub_out, cat_out)
    tiles = rows // ROWS
    scales = across_columns(values[0], columns), across_columns(values[1], columns)

    def put(s, k, end):
        at = pl.ds(end * (rows - ROWS), ROWS)
        return pltpu.make_async_copy(new.at[s, end, k], outputs[s].at[k, at], sem_out.at[s, end, k])

    which = lax.broadcasted_iota(jnp.int32, (depth, columns), 0)
    for got, at, own, at_own, out in (
        (from_low, 1, own_low, 0, rows_low),
        (from_high, 0, own_high, 1, rows_high),
    ):
        sums, olds = [], []
        for s in range(2):
            here = got[s, at]
            ahead = jnp.where(which == 0, 0.0, pltpu.roll(here, 1, axis=0))
            behind = jnp.where(which == depth - 1, 0.0, pltpu.roll(here, depth - 1, axis=0))
            sums.append(lanes(here) + (got[s, 1 - at] + own[s, at_own]) + (ahead + behind))
            olds.append(here)
        sub, cat = react(olds[0], olds[1], sums[0], sums[1])
        out[0] = sub
        out[1] = cat

    index = lax.broadcasted_iota(jnp.int32, (ROWS, columns), 0)

    def with_low(s, k, tile):
        row = jnp.broadcast_to(from_low[s, 1, pl.ds(k, 1)], tile.shape)
        return tile + jnp.where(index == 0, RATES[s] * row, 0.0)

    def with_high(s, k, tile):
        row = jnp.broadcast_to(from_high[s, 0, pl.ds(k, 1)], tile.shape)
        return tile + jnp.where(index == ROWS - 1, RATES[s] * row, 0.0)

    @pl.loop(1, depth - 1)
    def _(k):
        for s in range(2):
            heads[s, k] = with_low(s, k, mid[s, k, span(0), :])
            tails[s, k] = with_high(s, k, mid[s, k, span(tiles - 1), :])

    def load(s, k, tile):
        if tile == 0:
            return heads[s, k]
        if tile == tiles - 1:
            return tails[s, k]
        return mid[s, k, span(tile), :]

    for s in range(2):
        for tile in range(tiles):
            if 0 < tile < tiles - 1:
                at = pl.ds(rows + (tile - 1) * ROWS, ROWS)
                first, last = down[s, at, :], up[s, at, :]
            else:
                first, last = q_down[s, span(1 if tile else 0), :], q_up[s, span(1 if tile else 0), :]
            if tile == 0:
                first, last = with_low(s, 0, first), with_low(s, depth - 1, last)
            if tile == tiles - 1:
                first, last = with_high(s, 0, first), with_high(s, depth - 1, last)
            near[s, 0, span(tile), :] = first
            far[s, 2, span(tile), :] = last
            for j in range(2):
                near[s, 1 + j, span(tile), :] = load(s, 1 + j, tile)
                far[s, j, span(tile), :] = load(s, depth - 3 + j, tile)

    clear_image(seen)
    for tile in range(1, tiles - 1):
        for part in range(3):
            seen[part, span(tile), :] = center[part, span(tile), :]

    @pl.loop(2, depth - 2)
    def _(k):
        def keep(tile, sub, cat):
            new[0, 1 if tile else 0, k] = sub
            new[1, 1 if tile else 0, k] = cat

        image_step(
            k,
            load,
            tiles,
            (0, tiles - 1),
            [rows_low[s, pl.ds(k, 1)] for s in range(2)],
            [rows_high[s, pl.ds(k, 1)] for s in range(2)],
            scales,
            seen,
            keep,
        )
        for s in range(2):
            for end in range(2):
                put(s, k, end).start()

    @pl.loop(2, depth - 2)
    def _(k):
        for s in range(2):
            for end in range(2):
                put(s, k, end).wait()


def rows_kernel(q_up, q_down, from_low, from_high, up, down):
    depth = from_low.shape[2]
    for plane, q, out in ((depth - 1, q_up, up), (0, q_down, down)):
        for place, edge, source in ((0, 0, from_low.at[:, 1]), (1, ROWS - 1, from_high.at[:, 0])):
            for s in range(2):
                tile = q[s, span(place), :]
                index = lax.broadcasted_iota(jnp.int32, tile.shape, 0)
                row = jnp.broadcast_to(source[s, plane : plane + 1], tile.shape)
                out[s, span(place), :] = tile + jnp.where(index == edge, (2.0 * RATES[s]) * row, 0.0)


def rim_kernel(
    values, p_low, p_high, down, up, near, far, rows_low, rows_high, inner,
    ring, known, seen, mid,
):
    depth = rows_low.shape[1]
    rows, columns = inner.shape[1:]
    tiles = rows // ROWS
    scale_sub, scale_cat = across_columns(values[0], columns), across_columns(values[1], columns)
    for side, p, own, inside in ((0, p_low, down, near), (1, p_high, up, far)):
        zero, one, two = (0, 1, 2) if side == 0 else (2, 1, 0)
        outer, beside = (0, 1) if side == 0 else (depth - 1, depth - 2)
        for s in range(2):
            mid[side, s] = inside[s, zero] + RATES[s] * p[s, :rows]

        def store_known(tile, sub, cat, side=side, own=own):
            at = span(tile)
            known[side, 0, at, :] = sub + (RATES[0] * RATES[0]) * own[0, at, :]
            known[side, 1, at, :] = cat + (RATES[1] * RATES[1]) * own[1, at, :]

        plane_step(
            lambda s, tile, side=side: mid[side, s, span(tile), :],
            tiles,
            [rows_low[s, outer : outer + 1] for s in range(2)],
            [rows_high[s, outer : outer + 1] for s in range(2)],
            lambda s, tile, inside=inside, one=one: inside[s, one, span(tile), :],
            store_known,
        )

        def store_ring(tile, sub, cat, side=side):
            ring[0, side, span(tile), :] = sub
            ring[1, side, span(tile), :] = cat

        plane_step(
            lambda s, tile, inside=inside, one=one: inside[s, one, span(tile), :],
            tiles,
            [rows_low[s, beside : beside + 1] for s in range(2)],
            [rows_high[s, beside : beside + 1] for s in range(2)],
            lambda s, tile, inside=inside, two=two, side=side: inside[s, two, span(tile), :]
            + mid[side, s, span(tile), :],
            store_ring,
        )

    for tile in range(tiles):
        at = span(tile)
        one, two, clear = composite(ring[0, 0, at, :], ring[1, 0, at, :], scale_sub, scale_cat, 1.0)
        sub = one + clear * inner[0, at, :]
        cat = two + clear * inner[1, at, :]
        clear = clear * inner[2, at, :]
        one, two, clear = composite(ring[0, 1, at, :], ring[1, 1, at, :], scale_sub, scale_cat, clear)
        seen[0, at, :] = sub + one
        seen[1, at, :] = cat + two
        seen[2, at, :] = clear


def last_kernel(outermost, values, known, q_low, q_high, seen, *rest):
    *pieces, outer, whole = rest
    rows, columns = seen.shape[1:]
    count = len(pieces)
    wide = columns // count
    tiles = rows // ROWS
    scale_sub, scale_cat = across_columns(values[0], columns), across_columns(values[1], columns)
    for place, tile in enumerate((0, tiles - 1) if outermost else range(1, tiles - 1)):
        at, to = span(tile), span(place)
        source = to if outermost else pl.ds(rows + place * ROWS, ROWS)
        planes = []
        for side, q in enumerate((q_low, q_high)):
            for s in range(2):
                value = known[side, s, at, :] + RATES[s] * q[s, source, :]
                outer[s, side, to, :] = value
                planes.append(value)
        one, two, clear = composite(planes[0], planes[1], scale_sub, scale_cat, 1.0)
        sub = one + clear * seen[0, at, :]
        cat = two + clear * seen[1, at, :]
        clear = clear * seen[2, at, :]
        one, two, clear = composite(planes[2], planes[3], scale_sub, scale_cat, clear)
        whole[0, to, :] = sub + one
        whole[1, to, :] = cat + two
        whole[2, to, :] = clear
    me = lax.axis_index("gz")
    for shift, piece in enumerate(pieces):
        target = lax.rem(me + shift, count)
        if wide % LANES == 0:
            piece[...] = whole[:, :, pl.ds(pl.multiple_of(target * wide, LANES), wide)]
        else:
            for other in range(count):

                @pl.when(target == other)
                def _(piece=piece, other=other):
                    piece[...] = whole[:, :, other * wide : (other + 1) * wide]


def shade_kernel(values, *pieces_and_rest):
    *pieces, image, slabs = pieces_and_rest
    count = len(pieces) // 2
    rows, wide = image.shape[1:]
    me = lax.axis_index("gz")
    for shift in range(count):
        slab = lax.rem(me + count - shift, count)
        inner, outer = pieces[shift], pieces[count + shift]
        slabs[slab, :, pl.ds(ROWS, rows - 2 * ROWS), :] = inner[...]
        slabs[slab, :, pl.ds(0, ROWS), :] = outer[:, :ROWS]
        slabs[slab, :, pl.ds(rows - ROWS, ROWS), :] = outer[:, ROWS:]
    for tile in range(rows // ROWS):
        at = span(tile)
        sub, cat, clear = slabs[0, 0, at, :], slabs[0, 1, at, :], slabs[0, 2, at, :]
        for slab in range(1, count):
            sub = sub + clear * slabs[slab, 0, at, :]
            cat = cat + clear * slabs[slab, 1, at, :]
            clear = clear * slabs[slab, 2, at, :]
        for channel in range(3):
            of_sub = across_columns(values[2 + channel * 2], wide)
            of_cat = across_columns(values[3 + channel * 2], wide)
            image[channel, at, :] = of_sub * sub + of_cat * cat
        image[3, at, :] = 1.0 - clear


def place_kernel(ring, inner, outer, sub_in, cat_in, sub_out, cat_out, sems):
    del sub_in, cat_in
    depth, rows, _ = sub_out.shape
    copies = []
    for s, out in enumerate((sub_out, cat_out)):
        for side in range(2):
            plane = side * (depth - 1)
            for source, target in (
                (ring.at[s, side], out.at[1 + side * (depth - 3)]),
                (inner.at[s, side], out.at[plane, pl.ds(ROWS, rows - 2 * ROWS)]),
                (outer.at[s, side, pl.ds(0, ROWS)], out.at[plane, pl.ds(0, ROWS)]),
                (outer.at[s, side, pl.ds(ROWS, ROWS)], out.at[plane, pl.ds(rows - ROWS, ROWS)]),
            ):
                copies.append(pltpu.make_async_copy(source, target, sems.at[len(copies)]))
    for copy in copies:
        copy.start()
    for copy in copies:
        copy.wait()


def call(kernel, flops, room, **kwargs):
    return pl.pallas_call(
        kernel,
        cost_estimate=pl.CostEstimate(flops=flops, bytes_accessed=1 << 16, transcendentals=0),
        compiler_params=pltpu.CompilerParams(vmem_limit_bytes=room << 20),
        **kwargs,
    )


def body(substrate, catalyst, extinction, emission):
    depth, rows, columns = substrate.shape
    count = lax.axis_size("gz")
    wide = columns // count
    share = OPTICAL / (depth * count)
    middle = rows - 2 * ROWS
    outers = 2 * ROWS

    def ring(size, shift):
        return [(i, (i + shift) % size) for i in range(size)]

    def shifted(x, axis, shift):
        return lax.ppermute(x, axis, ring(lax.axis_size(axis), shift))

    up, down, second, penult = call(
        planes_kernel,
        1 << 20,
        2,
        name="planes",
        out_shape=(f32(2, rows + middle, columns),) * 2 + (f32(2, rows, columns),) * 2,
        in_specs=[HBM, HBM],
        out_specs=(VMEM,) * 4,
        scratch_shapes=[pltpu.SemaphoreType.DMA((8,))],
    )(hbm(substrate), hbm(catalyst))
    p_low = shifted(up, "gz", 1)
    p_high = shifted(down, "gz", -1)

    own_low, own_high, q_up, q_down = call(
        prepare_kernel,
        1 << 22,
        2,
        name="prepare",
        out_shape=(
            f32(2, 2, depth, columns),
            f32(2, 2, depth, columns),
            f32(2, outers, columns),
            f32(2, outers, columns),
        ),
        in_specs=[VMEM] * 6,
        out_specs=(VMEM,) * 4,
    )(substrate, catalyst, up, down, second, penult)
    from_low = shifted(own_high, "gx", 1)
    from_high = shifted(own_low, "gx", -1)

    mid = call(
        first_kernel,
        1 << 24,
        2,
        name="first",
        out_shape=f32(2, depth, rows, columns),
        in_specs=[VMEM, VMEM],
        out_specs=VMEM,
    )(substrate, catalyst)
    values = call(
        functools.partial(scalars_kernel, share),
        1 << 18,
        2,
        name="scalars",
        out_shape=f32(8, ROWS, LANES),
        in_specs=[SMEM, SMEM],
        out_specs=VMEM,
    )(extinction, emission.T)

    sub_part, cat_part, center = call(
        center_kernel,
        1 << 24,
        4,
        name="center",
        out_shape=(f32(depth, rows, columns), f32(depth, rows, columns), f32(3, rows, columns)),
        in_specs=[VMEM, VMEM],
        out_specs=(HBM, HBM, VMEM),
        scratch_shapes=[
            pltpu.VMEM((2, depth, middle, columns), jnp.float32),
            pltpu.SemaphoreType.DMA((2, depth)),
        ],
    )(values, mid)

    m_up, m_down = call(
        rows_kernel,
        1 << 18,
        2,
        name="rows",
        out_shape=(f32(2, outers, columns),) * 2,
        in_specs=[VMEM] * 4,
        out_specs=(VMEM,) * 2,
    )(q_up, q_down, from_low, from_high)
    q_low = shifted(m_up, "gz", 1)
    q_high = shifted(m_down, "gz", -1)

    sub_part, cat_part, inner, near, far, rows_low, rows_high = call(
        second_kernel,
        1 << 25,
        10,
        name="second",
        out_shape=(
            f32(depth, rows, columns),
            f32(depth, rows, columns),
            f32(3, rows, columns),
            f32(2, 3, rows, columns),
            f32(2, 3, rows, columns),
            f32(2, depth, columns),
            f32(2, depth, columns),
        ),
        in_specs=[VMEM] * 11 + [HBM, HBM],
        out_specs=(HBM, HBM) + (VMEM,) * 5,
        input_output_aliases={11: 0, 12: 1},
        scratch_shapes=[
            pltpu.VMEM((2, depth, ROWS, columns), jnp.float32),
            pltpu.VMEM((2, depth, ROWS, columns), jnp.float32),
            pltpu.VMEM((2, 2, depth, ROWS, columns), jnp.float32),
            pltpu.SemaphoreType.DMA((2, 2, depth)),
        ],
    )(values, mid, up, down, q_up, q_down, from_low, from_high, own_low, own_high, center, sub_part, cat_part)

    p_low, p_high, inner = lax.optimization_barrier((p_low, p_high, inner))
    ring_planes, known, seen = call(
        rim_kernel,
        1 << 23,
        4,
        name="rim",
        out_shape=(f32(2, 2, rows, columns), f32(2, 2, rows, columns), f32(3, rows, columns)),
        in_specs=[VMEM] * 10,
        out_specs=(VMEM,) * 3,
        scratch_shapes=[pltpu.VMEM((2, 2, rows, columns), jnp.float32)],
    )(values, p_low, p_high, down, up, near, far, rows_low, rows_high, inner)

    def finish(outermost, high, *args):
        *pieces, outer = call(
            functools.partial(last_kernel, outermost),
            1 << 22,
            4,
            name="last" if outermost else "most",
            out_shape=(f32(3, high, wide),) * count + (f32(2, 2, high, columns),),
            in_specs=[VMEM] * len(args),
            out_specs=(VMEM,) * (count + 1),
            scratch_shapes=[pltpu.VMEM((3, high, columns), jnp.float32)],
        )(*args)
        received = [pieces[0]]
        for shift in range(1, count):
            received.append(shifted(pieces[shift], "gz", shift))
        return received, outer

    inner_pieces, inner_rows = finish(False, middle, values, known, p_low, p_high, seen)

    outer_pieces, outer_rows = finish(True, outers, values, known, q_low, q_high, seen)

    sub_final, cat_final = call(
        place_kernel,
        1 << 22,
        2,
        name="place",
        out_shape=(f32(depth, rows, columns), f32(depth, rows, columns)),
        in_specs=[VMEM, VMEM, VMEM, HBM, HBM],
        out_specs=(HBM, HBM),
        input_output_aliases={3: 0, 4: 1},
        scratch_shapes=[pltpu.SemaphoreType.DMA((16,))],
    )(ring_planes, inner_rows, outer_rows, sub_part, cat_part)

    image = call(
        shade_kernel,
        1 << 20,
        4,
        name="shade",
        out_shape=f32(4, rows, wide),
        in_specs=[VMEM] * (1 + 2 * count),
        out_specs=VMEM,
        scratch_shapes=[pltpu.VMEM((count, 3, rows, wide), jnp.float32)],
    )(values, *inner_pieces, *outer_pieces)
    return sub_final, cat_final, image


def solution(mesh):
    placed = (P("gz", "gx", None), P("gz", "gx", None), P(), P())

    return jax.shard_map(
        body,
        mesh=mesh,
        in_specs=placed,
        out_specs=(P("gz", "gx", None), P("gz", "gx", None), P(None, "gx", "gz")),
        check_vma=False,
    )
```

```python
import functools

import jax
import jax.numpy as jnp
from jax import lax
from jax.experimental import pallas as pl
from jax.experimental.pallas import tpu as pltpu
from jax.sharding import PartitionSpec as P


RATES = (0.16, 0.08)
FEED = 0.037
KILL = 0.06
OPTICAL = 4.0
ROWS, LANES = 8, 128

HBM = pl.BlockSpec(memory_space=pltpu.HBM)
VMEM = pl.BlockSpec(memory_space=pltpu.VMEM)
SMEM = pl.BlockSpec(memory_space=pltpu.SMEM)


def f32(*shape):
    return jax.ShapeDtypeStruct(shape, jnp.float32)


def hbm(x):
    return pltpu.with_memory_space_constraint(x, pltpu.HBM)


def lanes(x):
    return pltpu.roll(x, 1, axis=x.ndim - 1) + pltpu.roll(x, x.shape[-1] - 1, axis=x.ndim - 1)


def react(sub, cat, around_sub, around_cat):
    growth = sub * cat * cat
    sub_new = (1.0 - 6.0 * RATES[0] - FEED) * sub + RATES[0] * around_sub - growth + FEED
    cat_new = (1.0 - 6.0 * RATES[1] - FEED - KILL) * cat + RATES[1] * around_cat + growth
    return sub_new, cat_new


def plane_step(load, tiles, low_rows, high_rows, across, store, only=None):
    for tile in range(tiles) if only is None else only:
        sums, olds = [], []
        for s in range(2):
            old = load(s, tile)
            index = lax.broadcasted_iota(jnp.int32, old.shape, 0)
            above = load(s, tile - 1)[ROWS - 1 :] if tile else low_rows and low_rows[s]
            below = load(s, tile + 1)[:1] if tile < tiles - 1 else high_rows and high_rows[s]
            above = 0.0 if above is None else jnp.broadcast_to(above, old.shape)
            below = 0.0 if below is None else jnp.broadcast_to(below, old.shape)
            up = jnp.where(index == 0, above, pltpu.roll(old, 1, axis=0))
            down = jnp.where(index == ROWS - 1, below, pltpu.roll(old, ROWS - 1, axis=0))
            sums.append(lanes(old) + (up + down) + across(s, tile))
            olds.append(old)
        store(tile, *react(olds[0], olds[1], sums[0], sums[1]))


def span(tile):
    return pl.ds(tile * ROWS, ROWS)


def across_columns(tile, columns):
    return tile[:, :columns] if columns <= LANES else jnp.concatenate([tile] * (columns // LANES), axis=1)


def planes_kernel(sub, cat, up, down, sems):
    depth = sub.shape[0]
    copies = []
    for out, plane in ((up, depth - 1), (down, 0)):
        for s, field in enumerate((sub, cat)):
            copies.append(pltpu.make_async_copy(field.at[plane], out.at[s], sems.at[len(copies)]))
    for copy in copies:
        copy.start()
    for copy in copies:
        copy.wait()


def prepare_kernel(sub, cat, low, high, q_up, q_down):
    depth, rows, _ = sub.shape
    fields = (sub, cat)
    for s, field in enumerate(fields):
        for plane in range(depth):
            for row in range(2):
                low[s, row, plane : plane + 1] = field[plane, row : row + 1]
                high[s, row, plane : plane + 1] = field[plane, rows - 2 + row : rows - 1 + row]
    for outer, inner, out in ((depth - 1, depth - 2, q_up), (0, 1, q_down)):

        def store(tile, sub_new, cat_new, out=out):
            out[0, span(tile), :] = sub_new
            out[1, span(tile), :] = cat_new

        plane_step(
            lambda s, tile, outer=outer: fields[s][outer, span(tile), :],
            rows // ROWS,
            None,
            None,
            lambda s, tile, inner=inner: fields[s][inner, span(tile), :],
            store,
        )


def composite(sub, cat, scale_sub, scale_cat, clear):
    keep = jnp.exp(-(scale_sub * sub + scale_cat * cat))
    weight = clear * (1.0 - keep)
    return weight * sub, weight * cat, clear * keep


def scalars_kernel(share, scale, emission, values):
    shape = values.shape[1:]
    for s in range(2):
        values[s] = jnp.full(shape, scale[s] * share, jnp.float32)
        for channel in range(3):
            values[2 + channel * 2 + s] = jnp.full(shape, emission[s, channel], jnp.float32)


def first_kernel(sub, cat, mid):
    depth, rows, _ = sub.shape
    old = (sub, cat)

    @pl.loop(1, depth - 1)
    def _(k):
        def store(tile, sub_new, cat_new):
            mid[0, k, span(tile), :] = sub_new
            mid[1, k, span(tile), :] = cat_new

        plane_step(
            lambda s, tile: old[s][k, span(tile), :],
            rows // ROWS,
            None,
            None,
            lambda s, tile: old[s][k - 1, span(tile), :] + old[s][k + 1, span(tile), :],
            store,
        )


def image_step(k, load, tiles, only, low_rows, high_rows, scales, seen, keep):
    def store(tile, sub, cat):
        at = span(tile)
        keep(tile, sub, cat)
        one, two, clear = composite(sub, cat, *scales, seen[2, at, :])
        seen[0, at, :] += one
        seen[1, at, :] += two
        seen[2, at, :] = clear

    plane_step(
        lambda s, tile: load(s, k, tile),
        tiles,
        low_rows,
        high_rows,
        lambda s, tile: load(s, k - 1, tile) + load(s, k + 1, tile),
        store,
        only,
    )


def clear_image(seen):
    seen[0] = jnp.zeros(seen.shape[1:], jnp.float32)
    seen[1] = jnp.zeros(seen.shape[1:], jnp.float32)
    seen[2] = jnp.ones(seen.shape[1:], jnp.float32)


def center_kernel(values, mid, sub_out, cat_out, seen, new, sem_out):
    depth, rows, columns = sub_out.shape
    outputs = (sub_out, cat_out)
    tiles = rows // ROWS
    scales = across_columns(values[0], columns), across_columns(values[1], columns)
    inside = pl.ds(ROWS, rows - 2 * ROWS)

    def put(s, k):
        return pltpu.make_async_copy(new.at[s, k], outputs[s].at[k, inside], sem_out.at[s, k])

    clear_image(seen)

    @pl.loop(2, depth - 2)
    def _(k):
        def keep(tile, sub, cat):
            new[0, k, span(tile - 1), :] = sub
            new[1, k, span(tile - 1), :] = cat

        image_step(
            k, lambda s, k, tile: mid[s, k, span(tile), :], tiles, range(1, tiles - 1), None, None, scales, seen, keep
        )
        for s in range(2):
            put(s, k).start()

    @pl.loop(2, depth - 2)
    def _(k):
        for s in range(2):
            put(s, k).wait()


def second_kernel(
    values, mid, q_up, q_down, from_low, from_high, own_low, own_high, center, sub_in, cat_in,
    sub_out, cat_out, seen, near, far, rows_low, rows_high,
    heads, tails, new, sem_out,
):
    del sub_in, cat_in
    depth, rows, columns = sub_out.shape
    outputs = (sub_out, cat_out)
    tiles = rows // ROWS
    scales = across_columns(values[0], columns), across_columns(values[1], columns)

    def put(s, k, end):
        at = pl.ds(end * (rows - ROWS), ROWS)
        return pltpu.make_async_copy(new.at[s, end, k], outputs[s].at[k, at], sem_out.at[s, end, k])

    which = lax.broadcasted_iota(jnp.int32, (depth, columns), 0)
    for got, at, own, at_own, out in (
        (from_low, 1, own_low, 0, rows_low),
        (from_high, 0, own_high, 1, rows_high),
    ):
        sums, olds = [], []
        for s in range(2):
            here = got[s, at]
            ahead = jnp.where(which == 0, 0.0, pltpu.roll(here, 1, axis=0))
            behind = jnp.where(which == depth - 1, 0.0, pltpu.roll(here, depth - 1, axis=0))
            sums.append(lanes(here) + (got[s, 1 - at] + own[s, at_own]) + (ahead + behind))
            olds.append(here)
        sub, cat = react(olds[0], olds[1], sums[0], sums[1])
        out[0] = sub
        out[1] = cat

    index = lax.broadcasted_iota(jnp.int32, (ROWS, columns), 0)

    def with_low(s, k, tile):
        row = jnp.broadcast_to(from_low[s, 1, pl.ds(k, 1)], tile.shape)
        return tile + jnp.where(index == 0, RATES[s] * row, 0.0)

    def with_high(s, k, tile):
        row = jnp.broadcast_to(from_high[s, 0, pl.ds(k, 1)], tile.shape)
        return tile + jnp.where(index == ROWS - 1, RATES[s] * row, 0.0)

    @pl.loop(1, depth - 1)
    def _(k):
        for s in range(2):
            heads[s, k] = with_low(s, k, mid[s, k, span(0), :])
            tails[s, k] = with_high(s, k, mid[s, k, span(tiles - 1), :])

    def load(s, k, tile):
        if tile == 0:
            return heads[s, k]
        if tile == tiles - 1:
            return tails[s, k]
        return mid[s, k, span(tile), :]

    for s in range(2):
        for tile in range(tiles):
            first, last = q_down[s, span(tile), :], q_up[s, span(tile), :]
            if tile == 0:
                first, last = with_low(s, 0, first), with_low(s, depth - 1, last)
            if tile == tiles - 1:
                first, last = with_high(s, 0, first), with_high(s, depth - 1, last)
            near[s, 0, span(tile), :] = first
            far[s, 2, span(tile), :] = last
            for j in range(2):
                near[s, 1 + j, span(tile), :] = load(s, 1 + j, tile)
                far[s, j, span(tile), :] = load(s, depth - 3 + j, tile)

    clear_image(seen)
    for tile in range(1, tiles - 1):
        for part in range(3):
            seen[part, span(tile), :] = center[part, span(tile), :]

    @pl.loop(2, depth - 2)
    def _(k):
        def keep(tile, sub, cat):
            new[0, 1 if tile else 0, k] = sub
            new[1, 1 if tile else 0, k] = cat

        image_step(
            k,
            load,
            tiles,
            (0, tiles - 1),
            [rows_low[s, pl.ds(k, 1)] for s in range(2)],
            [rows_high[s, pl.ds(k, 1)] for s in range(2)],
            scales,
            seen,
            keep,
        )
        for s in range(2):
            for end in range(2):
                put(s, k, end).start()

    @pl.loop(2, depth - 2)
    def _(k):
        for s in range(2):
            for end in range(2):
                put(s, k, end).wait()


def rows_kernel(q_up, q_down, from_low, from_high, up, down):
    depth = from_low.shape[2]
    tiles = q_up.shape[1] // ROWS
    for plane, q, out in ((depth - 1, q_up, up), (0, q_down, down)):
        for s in range(2):
            for tile in range(tiles):
                value = q[s, span(tile), :]
                index = lax.broadcasted_iota(jnp.int32, value.shape, 0)
                for at, edge, row in (
                    (0, 0, from_low[s, 1, plane : plane + 1]),
                    (tiles - 1, ROWS - 1, from_high[s, 0, plane : plane + 1]),
                ):
                    if tile == at:
                        beside = jnp.broadcast_to((2.0 * RATES[s]) * row, value.shape)
                        value = value + jnp.where(index == edge, beside, 0.0)
                out[s, span(tile), :] = value


def rim_kernel(
    values, p_low, p_high, down, up, near, far, rows_low, rows_high, inner,
    ring, known, seen, mid,
):
    depth = rows_low.shape[1]
    rows, columns = inner.shape[1:]
    tiles = rows // ROWS
    scale_sub, scale_cat = across_columns(values[0], columns), across_columns(values[1], columns)
    for side, p, own, inside in ((0, p_low, down, near), (1, p_high, up, far)):
        zero, one, two = (0, 1, 2) if side == 0 else (2, 1, 0)
        outer, beside = (0, 1) if side == 0 else (depth - 1, depth - 2)
        for s in range(2):
            mid[side, s] = inside[s, zero] + RATES[s] * p[s]

        def store_known(tile, sub, cat, side=side, own=own):
            at = span(tile)
            known[side, 0, at, :] = sub + (RATES[0] * RATES[0]) * own[0, at, :]
            known[side, 1, at, :] = cat + (RATES[1] * RATES[1]) * own[1, at, :]

        plane_step(
            lambda s, tile, side=side: mid[side, s, span(tile), :],
            tiles,
            [rows_low[s, outer : outer + 1] for s in range(2)],
            [rows_high[s, outer : outer + 1] for s in range(2)],
            lambda s, tile, inside=inside, one=one: inside[s, one, span(tile), :],
            store_known,
        )

        def store_ring(tile, sub, cat, side=side):
            ring[0, side, span(tile), :] = sub
            ring[1, side, span(tile), :] = cat

        plane_step(
            lambda s, tile, inside=inside, one=one: inside[s, one, span(tile), :],
            tiles,
            [rows_low[s, beside : beside + 1] for s in range(2)],
            [rows_high[s, beside : beside + 1] for s in range(2)],
            lambda s, tile, inside=inside, two=two, side=side: inside[s, two, span(tile), :]
            + mid[side, s, span(tile), :],
            store_ring,
        )

    for tile in range(tiles):
        at = span(tile)
        one, two, clear = composite(ring[0, 0, at, :], ring[1, 0, at, :], scale_sub, scale_cat, 1.0)
        sub = one + clear * inner[0, at, :]
        cat = two + clear * inner[1, at, :]
        clear = clear * inner[2, at, :]
        one, two, clear = composite(ring[0, 1, at, :], ring[1, 1, at, :], scale_sub, scale_cat, clear)
        seen[0, at, :] = sub + one
        seen[1, at, :] = cat + two
        seen[2, at, :] = clear


def partner(index, shift, count):
    return index ^ shift if count & (count - 1) == 0 else (index + shift) % count


def origin(index, shift, count):
    return index ^ shift if count & (count - 1) == 0 else (index + count - shift) % count


def last_kernel(values, known, q_low, q_high, seen, *rest):
    *pieces, outer, whole = rest
    rows, columns = seen.shape[1:]
    count = len(pieces)
    wide = columns // count
    scales = across_columns(values[0], columns), across_columns(values[1], columns)
    for tile in range(rows // ROWS):
        at = span(tile)
        planes = []
        for side, q in enumerate((q_low, q_high)):
            for s in range(2):
                value = known[side, s, at, :] + RATES[s] * q[s, at, :]
                outer[s, side, at, :] = value
                planes.append(value)
        one, two, clear = composite(planes[0], planes[1], *scales, 1.0)
        sub = one + clear * seen[0, at, :]
        cat = two + clear * seen[1, at, :]
        clear = clear * seen[2, at, :]
        one, two, clear = composite(planes[2], planes[3], *scales, clear)
        whole[0, at, :] = sub + one
        whole[1, at, :] = cat + two
        whole[2, at, :] = clear
    me = lax.axis_index("gz")
    for shift, piece in enumerate(pieces):
        target = partner(me, shift, count)
        if wide % LANES == 0:
            piece[...] = whole[:, :, pl.ds(pl.multiple_of(target * wide, LANES), wide)]
        else:
            for other in range(count):

                @pl.when(target == other)
                def _(piece=piece, other=other):
                    piece[...] = whole[:, :, other * wide : (other + 1) * wide]


def shade_kernel(values, *pieces_and_rest):
    *pieces, image, slabs = pieces_and_rest
    count = len(pieces)
    rows, wide = image.shape[1:]
    me = lax.axis_index("gz")
    for shift, piece in enumerate(pieces):
        slabs[origin(me, shift, count)] = piece[...]
    for tile in range(rows // ROWS):
        at = span(tile)
        sub, cat, clear = slabs[0, 0, at, :], slabs[0, 1, at, :], slabs[0, 2, at, :]
        for slab in range(1, count):
            sub = sub + clear * slabs[slab, 0, at, :]
            cat = cat + clear * slabs[slab, 1, at, :]
            clear = clear * slabs[slab, 2, at, :]
        for channel in range(3):
            of_sub = across_columns(values[2 + channel * 2], wide)
            of_cat = across_columns(values[3 + channel * 2], wide)
            image[channel, at, :] = of_sub * sub + of_cat * cat
        image[3, at, :] = 1.0 - clear


def place_kernel(ring, outer, sub_in, cat_in, sub_out, cat_out, sems):
    del sub_in, cat_in
    depth = sub_out.shape[0]
    copies = []
    for s, out in enumerate((sub_out, cat_out)):
        for side in range(2):
            for at, source in ((side * (depth - 1), outer), (1 + side * (depth - 3), ring)):
                copies.append(pltpu.make_async_copy(source.at[s, side], out.at[at], sems.at[len(copies)]))
    for copy in copies:
        copy.start()
    for copy in copies:
        copy.wait()


def call(kernel, flops, room, **kwargs):
    return pl.pallas_call(
        kernel,
        cost_estimate=pl.CostEstimate(flops=flops, bytes_accessed=1 << 16, transcendentals=0),
        compiler_params=pltpu.CompilerParams(vmem_limit_bytes=room << 20),
        **kwargs,
    )


def body(substrate, catalyst, extinction, emission):
    depth, rows, columns = substrate.shape
    count = lax.axis_size("gz")
    wide = columns // count
    share = OPTICAL / (depth * count)
    middle = rows - 2 * ROWS

    def ring(size, shift):
        return [(i, (i + shift) % size) for i in range(size)]

    def shifted(x, axis, shift):
        return lax.ppermute(x, axis, ring(lax.axis_size(axis), shift))

    up, down = call(
        planes_kernel,
        1 << 20,
        2,
        name="planes",
        out_shape=(f32(2, rows, columns),) * 2,
        in_specs=[HBM, HBM],
        out_specs=(VMEM,) * 2,
        scratch_shapes=[pltpu.SemaphoreType.DMA((4,))],
    )(hbm(substrate), hbm(catalyst))
    p_low = shifted(up, "gz", 1)
    p_high = shifted(down, "gz", -1)

    own_low, own_high, q_up, q_down = call(
        prepare_kernel,
        1 << 22,
        2,
        name="prepare",
        out_shape=(f32(2, 2, depth, columns),) * 2 + (f32(2, rows, columns),) * 2,
        in_specs=[VMEM] * 2,
        out_specs=(VMEM,) * 4,
    )(substrate, catalyst)
    from_low = shifted(own_high, "gx", 1)
    from_high = shifted(own_low, "gx", -1)

    mid = call(
        first_kernel,
        1 << 24,
        2,
        name="first",
        out_shape=f32(2, depth, rows, columns),
        in_specs=[VMEM, VMEM],
        out_specs=VMEM,
    )(substrate, catalyst)
    values = call(
        functools.partial(scalars_kernel, share),
        1 << 18,
        2,
        name="scalars",
        out_shape=f32(8, ROWS, LANES),
        in_specs=[SMEM, SMEM],
        out_specs=VMEM,
    )(extinction, emission.T)

    sub_part, cat_part, center = call(
        center_kernel,
        1 << 24,
        4,
        name="center",
        out_shape=(f32(depth, rows, columns), f32(depth, rows, columns), f32(3, rows, columns)),
        in_specs=[VMEM, VMEM],
        out_specs=(HBM, HBM, VMEM),
        scratch_shapes=[
            pltpu.VMEM((2, depth, middle, columns), jnp.float32),
            pltpu.SemaphoreType.DMA((2, depth)),
        ],
    )(values, mid)

    m_up, m_down = call(
        rows_kernel,
        1 << 18,
        2,
        name="rows",
        out_shape=(f32(2, rows, columns),) * 2,
        in_specs=[VMEM] * 4,
        out_specs=(VMEM,) * 2,
    )(q_up, q_down, from_low, from_high)
    q_low = shifted(m_up, "gz", 1)
    q_high = shifted(m_down, "gz", -1)

    sub_part, cat_part, inner, near, far, rows_low, rows_high = call(
        second_kernel,
        1 << 25,
        10,
        name="second",
        out_shape=(
            f32(depth, rows, columns),
            f32(depth, rows, columns),
            f32(3, rows, columns),
            f32(2, 3, rows, columns),
            f32(2, 3, rows, columns),
            f32(2, depth, columns),
            f32(2, depth, columns),
        ),
        in_specs=[VMEM] * 9 + [HBM, HBM],
        out_specs=(HBM, HBM) + (VMEM,) * 5,
        input_output_aliases={9: 0, 10: 1},
        scratch_shapes=[
            pltpu.VMEM((2, depth, ROWS, columns), jnp.float32),
            pltpu.VMEM((2, depth, ROWS, columns), jnp.float32),
            pltpu.VMEM((2, 2, depth, ROWS, columns), jnp.float32),
            pltpu.SemaphoreType.DMA((2, 2, depth)),
        ],
    )(values, mid, q_up, q_down, from_low, from_high, own_low, own_high, center, sub_part, cat_part)

    p_low, p_high, inner = lax.optimization_barrier((p_low, p_high, inner))
    ring_planes, known, seen = call(
        rim_kernel,
        1 << 23,
        4,
        name="rim",
        out_shape=(f32(2, 2, rows, columns), f32(2, 2, rows, columns), f32(3, rows, columns)),
        in_specs=[VMEM] * 10,
        out_specs=(VMEM,) * 3,
        scratch_shapes=[pltpu.VMEM((2, 2, rows, columns), jnp.float32)],
    )(values, p_low, p_high, down, up, near, far, rows_low, rows_high, inner)

    *pieces, outer = call(
        last_kernel,
        1 << 22,
        4,
        name="last",
        out_shape=(f32(3, rows, wide),) * count + (f32(2, 2, rows, columns),),
        in_specs=[VMEM] * 5,
        out_specs=(VMEM,) * (count + 1),
        scratch_shapes=[pltpu.VMEM((3, rows, columns), jnp.float32)],
    )(values, known, q_low, q_high, seen)

    received = [pieces[0]] * count
    for shift in piece_order(count):
        pairs = [(i, int(partner(i, shift, count))) for i in range(count)]
        received[shift] = lax.ppermute(pieces[shift], "gz", pairs)

    sub_final, cat_final = call(
        place_kernel,
        1 << 22,
        2,
        name="place",
        out_shape=(f32(depth, rows, columns), f32(depth, rows, columns)),
        in_specs=[VMEM, VMEM, HBM, HBM],
        out_specs=(HBM, HBM),
        input_output_aliases={2: 0, 3: 1},
        scratch_shapes=[pltpu.SemaphoreType.DMA((8,))],
    )(ring_planes, outer, sub_part, cat_part)

    image = call(
        shade_kernel,
        1 << 20,
        4,
        name="shade",
        out_shape=f32(4, rows, wide),
        in_specs=[VMEM] * (1 + count),
        out_specs=VMEM,
        scratch_shapes=[pltpu.VMEM((count, 3, rows, wide), jnp.float32)],
    )(values, *received)
    return sub_final, cat_final, image


def piece_order(count):
    half = count // 2
    return [half] + [shift for shift in range(count - 1, 0, -1) if shift != half]


def solution(mesh):
    placed = (P("gz", "gx", None), P("gz", "gx", None), P(), P())

    return jax.shard_map(
        body,
        mesh=mesh,
        in_specs=placed,
        out_specs=(P("gz", "gx", None), P("gz", "gx", None), P(None, "gx", "gz")),
        check_vma=False,
    )
```

```python
import functools

import jax
import jax.numpy as jnp
from jax import lax
from jax.experimental import pallas as pl
from jax.experimental.pallas import tpu as pltpu
from jax.sharding import PartitionSpec as P


RATES = (0.16, 0.08)
FEED = 0.037
KILL = 0.06
OPTICAL = 4.0
ROWS, LANES = 8, 128

HBM = pl.BlockSpec(memory_space=pltpu.HBM)
VMEM = pl.BlockSpec(memory_space=pltpu.VMEM)
SMEM = pl.BlockSpec(memory_space=pltpu.SMEM)


def f32(*shape):
    return jax.ShapeDtypeStruct(shape, jnp.float32)


def hbm(x):
    return pltpu.with_memory_space_constraint(x, pltpu.HBM)


def lanes(x):
    return pltpu.roll(x, 1, axis=x.ndim - 1) + pltpu.roll(x, x.shape[-1] - 1, axis=x.ndim - 1)


def react(sub, cat, around_sub, around_cat):
    growth = sub * cat * cat
    sub_new = (1.0 - 6.0 * RATES[0] - FEED) * sub + RATES[0] * around_sub - growth + FEED
    cat_new = (1.0 - 6.0 * RATES[1] - FEED - KILL) * cat + RATES[1] * around_cat + growth
    return sub_new, cat_new


def plane_step(load, tiles, low_rows, high_rows, across, store, only=None):
    for tile in range(tiles) if only is None else only:
        sums, olds = [], []
        for s in range(2):
            old = load(s, tile)
            index = lax.broadcasted_iota(jnp.int32, old.shape, 0)
            above = load(s, tile - 1)[ROWS - 1 :] if tile else low_rows and low_rows[s]
            below = load(s, tile + 1)[:1] if tile < tiles - 1 else high_rows and high_rows[s]
            above = 0.0 if above is None else jnp.broadcast_to(above, old.shape)
            below = 0.0 if below is None else jnp.broadcast_to(below, old.shape)
            up = jnp.where(index == 0, above, pltpu.roll(old, 1, axis=0))
            down = jnp.where(index == ROWS - 1, below, pltpu.roll(old, ROWS - 1, axis=0))
            sums.append(lanes(old) + (up + down) + across(s, tile))
            olds.append(old)
        store(tile, *react(olds[0], olds[1], sums[0], sums[1]))


def span(tile):
    return pl.ds(tile * ROWS, ROWS)


def across_columns(tile, columns):
    return tile[:, :columns] if columns <= LANES else jnp.concatenate([tile] * (columns // LANES), axis=1)


def tile_of(inner, outer, tile, tiles):
    if 0 < tile < tiles - 1:
        return inner, span(tile - 1)
    return outer, span(1 if tile else 0)


def planes_kernel(sub, cat, up, down, sems):
    depth = sub.shape[0]
    copies = []
    for out, plane in ((up, depth - 1), (down, 0)):
        for s, field in enumerate((sub, cat)):
            copies.append(pltpu.make_async_copy(field.at[plane], out.at[s], sems.at[len(copies)]))
    for copy in copies:
        copy.start()
    for copy in copies:
        copy.wait()


def prepare_kernel(sub, cat, low, high, q_up, q_down, r_up, r_down):
    depth, rows, _ = sub.shape
    tiles = rows // ROWS
    fields = (sub, cat)
    for s, field in enumerate(fields):
        for plane in range(depth):
            for row in range(2):
                low[s, row, plane : plane + 1] = field[plane, row : row + 1]
                high[s, row, plane : plane + 1] = field[plane, rows - 2 + row : rows - 1 + row]
    for outer, inner, q, r in ((depth - 1, depth - 2, q_up, r_up), (0, 1, q_down, r_down)):

        def store(tile, sub_new, cat_new, q=q, r=r):
            out, at = tile_of(q, r, tile, tiles)
            out[0, at, :] = sub_new
            out[1, at, :] = cat_new

        plane_step(
            lambda s, tile, outer=outer: fields[s][outer, span(tile), :],
            rows // ROWS,
            None,
            None,
            lambda s, tile, inner=inner: fields[s][inner, span(tile), :],
            store,
        )


def composite(sub, cat, scale_sub, scale_cat, clear):
    keep = jnp.exp(-(scale_sub * sub + scale_cat * cat))
    weight = clear * (1.0 - keep)
    return weight * sub, weight * cat, clear * keep


def scalars_kernel(share, scale, emission, values):
    shape = values.shape[1:]
    for s in range(2):
        values[s] = jnp.full(shape, scale[s] * share, jnp.float32)
        for channel in range(3):
            values[2 + channel * 2 + s] = jnp.full(shape, emission[s, channel], jnp.float32)


def first_kernel(sub, cat, mid):
    depth, rows, _ = sub.shape
    old = (sub, cat)

    @pl.loop(1, depth - 1)
    def _(k):
        def store(tile, sub_new, cat_new):
            mid[0, k, span(tile), :] = sub_new
            mid[1, k, span(tile), :] = cat_new

        plane_step(
            lambda s, tile: old[s][k, span(tile), :],
            rows // ROWS,
            None,
            None,
            lambda s, tile: old[s][k - 1, span(tile), :] + old[s][k + 1, span(tile), :],
            store,
        )


def image_step(k, load, tiles, only, low_rows, high_rows, scales, seen, keep):
    def store(tile, sub, cat):
        at = span(tile)
        keep(tile, sub, cat)
        one, two, clear = composite(sub, cat, *scales, seen[2, at, :])
        seen[0, at, :] += one
        seen[1, at, :] += two
        seen[2, at, :] = clear

    plane_step(
        lambda s, tile: load(s, k, tile),
        tiles,
        low_rows,
        high_rows,
        lambda s, tile: load(s, k - 1, tile) + load(s, k + 1, tile),
        store,
        only,
    )


def clear_image(seen):
    seen[0] = jnp.zeros(seen.shape[1:], jnp.float32)
    seen[1] = jnp.zeros(seen.shape[1:], jnp.float32)
    seen[2] = jnp.ones(seen.shape[1:], jnp.float32)


def center_kernel(values, mid, sub_out, cat_out, seen, new, sem_out):
    depth, rows, columns = sub_out.shape
    outputs = (sub_out, cat_out)
    tiles = rows // ROWS
    scales = across_columns(values[0], columns), across_columns(values[1], columns)
    inside = pl.ds(ROWS, rows - 2 * ROWS)

    def put(s, k):
        return pltpu.make_async_copy(new.at[s, k], outputs[s].at[k, inside], sem_out.at[s, k])

    clear_image(seen)

    @pl.loop(2, depth - 2)
    def _(k):
        def keep(tile, sub, cat):
            new[0, k, span(tile - 1), :] = sub
            new[1, k, span(tile - 1), :] = cat

        image_step(
            k, lambda s, k, tile: mid[s, k, span(tile), :], tiles, range(1, tiles - 1), None, None, scales, seen, keep
        )
        for s in range(2):
            put(s, k).start()

    @pl.loop(2, depth - 2)
    def _(k):
        for s in range(2):
            put(s, k).wait()


def second_kernel(
    values, mid, q_up, q_down, r_up, r_down, from_low, from_high, own_low, own_high, center, sub_in, cat_in,
    sub_out, cat_out, seen, near, far, rows_low, rows_high,
    heads, tails, new, sem_out,
):
    del sub_in, cat_in
    depth, rows, columns = sub_out.shape
    outputs = (sub_out, cat_out)
    tiles = rows // ROWS
    scales = across_columns(values[0], columns), across_columns(values[1], columns)

    def put(s, k, end):
        at = pl.ds(end * (rows - ROWS), ROWS)
        return pltpu.make_async_copy(new.at[s, end, k], outputs[s].at[k, at], sem_out.at[s, end, k])

    which = lax.broadcasted_iota(jnp.int32, (depth, columns), 0)
    for got, at, own, at_own, out in (
        (from_low, 1, own_low, 0, rows_low),
        (from_high, 0, own_high, 1, rows_high),
    ):
        sums, olds = [], []
        for s in range(2):
            here = got[s, at]
            ahead = jnp.where(which == 0, 0.0, pltpu.roll(here, 1, axis=0))
            behind = jnp.where(which == depth - 1, 0.0, pltpu.roll(here, depth - 1, axis=0))
            sums.append(lanes(here) + (got[s, 1 - at] + own[s, at_own]) + (ahead + behind))
            olds.append(here)
        sub, cat = react(olds[0], olds[1], sums[0], sums[1])
        out[0] = sub
        out[1] = cat

    index = lax.broadcasted_iota(jnp.int32, (ROWS, columns), 0)

    def with_low(s, k, tile):
        row = jnp.broadcast_to(from_low[s, 1, pl.ds(k, 1)], tile.shape)
        return tile + jnp.where(index == 0, RATES[s] * row, 0.0)

    def with_high(s, k, tile):
        row = jnp.broadcast_to(from_high[s, 0, pl.ds(k, 1)], tile.shape)
        return tile + jnp.where(index == ROWS - 1, RATES[s] * row, 0.0)

    @pl.loop(1, depth - 1)
    def _(k):
        for s in range(2):
            heads[s, k] = with_low(s, k, mid[s, k, span(0), :])
            tails[s, k] = with_high(s, k, mid[s, k, span(tiles - 1), :])

    def load(s, k, tile):
        if tile == 0:
            return heads[s, k]
        if tile == tiles - 1:
            return tails[s, k]
        return mid[s, k, span(tile), :]

    for s in range(2):
        for tile in range(tiles):
            down, at = tile_of(q_down, r_down, tile, tiles)
            up, at = tile_of(q_up, r_up, tile, tiles)
            first, last = down[s, at, :], up[s, at, :]
            if tile == 0:
                first, last = with_low(s, 0, first), with_low(s, depth - 1, last)
            if tile == tiles - 1:
                first, last = with_high(s, 0, first), with_high(s, depth - 1, last)
            near[s, 0, span(tile), :] = first
            far[s, 2, span(tile), :] = last
            for j in range(2):
                near[s, 1 + j, span(tile), :] = load(s, 1 + j, tile)
                far[s, j, span(tile), :] = load(s, depth - 3 + j, tile)

    clear_image(seen)
    for tile in range(1, tiles - 1):
        for part in range(3):
            seen[part, span(tile), :] = center[part, span(tile), :]

    @pl.loop(2, depth - 2)
    def _(k):
        def keep(tile, sub, cat):
            new[0, 1 if tile else 0, k] = sub
            new[1, 1 if tile else 0, k] = cat

        image_step(
            k,
            load,
            tiles,
            (0, tiles - 1),
            [rows_low[s, pl.ds(k, 1)] for s in range(2)],
            [rows_high[s, pl.ds(k, 1)] for s in range(2)],
            scales,
            seen,
            keep,
        )
        for s in range(2):
            for end in range(2):
                put(s, k, end).start()

    @pl.loop(2, depth - 2)
    def _(k):
        for s in range(2):
            for end in range(2):
                put(s, k, end).wait()


def rows_kernel(r_up, r_down, from_low, from_high, up, down):
    depth = from_low.shape[2]
    for plane, r, out in ((depth - 1, r_up, up), (0, r_down, down)):
        for place, edge, source in ((0, 0, from_low.at[:, 1]), (1, ROWS - 1, from_high.at[:, 0])):
            for s in range(2):
                tile = r[s, span(place), :]
                index = lax.broadcasted_iota(jnp.int32, tile.shape, 0)
                row = jnp.broadcast_to((2.0 * RATES[s]) * source[s, plane : plane + 1], tile.shape)
                out[s, span(place), :] = tile + jnp.where(index == edge, row, 0.0)


def rim_kernel(
    values, p_low, p_high, down, up, near, far, rows_low, rows_high, inner,
    ring, known, seen, mid,
):
    depth = rows_low.shape[1]
    rows, columns = inner.shape[1:]
    tiles = rows // ROWS
    scale_sub, scale_cat = across_columns(values[0], columns), across_columns(values[1], columns)
    for side, p, own, inside in ((0, p_low, down, near), (1, p_high, up, far)):
        zero, one, two = (0, 1, 2) if side == 0 else (2, 1, 0)
        outer, beside = (0, 1) if side == 0 else (depth - 1, depth - 2)
        for s in range(2):
            mid[side, s] = inside[s, zero] + RATES[s] * p[s]

        def store_known(tile, sub, cat, side=side, own=own):
            at = span(tile)
            known[side, 0, at, :] = sub + (RATES[0] * RATES[0]) * own[0, at, :]
            known[side, 1, at, :] = cat + (RATES[1] * RATES[1]) * own[1, at, :]

        plane_step(
            lambda s, tile, side=side: mid[side, s, span(tile), :],
            tiles,
            [rows_low[s, outer : outer + 1] for s in range(2)],
            [rows_high[s, outer : outer + 1] for s in range(2)],
            lambda s, tile, inside=inside, one=one: inside[s, one, span(tile), :],
            store_known,
        )

        def store_ring(tile, sub, cat, side=side):
            ring[0, side, span(tile), :] = sub
            ring[1, side, span(tile), :] = cat

        plane_step(
            lambda s, tile, inside=inside, one=one: inside[s, one, span(tile), :],
            tiles,
            [rows_low[s, beside : beside + 1] for s in range(2)],
            [rows_high[s, beside : beside + 1] for s in range(2)],
            lambda s, tile, inside=inside, two=two, side=side: inside[s, two, span(tile), :]
            + mid[side, s, span(tile), :],
            store_ring,
        )

    for tile in range(tiles):
        at = span(tile)
        one, two, clear = composite(ring[0, 0, at, :], ring[1, 0, at, :], scale_sub, scale_cat, 1.0)
        sub = one + clear * inner[0, at, :]
        cat = two + clear * inner[1, at, :]
        clear = clear * inner[2, at, :]
        one, two, clear = composite(ring[0, 1, at, :], ring[1, 1, at, :], scale_sub, scale_cat, clear)
        seen[0, at, :] = sub + one
        seen[1, at, :] = cat + two
        seen[2, at, :] = clear


def partner(index, shift, count):
    return index ^ shift if count & (count - 1) == 0 else (index + shift) % count


def origin(index, shift, count):
    return index ^ shift if count & (count - 1) == 0 else (index + count - shift) % count


def last_kernel(values, known, q_low, q_high, r_low, r_high, seen, *rest):
    *pieces, outer, whole = rest
    rows, columns = seen.shape[1:]
    count = len(pieces)
    wide = columns // count
    scales = across_columns(values[0], columns), across_columns(values[1], columns)
    tiles = rows // ROWS
    for tile in range(tiles):
        at = span(tile)
        planes = []
        for side, (q, r) in enumerate(((q_low, r_low), (q_high, r_high))):
            got, place = tile_of(q, r, tile, tiles)
            for s in range(2):
                value = known[side, s, at, :] + RATES[s] * got[s, place, :]
                outer[s, side, at, :] = value
                planes.append(value)
        one, two, clear = composite(planes[0], planes[1], *scales, 1.0)
        sub = one + clear * seen[0, at, :]
        cat = two + clear * seen[1, at, :]
        clear = clear * seen[2, at, :]
        one, two, clear = composite(planes[2], planes[3], *scales, clear)
        whole[0, at, :] = sub + one
        whole[1, at, :] = cat + two
        whole[2, at, :] = clear
    me = lax.axis_index("gz")
    for shift, piece in enumerate(pieces):
        target = partner(me, shift, count)
        if wide % LANES == 0:
            piece[...] = whole[:, :, pl.ds(pl.multiple_of(target * wide, LANES), wide)]
        else:
            for other in range(count):

                @pl.when(target == other)
                def _(piece=piece, other=other):
                    piece[...] = whole[:, :, other * wide : (other + 1) * wide]


def shade_kernel(values, *pieces_and_rest):
    *pieces, image, slabs = pieces_and_rest
    count = len(pieces)
    rows, wide = image.shape[1:]
    me = lax.axis_index("gz")
    for shift, piece in enumerate(pieces):
        slabs[origin(me, shift, count)] = piece[...]
    for tile in range(rows // ROWS):
        at = span(tile)
        sub, cat, clear = slabs[0, 0, at, :], slabs[0, 1, at, :], slabs[0, 2, at, :]
        for slab in range(1, count):
            sub = sub + clear * slabs[slab, 0, at, :]
            cat = cat + clear * slabs[slab, 1, at, :]
            clear = clear * slabs[slab, 2, at, :]
        for channel in range(3):
            of_sub = across_columns(values[2 + channel * 2], wide)
            of_cat = across_columns(values[3 + channel * 2], wide)
            image[channel, at, :] = of_sub * sub + of_cat * cat
        image[3, at, :] = 1.0 - clear


def place_kernel(ring, outer, sub_in, cat_in, sub_out, cat_out, sems):
    del sub_in, cat_in
    depth = sub_out.shape[0]
    copies = []
    for s, out in enumerate((sub_out, cat_out)):
        for side in range(2):
            for at, source in ((side * (depth - 1), outer), (1 + side * (depth - 3), ring)):
                copies.append(pltpu.make_async_copy(source.at[s, side], out.at[at], sems.at[len(copies)]))
    for copy in copies:
        copy.start()
    for copy in copies:
        copy.wait()


def call(kernel, flops, room, **kwargs):
    return pl.pallas_call(
        kernel,
        cost_estimate=pl.CostEstimate(flops=flops, bytes_accessed=1 << 16, transcendentals=0),
        compiler_params=pltpu.CompilerParams(vmem_limit_bytes=room << 20),
        **kwargs,
    )


def body(substrate, catalyst, extinction, emission):
    depth, rows, columns = substrate.shape
    count = lax.axis_size("gz")
    wide = columns // count
    share = OPTICAL / (depth * count)
    middle = rows - 2 * ROWS

    def ring(size, shift):
        return [(i, (i + shift) % size) for i in range(size)]

    def shifted(x, axis, shift):
        return lax.ppermute(x, axis, ring(lax.axis_size(axis), shift))

    up, down = call(
        planes_kernel,
        1 << 20,
        2,
        name="planes",
        out_shape=(f32(2, rows, columns),) * 2,
        in_specs=[HBM, HBM],
        out_specs=(VMEM,) * 2,
        scratch_shapes=[pltpu.SemaphoreType.DMA((4,))],
    )(hbm(substrate), hbm(catalyst))
    p_low = shifted(up, "gz", 1)
    p_high = shifted(down, "gz", -1)

    own_low, own_high, q_up, q_down, r_up, r_down = call(
        prepare_kernel,
        1 << 22,
        2,
        name="prepare",
        out_shape=(f32(2, 2, depth, columns),) * 2 + (f32(2, middle, columns),) * 2 + (f32(2, 2 * ROWS, columns),) * 2,
        in_specs=[VMEM] * 2,
        out_specs=(VMEM,) * 6,
    )(substrate, catalyst)
    from_low = shifted(own_high, "gx", 1)
    from_high = shifted(own_low, "gx", -1)
    q_low = shifted(q_up, "gz", 1)
    q_high = shifted(q_down, "gz", -1)

    mid = call(
        first_kernel,
        1 << 24,
        2,
        name="first",
        out_shape=f32(2, depth, rows, columns),
        in_specs=[VMEM, VMEM],
        out_specs=VMEM,
    )(substrate, catalyst)
    values = call(
        functools.partial(scalars_kernel, share),
        1 << 18,
        2,
        name="scalars",
        out_shape=f32(8, ROWS, LANES),
        in_specs=[SMEM, SMEM],
        out_specs=VMEM,
    )(extinction, emission.T)

    sub_part, cat_part, center = call(
        center_kernel,
        1 << 24,
        4,
        name="center",
        out_shape=(f32(depth, rows, columns), f32(depth, rows, columns), f32(3, rows, columns)),
        in_specs=[VMEM, VMEM],
        out_specs=(HBM, HBM, VMEM),
        scratch_shapes=[
            pltpu.VMEM((2, depth, middle, columns), jnp.float32),
            pltpu.SemaphoreType.DMA((2, depth)),
        ],
    )(values, mid)

    m_up, m_down = call(
        rows_kernel,
        1 << 18,
        2,
        name="rows",
        out_shape=(f32(2, 2 * ROWS, columns),) * 2,
        in_specs=[VMEM] * 4,
        out_specs=(VMEM,) * 2,
    )(r_up, r_down, from_low, from_high)
    r_low = shifted(m_up, "gz", 1)
    r_high = shifted(m_down, "gz", -1)

    sub_part, cat_part, inner, near, far, rows_low, rows_high = call(
        second_kernel,
        1 << 25,
        10,
        name="second",
        out_shape=(
            f32(depth, rows, columns),
            f32(depth, rows, columns),
            f32(3, rows, columns),
            f32(2, 3, rows, columns),
            f32(2, 3, rows, columns),
            f32(2, depth, columns),
            f32(2, depth, columns),
        ),
        in_specs=[VMEM] * 11 + [HBM, HBM],
        out_specs=(HBM, HBM) + (VMEM,) * 5,
        input_output_aliases={11: 0, 12: 1},
        scratch_shapes=[
            pltpu.VMEM((2, depth, ROWS, columns), jnp.float32),
            pltpu.VMEM((2, depth, ROWS, columns), jnp.float32),
            pltpu.VMEM((2, 2, depth, ROWS, columns), jnp.float32),
            pltpu.SemaphoreType.DMA((2, 2, depth)),
        ],
    )(values, mid, q_up, q_down, r_up, r_down, from_low, from_high, own_low, own_high, center, sub_part, cat_part)

    p_low, p_high, inner = lax.optimization_barrier((p_low, p_high, inner))
    ring_planes, known, seen = call(
        rim_kernel,
        1 << 23,
        4,
        name="rim",
        out_shape=(f32(2, 2, rows, columns), f32(2, 2, rows, columns), f32(3, rows, columns)),
        in_specs=[VMEM] * 10,
        out_specs=(VMEM,) * 3,
        scratch_shapes=[pltpu.VMEM((2, 2, rows, columns), jnp.float32)],
    )(values, p_low, p_high, down, up, near, far, rows_low, rows_high, inner)

    *pieces, outer = call(
        last_kernel,
        1 << 22,
        4,
        name="last",
        out_shape=(f32(3, rows, wide),) * count + (f32(2, 2, rows, columns),),
        in_specs=[VMEM] * 7,
        out_specs=(VMEM,) * (count + 1),
        scratch_shapes=[pltpu.VMEM((3, rows, columns), jnp.float32)],
    )(values, known, q_low, q_high, r_low, r_high, seen)

    received = [pieces[0]] * count
    for shift in piece_order(count):
        pairs = [(i, int(partner(i, shift, count))) for i in range(count)]
        received[shift] = lax.ppermute(pieces[shift], "gz", pairs)

    sub_final, cat_final = call(
        place_kernel,
        1 << 22,
        2,
        name="place",
        out_shape=(f32(depth, rows, columns), f32(depth, rows, columns)),
        in_specs=[VMEM, VMEM, HBM, HBM],
        out_specs=(HBM, HBM),
        input_output_aliases={2: 0, 3: 1},
        scratch_shapes=[pltpu.SemaphoreType.DMA((8,))],
    )(ring_planes, outer, sub_part, cat_part)

    image = call(
        shade_kernel,
        1 << 20,
        4,
        name="shade",
        out_shape=f32(4, rows, wide),
        in_specs=[VMEM] * (1 + count),
        out_specs=VMEM,
        scratch_shapes=[pltpu.VMEM((count, 3, rows, wide), jnp.float32)],
    )(values, *received)
    return sub_final, cat_final, image


def piece_order(count):
    half = count // 2
    return [half] + [shift for shift in range(count - 1, 0, -1) if shift != half]


def solution(mesh):
    placed = (P("gz", "gx", None), P("gz", "gx", None), P(), P())

    return jax.shard_map(
        body,
        mesh=mesh,
        in_specs=placed,
        out_specs=(P("gz", "gx", None), P("gz", "gx", None), P(None, "gx", "gz")),
        check_vma=False,
    )
```

```python
import functools

import jax
import jax.numpy as jnp
from jax import lax
from jax.experimental import pallas as pl
from jax.experimental.pallas import tpu as pltpu
from jax.sharding import PartitionSpec as P


RATES = (0.16, 0.08)
FEED = 0.037
KILL = 0.06
OPTICAL = 4.0
ROWS, LANES = 8, 128

HBM = pl.BlockSpec(memory_space=pltpu.HBM)
VMEM = pl.BlockSpec(memory_space=pltpu.VMEM)
SMEM = pl.BlockSpec(memory_space=pltpu.SMEM)


def f32(*shape):
    return jax.ShapeDtypeStruct(shape, jnp.float32)


def hbm(x):
    return pltpu.with_memory_space_constraint(x, pltpu.HBM)


def lanes(x):
    return pltpu.roll(x, 1, axis=x.ndim - 1) + pltpu.roll(x, x.shape[-1] - 1, axis=x.ndim - 1)


def react(sub, cat, around_sub, around_cat):
    growth = sub * cat * cat
    sub_new = (1.0 - 6.0 * RATES[0] - FEED) * sub + RATES[0] * around_sub - growth + FEED
    cat_new = (1.0 - 6.0 * RATES[1] - FEED - KILL) * cat + RATES[1] * around_cat + growth
    return sub_new, cat_new


def plane_step(load, tiles, low_rows, high_rows, across, store, only=None):
    for tile in range(tiles) if only is None else only:
        sums, olds = [], []
        for s in range(2):
            old = load(s, tile)
            index = lax.broadcasted_iota(jnp.int32, old.shape, 0)
            above = load(s, tile - 1)[ROWS - 1 :] if tile else low_rows and low_rows[s]
            below = load(s, tile + 1)[:1] if tile < tiles - 1 else high_rows and high_rows[s]
            above = 0.0 if above is None else jnp.broadcast_to(above, old.shape)
            below = 0.0 if below is None else jnp.broadcast_to(below, old.shape)
            up = jnp.where(index == 0, above, pltpu.roll(old, 1, axis=0))
            down = jnp.where(index == ROWS - 1, below, pltpu.roll(old, ROWS - 1, axis=0))
            sums.append(lanes(old) + (up + down) + across(s, tile))
            olds.append(old)
        store(tile, *react(olds[0], olds[1], sums[0], sums[1]))


def span(tile):
    return pl.ds(tile * ROWS, ROWS)


def across_columns(tile, columns):
    return tile[:, :columns] if columns <= LANES else jnp.concatenate([tile] * (columns // LANES), axis=1)


def tile_of(inner, outer, tile, tiles):
    if 0 < tile < tiles - 1:
        return inner, span(tile - 1)
    return outer, span(1 if tile else 0)


def planes_kernel(sub, cat, up, down, sems):
    depth = sub.shape[0]
    copies = []
    for out, plane in ((up, depth - 1), (down, 0)):
        for s, field in enumerate((sub, cat)):
            copies.append(pltpu.make_async_copy(field.at[plane], out.at[s], sems.at[len(copies)]))
    for copy in copies:
        copy.start()
    for copy in copies:
        copy.wait()


def prepare_kernel(sub, cat, low, high, q_up, q_down, r_up, r_down):
    depth, rows, _ = sub.shape
    tiles = rows // ROWS
    fields = (sub, cat)
    for s, field in enumerate(fields):
        for plane in range(depth):
            for row in range(2):
                low[s, row, plane : plane + 1] = field[plane, row : row + 1]
                high[s, row, plane : plane + 1] = field[plane, rows - 2 + row : rows - 1 + row]
    for outer, inner, q, r in ((depth - 1, depth - 2, q_up, r_up), (0, 1, q_down, r_down)):

        def store(tile, sub_new, cat_new, q=q, r=r):
            out, at = tile_of(q, r, tile, tiles)
            out[0, at, :] = sub_new
            out[1, at, :] = cat_new

        plane_step(
            lambda s, tile, outer=outer: fields[s][outer, span(tile), :],
            rows // ROWS,
            None,
            None,
            lambda s, tile, inner=inner: fields[s][inner, span(tile), :],
            store,
        )


def composite(sub, cat, scale_sub, scale_cat, clear):
    keep = jnp.exp(-(scale_sub * sub + scale_cat * cat))
    weight = clear * (1.0 - keep)
    return weight * sub, weight * cat, clear * keep


def scalars_kernel(share, scale, emission, values):
    shape = values.shape[1:]
    for s in range(2):
        values[s] = jnp.full(shape, scale[s] * share, jnp.float32)
        for channel in range(3):
            values[2 + channel * 2 + s] = jnp.full(shape, emission[s, channel], jnp.float32)


def first_kernel(sub, cat, mid):
    depth, rows, _ = sub.shape
    old = (sub, cat)

    @pl.loop(1, depth - 1)
    def _(k):
        def store(tile, sub_new, cat_new):
            mid[0, k, span(tile), :] = sub_new
            mid[1, k, span(tile), :] = cat_new

        plane_step(
            lambda s, tile: old[s][k, span(tile), :],
            rows // ROWS,
            None,
            None,
            lambda s, tile: old[s][k - 1, span(tile), :] + old[s][k + 1, span(tile), :],
            store,
        )


def image_step(k, load, tiles, only, low_rows, high_rows, scales, seen, keep):
    def store(tile, sub, cat):
        at = span(tile)
        keep(tile, sub, cat)
        one, two, clear = composite(sub, cat, *scales, seen[2, at, :])
        seen[0, at, :] += one
        seen[1, at, :] += two
        seen[2, at, :] = clear

    plane_step(
        lambda s, tile: load(s, k, tile),
        tiles,
        low_rows,
        high_rows,
        lambda s, tile: load(s, k - 1, tile) + load(s, k + 1, tile),
        store,
        only,
    )


def clear_image(seen):
    seen[0] = jnp.zeros(seen.shape[1:], jnp.float32)
    seen[1] = jnp.zeros(seen.shape[1:], jnp.float32)
    seen[2] = jnp.ones(seen.shape[1:], jnp.float32)


def center_kernel(values, mid, sub_out, cat_out, seen, new, sem_out):
    depth, rows, columns = sub_out.shape
    outputs = (sub_out, cat_out)
    tiles = rows // ROWS
    scales = across_columns(values[0], columns), across_columns(values[1], columns)
    inside = pl.ds(ROWS, rows - 2 * ROWS)

    def put(s, k):
        return pltpu.make_async_copy(new.at[s, k], outputs[s].at[k, inside], sem_out.at[s, k])

    clear_image(seen)

    @pl.loop(2, depth - 2)
    def _(k):
        def keep(tile, sub, cat):
            new[0, k, span(tile - 1), :] = sub
            new[1, k, span(tile - 1), :] = cat

        image_step(
            k, lambda s, k, tile: mid[s, k, span(tile), :], tiles, range(1, tiles - 1), None, None, scales, seen, keep
        )
        for s in range(2):
            put(s, k).start()

    @pl.loop(2, depth - 2)
    def _(k):
        for s in range(2):
            put(s, k).wait()


def second_kernel(
    values, mid, q_up, q_down, r_up, r_down, from_low, from_high, own_low, own_high, center, sub_in, cat_in,
    sub_out, cat_out, seen, near, far, rows_low, rows_high,
    heads, tails, new, sem_out,
):
    del sub_in, cat_in
    depth, rows, columns = sub_out.shape
    outputs = (sub_out, cat_out)
    tiles = rows // ROWS
    scales = across_columns(values[0], columns), across_columns(values[1], columns)

    def put(s, k, end):
        at = pl.ds(end * (rows - ROWS), ROWS)
        return pltpu.make_async_copy(new.at[s, end, k], outputs[s].at[k, at], sem_out.at[s, end, k])

    which = lax.broadcasted_iota(jnp.int32, (depth, columns), 0)
    for got, at, own, at_own, out in (
        (from_low, 1, own_low, 0, rows_low),
        (from_high, 0, own_high, 1, rows_high),
    ):
        sums, olds = [], []
        for s in range(2):
            here = got[s, at]
            ahead = jnp.where(which == 0, 0.0, pltpu.roll(here, 1, axis=0))
            behind = jnp.where(which == depth - 1, 0.0, pltpu.roll(here, depth - 1, axis=0))
            sums.append(lanes(here) + (got[s, 1 - at] + own[s, at_own]) + (ahead + behind))
            olds.append(here)
        sub, cat = react(olds[0], olds[1], sums[0], sums[1])
        out[0] = sub
        out[1] = cat

    index = lax.broadcasted_iota(jnp.int32, (ROWS, columns), 0)

    def with_low(s, k, tile):
        row = jnp.broadcast_to(from_low[s, 1, pl.ds(k, 1)], tile.shape)
        return tile + jnp.where(index == 0, RATES[s] * row, 0.0)

    def with_high(s, k, tile):
        row = jnp.broadcast_to(from_high[s, 0, pl.ds(k, 1)], tile.shape)
        return tile + jnp.where(index == ROWS - 1, RATES[s] * row, 0.0)

    @pl.loop(1, depth - 1)
    def _(k):
        for s in range(2):
            heads[s, k] = with_low(s, k, mid[s, k, span(0), :])
            tails[s, k] = with_high(s, k, mid[s, k, span(tiles - 1), :])

    def load(s, k, tile):
        if tile == 0:
            return heads[s, k]
        if tile == tiles - 1:
            return tails[s, k]
        return mid[s, k, span(tile), :]

    for s in range(2):
        for tile in range(tiles):
            down, at = tile_of(q_down, r_down, tile, tiles)
            up, at = tile_of(q_up, r_up, tile, tiles)
            first, last = down[s, at, :], up[s, at, :]
            if tile == 0:
                first, last = with_low(s, 0, first), with_low(s, depth - 1, last)
            if tile == tiles - 1:
                first, last = with_high(s, 0, first), with_high(s, depth - 1, last)
            near[s, 0, span(tile), :] = first
            far[s, 2, span(tile), :] = last
            for j in range(2):
                near[s, 1 + j, span(tile), :] = load(s, 1 + j, tile)
                far[s, j, span(tile), :] = load(s, depth - 3 + j, tile)

    clear_image(seen)
    for tile in range(1, tiles - 1):
        for part in range(3):
            seen[part, span(tile), :] = center[part, span(tile), :]

    @pl.loop(2, depth - 2)
    def _(k):
        def keep(tile, sub, cat):
            new[0, 1 if tile else 0, k] = sub
            new[1, 1 if tile else 0, k] = cat

        image_step(
            k,
            load,
            tiles,
            (0, tiles - 1),
            [rows_low[s, pl.ds(k, 1)] for s in range(2)],
            [rows_high[s, pl.ds(k, 1)] for s in range(2)],
            scales,
            seen,
            keep,
        )
        for s in range(2):
            for end in range(2):
                put(s, k, end).start()

    @pl.loop(2, depth - 2)
    def _(k):
        for s in range(2):
            for end in range(2):
                put(s, k, end).wait()


def rows_kernel(r_up, r_down, from_low, from_high, up, down):
    depth = from_low.shape[2]
    for plane, r, out in ((depth - 1, r_up, up), (0, r_down, down)):
        for place, edge, source in ((0, 0, from_low.at[:, 1]), (1, ROWS - 1, from_high.at[:, 0])):
            for s in range(2):
                tile = r[s, span(place), :]
                index = lax.broadcasted_iota(jnp.int32, tile.shape, 0)
                row = jnp.broadcast_to((2.0 * RATES[s]) * source[s, plane : plane + 1], tile.shape)
                out[s, span(place), :] = tile + jnp.where(index == edge, row, 0.0)


def rim_kernel(
    values, p_low, p_high, down, up, near, far, rows_low, rows_high, inner,
    ring, known, seen, mid,
):
    depth = rows_low.shape[1]
    rows, columns = inner.shape[1:]
    tiles = rows // ROWS
    scale_sub, scale_cat = across_columns(values[0], columns), across_columns(values[1], columns)
    for side, p, own, inside in ((0, p_low, down, near), (1, p_high, up, far)):
        zero, one, two = (0, 1, 2) if side == 0 else (2, 1, 0)
        outer, beside = (0, 1) if side == 0 else (depth - 1, depth - 2)
        for s in range(2):
            mid[side, s] = inside[s, zero] + RATES[s] * p[s]

        def store_known(tile, sub, cat, side=side, own=own):
            at = span(tile)
            known[side, 0, at, :] = sub + (RATES[0] * RATES[0]) * own[0, at, :]
            known[side, 1, at, :] = cat + (RATES[1] * RATES[1]) * own[1, at, :]

        plane_step(
            lambda s, tile, side=side: mid[side, s, span(tile), :],
            tiles,
            [rows_low[s, outer : outer + 1] for s in range(2)],
            [rows_high[s, outer : outer + 1] for s in range(2)],
            lambda s, tile, inside=inside, one=one: inside[s, one, span(tile), :],
            store_known,
        )

        def store_ring(tile, sub, cat, side=side):
            ring[0, side, span(tile), :] = sub
            ring[1, side, span(tile), :] = cat

        plane_step(
            lambda s, tile, inside=inside, one=one: inside[s, one, span(tile), :],
            tiles,
            [rows_low[s, beside : beside + 1] for s in range(2)],
            [rows_high[s, beside : beside + 1] for s in range(2)],
            lambda s, tile, inside=inside, two=two, side=side: inside[s, two, span(tile), :]
            + mid[side, s, span(tile), :],
            store_ring,
        )

    for tile in range(tiles):
        at = span(tile)
        one, two, clear = composite(ring[0, 0, at, :], ring[1, 0, at, :], scale_sub, scale_cat, 1.0)
        sub = one + clear * inner[0, at, :]
        cat = two + clear * inner[1, at, :]
        clear = clear * inner[2, at, :]
        one, two, clear = composite(ring[0, 1, at, :], ring[1, 1, at, :], scale_sub, scale_cat, clear)
        seen[0, at, :] = sub + one
        seen[1, at, :] = cat + two
        seen[2, at, :] = clear


def partner(index, shift, count):
    return index ^ shift if count & (count - 1) == 0 else (index + shift) % count


def origin(index, shift, count):
    return index ^ shift if count & (count - 1) == 0 else (index + count - shift) % count


def finish(values, known, seen, low, high, tiles, outer, whole, where):
    columns = seen.shape[2]
    scales = across_columns(values[0], columns), across_columns(values[1], columns)
    for place, tile in enumerate(tiles):
        at, to = span(tile), span(place)
        planes = []
        for side, q in enumerate((low, high)):
            for s in range(2):
                value = known[side, s, at, :] + RATES[s] * q[s, to, :]
                outer[s, side, to, :] = value
                planes.append(value)
        one, two, clear = composite(planes[0], planes[1], *scales, 1.0)
        sub = one + clear * seen[0, at, :]
        cat = two + clear * seen[1, at, :]
        clear = clear * seen[2, at, :]
        one, two, clear = composite(planes[2], planes[3], *scales, clear)
        whole[0, where(tile), :] = sub + one
        whole[1, where(tile), :] = cat + two
        whole[2, where(tile), :] = clear


def cut(whole, rows, piece, to, target, count):
    wide = whole.shape[2] // count
    if wide % LANES == 0:
        piece[:, to, :] = whole[:, rows, pl.ds(pl.multiple_of(target * wide, LANES), wide)]
        return
    for other in range(count):

        @pl.when(target == other)
        def _(other=other):
            piece[:, to, :] = whole[:, rows, other * wide : (other + 1) * wide]


def most_kernel(count, values, known, q_low, q_high, seen, piece, outer, whole):
    tiles = seen.shape[1] // ROWS
    finish(values, known, seen, q_low, q_high, range(1, tiles - 1), outer, whole, lambda tile: span(tile - 1))
    everything = pl.ds(0, piece.shape[1])
    cut(whole, everything, piece, everything, partner(lax.axis_index("gz"), count // 2, count), count)


def last_kernel(values, known, r_low, r_high, seen, most, *rest):
    *pieces, outer, whole = rest
    rows = seen.shape[1]
    tiles = rows // ROWS
    count = len(pieces)
    finish(values, known, seen, r_low, r_high, (0, tiles - 1), outer, whole, span)
    inside = pl.ds(ROWS, rows - 2 * ROWS)
    whole[:, inside, :] = most[...]
    me = lax.axis_index("gz")
    for shift, piece in enumerate(pieces):
        target = partner(me, shift, count)
        if piece.shape[1] == rows:
            everything = pl.ds(0, rows)
            cut(whole, everything, piece, everything, target, count)
        else:
            cut(whole, pl.ds(0, ROWS), piece, span(0), target, count)
            cut(whole, pl.ds(rows - ROWS, ROWS), piece, span(1), target, count)


def shade_kernel(values, half, *pieces_and_rest):
    *pieces, image, slabs = pieces_and_rest
    count = len(pieces)
    rows, wide = image.shape[1:]
    me = lax.axis_index("gz")
    for shift, piece in enumerate(pieces):
        slab = origin(me, shift, count)
        if piece.shape[1] == rows:
            slabs[slab] = piece[...]
        else:
            slabs[slab, :, pl.ds(ROWS, rows - 2 * ROWS), :] = half[...]
            slabs[slab, :, span(0), :] = piece[:, :ROWS]
            slabs[slab, :, pl.ds(rows - ROWS, ROWS), :] = piece[:, ROWS:]
    for tile in range(rows // ROWS):
        at = span(tile)
        sub, cat, clear = slabs[0, 0, at, :], slabs[0, 1, at, :], slabs[0, 2, at, :]
        for slab in range(1, count):
            sub = sub + clear * slabs[slab, 0, at, :]
            cat = cat + clear * slabs[slab, 1, at, :]
            clear = clear * slabs[slab, 2, at, :]
        for channel in range(3):
            of_sub = across_columns(values[2 + channel * 2], wide)
            of_cat = across_columns(values[3 + channel * 2], wide)
            image[channel, at, :] = of_sub * sub + of_cat * cat
        image[3, at, :] = 1.0 - clear


def place_kernel(ring, inner, outer, sub_in, cat_in, sub_out, cat_out, sems):
    del sub_in, cat_in
    depth, rows, _ = sub_out.shape
    copies = []
    for s, out in enumerate((sub_out, cat_out)):
        for side in range(2):
            plane = side * (depth - 1)
            for source, target in (
                (ring.at[s, side], out.at[1 + side * (depth - 3)]),
                (inner.at[s, side], out.at[plane, pl.ds(ROWS, rows - 2 * ROWS)]),
                (outer.at[s, side, span(0)], out.at[plane, span(0)]),
                (outer.at[s, side, span(1)], out.at[plane, pl.ds(rows - ROWS, ROWS)]),
            ):
                copies.append(pltpu.make_async_copy(source, target, sems.at[len(copies)]))
    for copy in copies:
        copy.start()
    for copy in copies:
        copy.wait()


def call(kernel, flops, room, **kwargs):
    return pl.pallas_call(
        kernel,
        cost_estimate=pl.CostEstimate(flops=flops, bytes_accessed=1 << 16, transcendentals=0),
        compiler_params=pltpu.CompilerParams(vmem_limit_bytes=room << 20),
        **kwargs,
    )


def body(substrate, catalyst, extinction, emission):
    depth, rows, columns = substrate.shape
    count = lax.axis_size("gz")
    wide = columns // count
    share = OPTICAL / (depth * count)
    middle = rows - 2 * ROWS

    def ring(size, shift):
        return [(i, (i + shift) % size) for i in range(size)]

    def shifted(x, axis, shift):
        return lax.ppermute(x, axis, ring(lax.axis_size(axis), shift))

    up, down = call(
        planes_kernel,
        1 << 20,
        2,
        name="planes",
        out_shape=(f32(2, rows, columns),) * 2,
        in_specs=[HBM, HBM],
        out_specs=(VMEM,) * 2,
        scratch_shapes=[pltpu.SemaphoreType.DMA((4,))],
    )(hbm(substrate), hbm(catalyst))
    p_low = shifted(up, "gz", 1)
    p_high = shifted(down, "gz", -1)

    own_low, own_high, q_up, q_down, r_up, r_down = call(
        prepare_kernel,
        1 << 22,
        2,
        name="prepare",
        out_shape=(f32(2, 2, depth, columns),) * 2 + (f32(2, middle, columns),) * 2 + (f32(2, 2 * ROWS, columns),) * 2,
        in_specs=[VMEM] * 2,
        out_specs=(VMEM,) * 6,
    )(substrate, catalyst)
    from_low = shifted(own_high, "gx", 1)
    from_high = shifted(own_low, "gx", -1)
    q_low = shifted(q_up, "gz", 1)
    q_high = shifted(q_down, "gz", -1)

    mid = call(
        first_kernel,
        1 << 24,
        2,
        name="first",
        out_shape=f32(2, depth, rows, columns),
        in_specs=[VMEM, VMEM],
        out_specs=VMEM,
    )(substrate, catalyst)
    values = call(
        functools.partial(scalars_kernel, share),
        1 << 18,
        2,
        name="scalars",
        out_shape=f32(8, ROWS, LANES),
        in_specs=[SMEM, SMEM],
        out_specs=VMEM,
    )(extinction, emission.T)

    sub_part, cat_part, center = call(
        center_kernel,
        1 << 24,
        4,
        name="center",
        out_shape=(f32(depth, rows, columns), f32(depth, rows, columns), f32(3, rows, columns)),
        in_specs=[VMEM, VMEM],
        out_specs=(HBM, HBM, VMEM),
        scratch_shapes=[
            pltpu.VMEM((2, depth, middle, columns), jnp.float32),
            pltpu.SemaphoreType.DMA((2, depth)),
        ],
    )(values, mid)

    m_up, m_down = call(
        rows_kernel,
        1 << 18,
        2,
        name="rows",
        out_shape=(f32(2, 2 * ROWS, columns),) * 2,
        in_specs=[VMEM] * 4,
        out_specs=(VMEM,) * 2,
    )(r_up, r_down, from_low, from_high)
    r_low = shifted(m_up, "gz", 1)
    r_high = shifted(m_down, "gz", -1)

    sub_part, cat_part, inner, near, far, rows_low, rows_high = call(
        second_kernel,
        1 << 25,
        10,
        name="second",
        out_shape=(
            f32(depth, rows, columns),
            f32(depth, rows, columns),
            f32(3, rows, columns),
            f32(2, 3, rows, columns),
            f32(2, 3, rows, columns),
            f32(2, depth, columns),
            f32(2, depth, columns),
        ),
        in_specs=[VMEM] * 11 + [HBM, HBM],
        out_specs=(HBM, HBM) + (VMEM,) * 5,
        input_output_aliases={11: 0, 12: 1},
        scratch_shapes=[
            pltpu.VMEM((2, depth, ROWS, columns), jnp.float32),
            pltpu.VMEM((2, depth, ROWS, columns), jnp.float32),
            pltpu.VMEM((2, 2, depth, ROWS, columns), jnp.float32),
            pltpu.SemaphoreType.DMA((2, 2, depth)),
        ],
    )(values, mid, q_up, q_down, r_up, r_down, from_low, from_high, own_low, own_high, center, sub_part, cat_part)

    p_low, p_high, inner = lax.optimization_barrier((p_low, p_high, inner))
    ring_planes, known, seen = call(
        rim_kernel,
        1 << 23,
        4,
        name="rim",
        out_shape=(f32(2, 2, rows, columns), f32(2, 2, rows, columns), f32(3, rows, columns)),
        in_specs=[VMEM] * 10,
        out_specs=(VMEM,) * 3,
        scratch_shapes=[pltpu.VMEM((2, 2, rows, columns), jnp.float32)],
    )(values, p_low, p_high, down, up, near, far, rows_low, rows_high, inner)

    half = count // 2
    half_piece, inner_rows, most = call(
        functools.partial(most_kernel, count),
        1 << 22,
        2,
        name="most",
        out_shape=(f32(3, middle, wide), f32(2, 2, middle, columns), f32(3, middle, columns)),
        in_specs=[VMEM] * 5,
        out_specs=(VMEM,) * 3,
    )(values, known, q_low, q_high, seen)

    def paired(piece, shift):
        return lax.ppermute(piece, "gz", [(i, int(partner(i, shift, count))) for i in range(count)])

    half_piece = paired(half_piece, half)

    *pieces, outer_rows = call(
        last_kernel,
        1 << 22,
        4,
        name="last",
        out_shape=tuple(f32(3, 2 * ROWS if shift == half else rows, wide) for shift in range(count))
        + (f32(2, 2, 2 * ROWS, columns),),
        in_specs=[VMEM] * 6,
        out_specs=(VMEM,) * (count + 1),
        scratch_shapes=[pltpu.VMEM((3, rows, columns), jnp.float32)],
    )(values, known, r_low, r_high, seen, most)

    received = [pieces[0]] * count
    for shift in range(count - 1, 0, -1):
        received[shift] = paired(pieces[shift], shift)

    sub_final, cat_final = call(
        place_kernel,
        1 << 22,
        2,
        name="place",
        out_shape=(f32(depth, rows, columns), f32(depth, rows, columns)),
        in_specs=[VMEM, VMEM, VMEM, HBM, HBM],
        out_specs=(HBM, HBM),
        input_output_aliases={3: 0, 4: 1},
        scratch_shapes=[pltpu.SemaphoreType.DMA((16,))],
    )(ring_planes, inner_rows, outer_rows, sub_part, cat_part)

    image = call(
        shade_kernel,
        1 << 20,
        4,
        name="shade",
        out_shape=f32(4, rows, wide),
        in_specs=[VMEM] * (2 + count),
        out_specs=VMEM,
        scratch_shapes=[pltpu.VMEM((count, 3, rows, wide), jnp.float32)],
    )(values, half_piece, *received)
    return sub_final, cat_final, image


def solution(mesh):
    placed = (P("gz", "gx", None), P("gz", "gx", None), P(), P())

    return jax.shard_map(
        body,
        mesh=mesh,
        in_specs=placed,
        out_specs=(P("gz", "gx", None), P("gz", "gx", None), P(None, "gx", "gz")),
        check_vma=False,
    )
```

```python
import functools

import jax
import jax.numpy as jnp
from jax import lax
from jax.experimental import pallas as pl
from jax.experimental.pallas import tpu as pltpu
from jax.sharding import PartitionSpec as P


RATES = (0.16, 0.08)
FEED = 0.037
KILL = 0.06
OPTICAL = 4.0
ROWS, LANES = 8, 128

HBM = pl.BlockSpec(memory_space=pltpu.HBM)
VMEM = pl.BlockSpec(memory_space=pltpu.VMEM)
SMEM = pl.BlockSpec(memory_space=pltpu.SMEM)


def f32(*shape):
    return jax.ShapeDtypeStruct(shape, jnp.float32)


def hbm(x):
    return pltpu.with_memory_space_constraint(x, pltpu.HBM)


def lanes(x):
    return pltpu.roll(x, 1, axis=x.ndim - 1) + pltpu.roll(x, x.shape[-1] - 1, axis=x.ndim - 1)


def react(sub, cat, around_sub, around_cat):
    growth = sub * cat * cat
    sub_new = (1.0 - 6.0 * RATES[0] - FEED) * sub + RATES[0] * around_sub - growth + FEED
    cat_new = (1.0 - 6.0 * RATES[1] - FEED - KILL) * cat + RATES[1] * around_cat + growth
    return sub_new, cat_new


def plane_step(load, tiles, low_rows, high_rows, across, store, only=None):
    for tile in range(tiles) if only is None else only:
        sums, olds = [], []
        for s in range(2):
            old = load(s, tile)
            index = lax.broadcasted_iota(jnp.int32, old.shape, 0)
            above = load(s, tile - 1)[ROWS - 1 :] if tile else low_rows and low_rows[s]
            below = load(s, tile + 1)[:1] if tile < tiles - 1 else high_rows and high_rows[s]
            above = 0.0 if above is None else jnp.broadcast_to(above, old.shape)
            below = 0.0 if below is None else jnp.broadcast_to(below, old.shape)
            up = jnp.where(index == 0, above, pltpu.roll(old, 1, axis=0))
            down = jnp.where(index == ROWS - 1, below, pltpu.roll(old, ROWS - 1, axis=0))
            sums.append(lanes(old) + (up + down) + across(s, tile))
            olds.append(old)
        store(tile, *react(olds[0], olds[1], sums[0], sums[1]))


def span(tile):
    return pl.ds(tile * ROWS, ROWS)


def across_columns(tile, columns):
    return tile[:, :columns] if columns <= LANES else jnp.concatenate([tile] * (columns // LANES), axis=1)


def tile_of(inner, outer, tile, tiles):
    if 0 < tile < tiles - 1:
        return inner, span(tile - 1)
    return outer, span(1 if tile else 0)


def planes_kernel(sub, cat, up, down, sems):
    depth = sub.shape[0]
    copies = []
    for out, plane in ((up, depth - 1), (down, 0)):
        for s, field in enumerate((sub, cat)):
            copies.append(pltpu.make_async_copy(field.at[plane], out.at[s], sems.at[len(copies)]))
    for copy in copies:
        copy.start()
    for copy in copies:
        copy.wait()


def prepare_kernel(sub, cat, low, high, q_up, q_down, r_up, r_down):
    depth, rows, _ = sub.shape
    tiles = rows // ROWS
    fields = (sub, cat)
    for s, field in enumerate(fields):
        for plane in range(depth):
            for row in range(2):
                low[s, row, plane : plane + 1] = field[plane, row : row + 1]
                high[s, row, plane : plane + 1] = field[plane, rows - 2 + row : rows - 1 + row]
    for outer, inner, q, r in ((depth - 1, depth - 2, q_up, r_up), (0, 1, q_down, r_down)):

        def store(tile, sub_new, cat_new, q=q, r=r):
            out, at = tile_of(q, r, tile, tiles)
            out[0, at, :] = sub_new
            out[1, at, :] = cat_new

        plane_step(
            lambda s, tile, outer=outer: fields[s][outer, span(tile), :],
            rows // ROWS,
            None,
            None,
            lambda s, tile, inner=inner: fields[s][inner, span(tile), :],
            store,
        )


def composite(sub, cat, scale_sub, scale_cat, clear):
    keep = jnp.exp(-(scale_sub * sub + scale_cat * cat))
    weight = clear * (1.0 - keep)
    return weight * sub, weight * cat, clear * keep


def first_kernel(share, scale_hbm, emission_hbm, sub, cat, mid, values, scale, emission, sems):
    depth, rows, _ = sub.shape
    old = (sub, cat)
    copies = [
        pltpu.make_async_copy(scale_hbm, scale, sems.at[0]),
        pltpu.make_async_copy(emission_hbm, emission, sems.at[1]),
    ]
    for copy in copies:
        copy.start()

    @pl.loop(1, depth - 1)
    def _(k):
        def store(tile, sub_new, cat_new):
            mid[0, k, span(tile), :] = sub_new
            mid[1, k, span(tile), :] = cat_new

        plane_step(
            lambda s, tile: old[s][k, span(tile), :],
            rows // ROWS,
            None,
            None,
            lambda s, tile: old[s][k - 1, span(tile), :] + old[s][k + 1, span(tile), :],
            store,
        )

    for copy in copies:
        copy.wait()
    shape = values.shape[1:]
    for s in range(2):
        values[s] = jnp.full(shape, scale[s] * share, jnp.float32)
        for channel in range(3):
            values[2 + channel * 2 + s] = jnp.full(shape, emission[s, channel], jnp.float32)


def image_step(k, load, tiles, only, low_rows, high_rows, scales, seen, keep):
    def store(tile, sub, cat):
        at = span(tile)
        keep(tile, sub, cat)
        one, two, clear = composite(sub, cat, *scales, seen[2, at, :])
        seen[0, at, :] += one
        seen[1, at, :] += two
        seen[2, at, :] = clear

    plane_step(
        lambda s, tile: load(s, k, tile),
        tiles,
        low_rows,
        high_rows,
        lambda s, tile: load(s, k - 1, tile) + load(s, k + 1, tile),
        store,
        only,
    )


def clear_image(seen):
    seen[0] = jnp.zeros(seen.shape[1:], jnp.float32)
    seen[1] = jnp.zeros(seen.shape[1:], jnp.float32)
    seen[2] = jnp.ones(seen.shape[1:], jnp.float32)


def center_kernel(values, mid, new, seen):
    depth, rows, columns = mid.shape[1:]
    tiles = rows // ROWS
    scales = across_columns(values[0], columns), across_columns(values[1], columns)
    clear_image(seen)

    @pl.loop(2, depth - 2)
    def _(k):
        def keep(tile, sub, cat):
            new[0, k, span(tile - 1), :] = sub
            new[1, k, span(tile - 1), :] = cat

        image_step(
            k, lambda s, k, tile: mid[s, k, span(tile), :], tiles, range(1, tiles - 1), None, None, scales, seen, keep
        )


def second_kernel(
    values, mid, q_up, q_down, r_up, r_down, from_low, from_high, own_low, own_high, center, done,
    sub_out, cat_out, new, seen, near, far, rows_low, rows_high,
    heads, tails, sems,
):
    depth, rows, columns = sub_out.shape
    tiles = rows // ROWS
    scales = across_columns(values[0], columns), across_columns(values[1], columns)
    planes = pl.ds(2, depth - 4)
    copies = [
        pltpu.make_async_copy(done.at[s, planes], out.at[planes, pl.ds(ROWS, rows - 2 * ROWS)], sems.at[s])
        for s, out in enumerate((sub_out, cat_out))
    ]
    for copy in copies:
        copy.start()

    which = lax.broadcasted_iota(jnp.int32, (depth, columns), 0)
    for got, at, own, at_own, out in (
        (from_low, 1, own_low, 0, rows_low),
        (from_high, 0, own_high, 1, rows_high),
    ):
        sums, olds = [], []
        for s in range(2):
            here = got[s, at]
            ahead = jnp.where(which == 0, 0.0, pltpu.roll(here, 1, axis=0))
            behind = jnp.where(which == depth - 1, 0.0, pltpu.roll(here, depth - 1, axis=0))
            sums.append(lanes(here) + (got[s, 1 - at] + own[s, at_own]) + (ahead + behind))
            olds.append(here)
        sub, cat = react(olds[0], olds[1], sums[0], sums[1])
        out[0] = sub
        out[1] = cat

    index = lax.broadcasted_iota(jnp.int32, (ROWS, columns), 0)

    def with_low(s, k, tile):
        row = jnp.broadcast_to(from_low[s, 1, pl.ds(k, 1)], tile.shape)
        return tile + jnp.where(index == 0, RATES[s] * row, 0.0)

    def with_high(s, k, tile):
        row = jnp.broadcast_to(from_high[s, 0, pl.ds(k, 1)], tile.shape)
        return tile + jnp.where(index == ROWS - 1, RATES[s] * row, 0.0)

    @pl.loop(1, depth - 1)
    def _(k):
        for s in range(2):
            heads[s, k] = with_low(s, k, mid[s, k, span(0), :])
            tails[s, k] = with_high(s, k, mid[s, k, span(tiles - 1), :])

    def load(s, k, tile):
        if tile == 0:
            return heads[s, k]
        if tile == tiles - 1:
            return tails[s, k]
        return mid[s, k, span(tile), :]

    for s in range(2):
        for tile in range(tiles):
            down, at = tile_of(q_down, r_down, tile, tiles)
            up, at = tile_of(q_up, r_up, tile, tiles)
            first, last = down[s, at, :], up[s, at, :]
            if tile == 0:
                first, last = with_low(s, 0, first), with_low(s, depth - 1, last)
            if tile == tiles - 1:
                first, last = with_high(s, 0, first), with_high(s, depth - 1, last)
            near[s, 0, span(tile), :] = first
            far[s, 2, span(tile), :] = last
            for j in range(2):
                near[s, 1 + j, span(tile), :] = load(s, 1 + j, tile)
                far[s, j, span(tile), :] = load(s, depth - 3 + j, tile)

    clear_image(seen)
    for tile in range(1, tiles - 1):
        for part in range(3):
            seen[part, span(tile), :] = center[part, span(tile), :]

    @pl.loop(2, depth - 2)
    def _(k):
        def keep(tile, sub, cat):
            new[0, 1 if tile else 0, k] = sub
            new[1, 1 if tile else 0, k] = cat

        image_step(
            k,
            load,
            tiles,
            (0, tiles - 1),
            [rows_low[s, pl.ds(k, 1)] for s in range(2)],
            [rows_high[s, pl.ds(k, 1)] for s in range(2)],
            scales,
            seen,
            keep,
        )

    for copy in copies:
        copy.wait()


def rows_kernel(r_up, r_down, from_low, from_high, up, down):
    depth = from_low.shape[2]
    for plane, r, out in ((depth - 1, r_up, up), (0, r_down, down)):
        for place, edge, source in ((0, 0, from_low.at[:, 1]), (1, ROWS - 1, from_high.at[:, 0])):
            for s in range(2):
                tile = r[s, span(place), :]
                index = lax.broadcasted_iota(jnp.int32, tile.shape, 0)
                row = jnp.broadcast_to((2.0 * RATES[s]) * source[s, plane : plane + 1], tile.shape)
                out[s, span(place), :] = tile + jnp.where(index == edge, row, 0.0)


def rim_kernel(
    values, p_low, p_high, down, up, near, far, rows_low, rows_high, inner,
    ring, known, seen, mid,
):
    depth = rows_low.shape[1]
    rows, columns = inner.shape[1:]
    tiles = rows // ROWS
    scale_sub, scale_cat = across_columns(values[0], columns), across_columns(values[1], columns)
    for side, p, own, inside in ((0, p_low, down, near), (1, p_high, up, far)):
        zero, one, two = (0, 1, 2) if side == 0 else (2, 1, 0)
        outer, beside = (0, 1) if side == 0 else (depth - 1, depth - 2)
        for s in range(2):
            mid[side, s] = inside[s, zero] + RATES[s] * p[s]

        def store_known(tile, sub, cat, side=side, own=own):
            at = span(tile)
            known[side, 0, at, :] = sub + (RATES[0] * RATES[0]) * own[0, at, :]
            known[side, 1, at, :] = cat + (RATES[1] * RATES[1]) * own[1, at, :]

        plane_step(
            lambda s, tile, side=side: mid[side, s, span(tile), :],
            tiles,
            [rows_low[s, outer : outer + 1] for s in range(2)],
            [rows_high[s, outer : outer + 1] for s in range(2)],
            lambda s, tile, inside=inside, one=one: inside[s, one, span(tile), :],
            store_known,
        )

        def store_ring(tile, sub, cat, side=side):
            ring[0, side, span(tile), :] = sub
            ring[1, side, span(tile), :] = cat

        plane_step(
            lambda s, tile, inside=inside, one=one: inside[s, one, span(tile), :],
            tiles,
            [rows_low[s, beside : beside + 1] for s in range(2)],
            [rows_high[s, beside : beside + 1] for s in range(2)],
            lambda s, tile, inside=inside, two=two, side=side: inside[s, two, span(tile), :]
            + mid[side, s, span(tile), :],
            store_ring,
        )

    for tile in range(tiles):
        at = span(tile)
        one, two, clear = composite(ring[0, 0, at, :], ring[1, 0, at, :], scale_sub, scale_cat, 1.0)
        sub = one + clear * inner[0, at, :]
        cat = two + clear * inner[1, at, :]
        clear = clear * inner[2, at, :]
        one, two, clear = composite(ring[0, 1, at, :], ring[1, 1, at, :], scale_sub, scale_cat, clear)
        seen[0, at, :] = sub + one
        seen[1, at, :] = cat + two
        seen[2, at, :] = clear


def partner(index, shift, count):
    return index ^ shift if count & (count - 1) == 0 else (index + shift) % count


def origin(index, shift, count):
    return index ^ shift if count & (count - 1) == 0 else (index + count - shift) % count


def finish(values, known, seen, low, high, tiles, outer, whole, where):
    columns = seen.shape[2]
    scales = across_columns(values[0], columns), across_columns(values[1], columns)
    for place, tile in enumerate(tiles):
        at, to = span(tile), span(place)
        planes = []
        for side, q in enumerate((low, high)):
            for s in range(2):
                value = known[side, s, at, :] + RATES[s] * q[s, to, :]
                outer[s, side, to, :] = value
                planes.append(value)
        one, two, clear = composite(planes[0], planes[1], *scales, 1.0)
        sub = one + clear * seen[0, at, :]
        cat = two + clear * seen[1, at, :]
        clear = clear * seen[2, at, :]
        one, two, clear = composite(planes[2], planes[3], *scales, clear)
        whole[0, where(tile), :] = sub + one
        whole[1, where(tile), :] = cat + two
        whole[2, where(tile), :] = clear


def cut(whole, rows, piece, to, target, count):
    wide = whole.shape[2] // count
    if wide % LANES == 0:
        piece[:, to, :] = whole[:, rows, pl.ds(pl.multiple_of(target * wide, LANES), wide)]
        return
    for other in range(count):

        @pl.when(target == other)
        def _(other=other):
            piece[:, to, :] = whole[:, rows, other * wide : (other + 1) * wide]


def most_kernel(count, values, known, q_low, q_high, seen, piece, outer, whole):
    tiles = seen.shape[1] // ROWS
    finish(values, known, seen, q_low, q_high, range(1, tiles - 1), outer, whole, lambda tile: span(tile - 1))
    everything = pl.ds(0, piece.shape[1])
    cut(whole, everything, piece, everything, partner(lax.axis_index("gz"), count // 2, count), count)


def last_kernel(values, known, r_low, r_high, seen, most, *rest):
    *pieces, outer, whole = rest
    rows = seen.shape[1]
    tiles = rows // ROWS
    count = len(pieces)
    finish(values, known, seen, r_low, r_high, (0, tiles - 1), outer, whole, span)
    inside = pl.ds(ROWS, rows - 2 * ROWS)
    whole[:, inside, :] = most[...]
    me = lax.axis_index("gz")
    for shift, piece in enumerate(pieces):
        target = partner(me, shift, count)
        if piece.shape[1] == rows:
            everything = pl.ds(0, rows)
            cut(whole, everything, piece, everything, target, count)
        else:
            cut(whole, pl.ds(0, ROWS), piece, span(0), target, count)
            cut(whole, pl.ds(rows - ROWS, ROWS), piece, span(1), target, count)


def shade_kernel(values, half, *pieces_and_rest):
    *pieces, image, slabs = pieces_and_rest
    count = len(pieces)
    rows, wide = image.shape[1:]
    me = lax.axis_index("gz")
    for shift, piece in enumerate(pieces):
        slab = origin(me, shift, count)
        if piece.shape[1] == rows:
            slabs[slab] = piece[...]
        else:
            slabs[slab, :, pl.ds(ROWS, rows - 2 * ROWS), :] = half[...]
            slabs[slab, :, span(0), :] = piece[:, :ROWS]
            slabs[slab, :, pl.ds(rows - ROWS, ROWS), :] = piece[:, ROWS:]
    for tile in range(rows // ROWS):
        at = span(tile)
        sub, cat, clear = slabs[0, 0, at, :], slabs[0, 1, at, :], slabs[0, 2, at, :]
        for slab in range(1, count):
            sub = sub + clear * slabs[slab, 0, at, :]
            cat = cat + clear * slabs[slab, 1, at, :]
            clear = clear * slabs[slab, 2, at, :]
        for channel in range(3):
            of_sub = across_columns(values[2 + channel * 2], wide)
            of_cat = across_columns(values[3 + channel * 2], wide)
            image[channel, at, :] = of_sub * sub + of_cat * cat
        image[3, at, :] = 1.0 - clear


def place_kernel(new, ring, inner, outer, sub_in, cat_in, sub_out, cat_out, sems):
    del sub_in, cat_in
    depth, rows, _ = sub_out.shape
    planes = pl.ds(2, depth - 4)
    copies = []
    for s, out in enumerate((sub_out, cat_out)):
        for end in range(2):
            target = out.at[planes, pl.ds(end * (rows - ROWS), ROWS)]
            copies.append(pltpu.make_async_copy(new.at[s, end, planes], target, sems.at[len(copies)]))
        for side in range(2):
            plane = side * (depth - 1)
            for source, target in (
                (ring.at[s, side], out.at[1 + side * (depth - 3)]),
                (inner.at[s, side], out.at[plane, pl.ds(ROWS, rows - 2 * ROWS)]),
                (outer.at[s, side, span(0)], out.at[plane, span(0)]),
                (outer.at[s, side, span(1)], out.at[plane, pl.ds(rows - ROWS, ROWS)]),
            ):
                copies.append(pltpu.make_async_copy(source, target, sems.at[len(copies)]))
    for copy in copies:
        copy.start()
    for copy in copies:
        copy.wait()


def call(kernel, flops, room, **kwargs):
    return pl.pallas_call(
        kernel,
        cost_estimate=pl.CostEstimate(flops=flops, bytes_accessed=1 << 16, transcendentals=0),
        compiler_params=pltpu.CompilerParams(vmem_limit_bytes=room << 20),
        **kwargs,
    )


def body(substrate, catalyst, extinction, emission):
    depth, rows, columns = substrate.shape
    count = lax.axis_size("gz")
    wide = columns // count
    share = OPTICAL / (depth * count)
    middle = rows - 2 * ROWS

    def ring(size, shift):
        return [(i, (i + shift) % size) for i in range(size)]

    def shifted(x, axis, shift):
        return lax.ppermute(x, axis, ring(lax.axis_size(axis), shift))

    up, down = call(
        planes_kernel,
        1 << 20,
        2,
        name="planes",
        out_shape=(f32(2, rows, columns),) * 2,
        in_specs=[HBM, HBM],
        out_specs=(VMEM,) * 2,
        scratch_shapes=[pltpu.SemaphoreType.DMA((4,))],
    )(hbm(substrate), hbm(catalyst))
    p_low = shifted(up, "gz", 1)
    p_high = shifted(down, "gz", -1)

    own_low, own_high, q_up, q_down, r_up, r_down = call(
        prepare_kernel,
        1 << 22,
        2,
        name="prepare",
        out_shape=(f32(2, 2, depth, columns),) * 2 + (f32(2, middle, columns),) * 2 + (f32(2, 2 * ROWS, columns),) * 2,
        in_specs=[VMEM] * 2,
        out_specs=(VMEM,) * 6,
    )(substrate, catalyst)
    from_low = shifted(own_high, "gx", 1)
    from_high = shifted(own_low, "gx", -1)
    q_low = shifted(q_up, "gz", 1)
    q_high = shifted(q_down, "gz", -1)

    mid, values = call(
        functools.partial(first_kernel, share),
        1 << 24,
        2,
        name="first",
        out_shape=(f32(2, depth, rows, columns), f32(8, ROWS, LANES)),
        in_specs=[HBM, HBM, VMEM, VMEM],
        out_specs=(VMEM, VMEM),
        scratch_shapes=[
            pltpu.SMEM((2,), jnp.float32),
            pltpu.SMEM((2, 3), jnp.float32),
            pltpu.SemaphoreType.DMA((2,)),
        ],
    )(hbm(extinction), hbm(emission.T), substrate, catalyst)
    done, center = call(
        center_kernel,
        1 << 24,
        2,
        name="center",
        out_shape=(f32(2, depth, middle, columns), f32(3, rows, columns)),
        in_specs=[VMEM, VMEM],
        out_specs=(VMEM, VMEM),
    )(values, mid)

    m_up, m_down = call(
        rows_kernel,
        1 << 18,
        2,
        name="rows",
        out_shape=(f32(2, 2 * ROWS, columns),) * 2,
        in_specs=[VMEM] * 4,
        out_specs=(VMEM,) * 2,
    )(r_up, r_down, from_low, from_high)
    r_low = shifted(m_up, "gz", 1)
    r_high = shifted(m_down, "gz", -1)

    sub_part, cat_part, new, inner, near, far, rows_low, rows_high = call(
        second_kernel,
        1 << 25,
        4,
        name="second",
        out_shape=(
            f32(depth, rows, columns),
            f32(depth, rows, columns),
            f32(2, 2, depth, ROWS, columns),
            f32(3, rows, columns),
            f32(2, 3, rows, columns),
            f32(2, 3, rows, columns),
            f32(2, depth, columns),
            f32(2, depth, columns),
        ),
        in_specs=[VMEM] * 12,
        out_specs=(HBM, HBM) + (VMEM,) * 6,
        scratch_shapes=[
            pltpu.VMEM((2, depth, ROWS, columns), jnp.float32),
            pltpu.VMEM((2, depth, ROWS, columns), jnp.float32),
            pltpu.SemaphoreType.DMA((2,)),
        ],
    )(values, mid, q_up, q_down, r_up, r_down, from_low, from_high, own_low, own_high, center, done)

    p_low, p_high, inner = lax.optimization_barrier((p_low, p_high, inner))
    ring_planes, known, seen = call(
        rim_kernel,
        1 << 23,
        4,
        name="rim",
        out_shape=(f32(2, 2, rows, columns), f32(2, 2, rows, columns), f32(3, rows, columns)),
        in_specs=[VMEM] * 10,
        out_specs=(VMEM,) * 3,
        scratch_shapes=[pltpu.VMEM((2, 2, rows, columns), jnp.float32)],
    )(values, p_low, p_high, down, up, near, far, rows_low, rows_high, inner)

    half = count // 2
    half_piece, inner_rows, most = call(
        functools.partial(most_kernel, count),
        1 << 22,
        2,
        name="most",
        out_shape=(f32(3, middle, wide), f32(2, 2, middle, columns), f32(3, middle, columns)),
        in_specs=[VMEM] * 5,
        out_specs=(VMEM,) * 3,
    )(values, known, q_low, q_high, seen)

    def paired(piece, shift):
        return lax.ppermute(piece, "gz", [(i, int(partner(i, shift, count))) for i in range(count)])

    half_piece = paired(half_piece, half)

    *pieces, outer_rows = call(
        last_kernel,
        1 << 22,
        4,
        name="last",
        out_shape=tuple(f32(3, 2 * ROWS if shift == half else rows, wide) for shift in range(count))
        + (f32(2, 2, 2 * ROWS, columns),),
        in_specs=[VMEM] * 6,
        out_specs=(VMEM,) * (count + 1),
        scratch_shapes=[pltpu.VMEM((3, rows, columns), jnp.float32)],
    )(values, known, r_low, r_high, seen, most)

    received = [pieces[0]] * count
    for shift in range(count - 1, 0, -1):
        received[shift] = paired(pieces[shift], shift)

    sub_final, cat_final = call(
        place_kernel,
        1 << 22,
        2,
        name="place",
        out_shape=(f32(depth, rows, columns), f32(depth, rows, columns)),
        in_specs=[VMEM, VMEM, VMEM, VMEM, HBM, HBM],
        out_specs=(HBM, HBM),
        input_output_aliases={4: 0, 5: 1},
        scratch_shapes=[pltpu.SemaphoreType.DMA((20,))],
    )(new, ring_planes, inner_rows, outer_rows, sub_part, cat_part)

    image = call(
        shade_kernel,
        1 << 20,
        4,
        name="shade",
        out_shape=f32(4, rows, wide),
        in_specs=[VMEM] * (2 + count),
        out_specs=VMEM,
        scratch_shapes=[pltpu.VMEM((count, 3, rows, wide), jnp.float32)],
    )(values, half_piece, *received)
    return sub_final, cat_final, image


def solution(mesh):
    placed = (P("gz", "gx", None), P("gz", "gx", None), P(), P())

    return jax.shard_map(
        body,
        mesh=mesh,
        in_specs=placed,
        out_specs=(P("gz", "gx", None), P("gz", "gx", None), P(None, "gx", "gz")),
        check_vma=False,
    )
```

```python
import functools

import jax
import jax.numpy as jnp
from jax import lax
from jax.experimental import pallas as pl
from jax.experimental.pallas import tpu as pltpu
from jax.sharding import PartitionSpec as P


RATES = (0.16, 0.08)
FEED = 0.037
KILL = 0.06
OPTICAL = 4.0
ROWS, LANES = 8, 128

HBM = pl.BlockSpec(memory_space=pltpu.HBM)
VMEM = pl.BlockSpec(memory_space=pltpu.VMEM)
SMEM = pl.BlockSpec(memory_space=pltpu.SMEM)


def f32(*shape):
    return jax.ShapeDtypeStruct(shape, jnp.float32)


def hbm(x):
    return pltpu.with_memory_space_constraint(x, pltpu.HBM)


def lanes(x):
    return pltpu.roll(x, 1, axis=x.ndim - 1) + pltpu.roll(x, x.shape[-1] - 1, axis=x.ndim - 1)


def react(sub, cat, around_sub, around_cat):
    growth = sub * cat * cat
    sub_new = (1.0 - 6.0 * RATES[0] - FEED) * sub + RATES[0] * around_sub - growth + FEED
    cat_new = (1.0 - 6.0 * RATES[1] - FEED - KILL) * cat + RATES[1] * around_cat + growth
    return sub_new, cat_new


def plane_step(load, tiles, low_rows, high_rows, across, store, only=None):
    for tile in range(tiles) if only is None else only:
        sums, olds = [], []
        for s in range(2):
            old = load(s, tile)
            index = lax.broadcasted_iota(jnp.int32, old.shape, 0)
            above = load(s, tile - 1)[ROWS - 1 :] if tile else low_rows and low_rows[s]
            below = load(s, tile + 1)[:1] if tile < tiles - 1 else high_rows and high_rows[s]
            above = 0.0 if above is None else jnp.broadcast_to(above, old.shape)
            below = 0.0 if below is None else jnp.broadcast_to(below, old.shape)
            up = jnp.where(index == 0, above, pltpu.roll(old, 1, axis=0))
            down = jnp.where(index == ROWS - 1, below, pltpu.roll(old, ROWS - 1, axis=0))
            sums.append(lanes(old) + (up + down) + across(s, tile))
            olds.append(old)
        store(tile, *react(olds[0], olds[1], sums[0], sums[1]))


def span(tile):
    return pl.ds(tile * ROWS, ROWS)


def across_columns(tile, columns):
    return tile[:, :columns] if columns <= LANES else jnp.concatenate([tile] * (columns // LANES), axis=1)


def tile_of(inner, outer, tile, tiles):
    if 0 < tile < tiles - 1:
        return inner, span(tile - 1)
    return outer, span(1 if tile else 0)


def planes_kernel(sub, cat, up, down, sems):
    depth = sub.shape[0]
    copies = []
    for out, plane in ((up, depth - 1), (down, 0)):
        for s, field in enumerate((sub, cat)):
            copies.append(pltpu.make_async_copy(field.at[plane], out.at[s], sems.at[len(copies)]))
    for copy in copies:
        copy.start()
    for copy in copies:
        copy.wait()


def prepare_kernel(sub, cat, low, high, q_up, q_down, r_up, r_down):
    depth, rows, _ = sub.shape
    tiles = rows // ROWS
    fields = (sub, cat)
    for s, field in enumerate(fields):
        for plane in range(depth):
            for row in range(2):
                low[s, row, plane : plane + 1] = field[plane, row : row + 1]
                high[s, row, plane : plane + 1] = field[plane, rows - 2 + row : rows - 1 + row]
    for outer, inner, q, r in ((depth - 1, depth - 2, q_up, r_up), (0, 1, q_down, r_down)):

        def store(tile, sub_new, cat_new, q=q, r=r):
            out, at = tile_of(q, r, tile, tiles)
            out[0, at, :] = sub_new
            out[1, at, :] = cat_new

        plane_step(
            lambda s, tile, outer=outer: fields[s][outer, span(tile), :],
            rows // ROWS,
            None,
            None,
            lambda s, tile, inner=inner: fields[s][inner, span(tile), :],
            store,
        )


def composite(sub, cat, scale_sub, scale_cat, clear):
    keep = jnp.exp(-(scale_sub * sub + scale_cat * cat))
    weight = clear * (1.0 - keep)
    return weight * sub, weight * cat, clear * keep


def first_kernel(share, scale_hbm, emission_hbm, sub, cat, mid, values, scale, emission, sems):
    depth, rows, _ = sub.shape
    old = (sub, cat)
    copies = [
        pltpu.make_async_copy(scale_hbm, scale, sems.at[0]),
        pltpu.make_async_copy(emission_hbm, emission, sems.at[1]),
    ]
    for copy in copies:
        copy.start()

    @pl.loop(1, depth - 1)
    def _(k):
        def store(tile, sub_new, cat_new):
            mid[0, k, span(tile), :] = sub_new
            mid[1, k, span(tile), :] = cat_new

        plane_step(
            lambda s, tile: old[s][k, span(tile), :],
            rows // ROWS,
            None,
            None,
            lambda s, tile: old[s][k - 1, span(tile), :] + old[s][k + 1, span(tile), :],
            store,
        )

    for copy in copies:
        copy.wait()
    shape = values.shape[1:]
    for s in range(2):
        values[s] = jnp.full(shape, scale[s] * share, jnp.float32)
        for channel in range(3):
            values[2 + channel * 2 + s] = jnp.full(shape, emission[s, channel], jnp.float32)


def image_step(k, load, tiles, only, low_rows, high_rows, scales, seen, keep):
    def store(tile, sub, cat):
        at = span(tile)
        keep(tile, sub, cat)
        one, two, clear = composite(sub, cat, *scales, seen[2, at, :])
        seen[0, at, :] += one
        seen[1, at, :] += two
        seen[2, at, :] = clear

    plane_step(
        lambda s, tile: load(s, k, tile),
        tiles,
        low_rows,
        high_rows,
        lambda s, tile: load(s, k - 1, tile) + load(s, k + 1, tile),
        store,
        only,
    )


def clear_image(seen):
    seen[0] = jnp.zeros(seen.shape[1:], jnp.float32)
    seen[1] = jnp.zeros(seen.shape[1:], jnp.float32)
    seen[2] = jnp.ones(seen.shape[1:], jnp.float32)


def center_kernel(values, mid, new, seen):
    depth, rows, columns = mid.shape[1:]
    tiles = rows // ROWS
    scales = across_columns(values[0], columns), across_columns(values[1], columns)
    clear_image(seen)

    @pl.loop(2, depth - 2)
    def _(k):
        def keep(tile, sub, cat):
            new[0, k, span(tile - 1), :] = sub
            new[1, k, span(tile - 1), :] = cat

        image_step(
            k, lambda s, k, tile: mid[s, k, span(tile), :], tiles, range(1, tiles - 1), None, None, scales, seen, keep
        )


def second_kernel(
    values, mid, q_up, q_down, r_up, r_down, from_low, from_high, own_low, own_high, center, done,
    sub_out, cat_out, new, seen, near, far, rows_low, rows_high,
    heads, tails, sems,
):
    depth, rows, columns = sub_out.shape
    tiles = rows // ROWS
    scales = across_columns(values[0], columns), across_columns(values[1], columns)
    planes = pl.ds(2, depth - 4)
    copies = [
        pltpu.make_async_copy(done.at[s, planes], out.at[planes, pl.ds(ROWS, rows - 2 * ROWS)], sems.at[s])
        for s, out in enumerate((sub_out, cat_out))
    ]
    for copy in copies:
        copy.start()

    which = lax.broadcasted_iota(jnp.int32, (depth, columns), 0)
    for got, at, own, at_own, out in (
        (from_low, 1, own_low, 0, rows_low),
        (from_high, 0, own_high, 1, rows_high),
    ):
        sums, olds = [], []
        for s in range(2):
            here = got[s, at]
            ahead = jnp.where(which == 0, 0.0, pltpu.roll(here, 1, axis=0))
            behind = jnp.where(which == depth - 1, 0.0, pltpu.roll(here, depth - 1, axis=0))
            sums.append(lanes(here) + (got[s, 1 - at] + own[s, at_own]) + (ahead + behind))
            olds.append(here)
        sub, cat = react(olds[0], olds[1], sums[0], sums[1])
        out[0] = sub
        out[1] = cat

    index = lax.broadcasted_iota(jnp.int32, (ROWS, columns), 0)

    def with_low(s, k, tile):
        row = jnp.broadcast_to(from_low[s, 1, pl.ds(k, 1)], tile.shape)
        return tile + jnp.where(index == 0, RATES[s] * row, 0.0)

    def with_high(s, k, tile):
        row = jnp.broadcast_to(from_high[s, 0, pl.ds(k, 1)], tile.shape)
        return tile + jnp.where(index == ROWS - 1, RATES[s] * row, 0.0)

    @pl.loop(1, depth - 1)
    def _(k):
        for s in range(2):
            heads[s, k] = with_low(s, k, mid[s, k, span(0), :])
            tails[s, k] = with_high(s, k, mid[s, k, span(tiles - 1), :])

    def load(s, k, tile):
        if tile == 0:
            return heads[s, k]
        if tile == tiles - 1:
            return tails[s, k]
        return mid[s, k, span(tile), :]

    for s in range(2):
        for tile in range(tiles):
            down, at = tile_of(q_down, r_down, tile, tiles)
            up, at = tile_of(q_up, r_up, tile, tiles)
            first, last = down[s, at, :], up[s, at, :]
            if tile == 0:
                first, last = with_low(s, 0, first), with_low(s, depth - 1, last)
            if tile == tiles - 1:
                first, last = with_high(s, 0, first), with_high(s, depth - 1, last)
            near[s, 0, span(tile), :] = first
            far[s, 2, span(tile), :] = last
            for j in range(2):
                near[s, 1 + j, span(tile), :] = load(s, 1 + j, tile)
                far[s, j, span(tile), :] = load(s, depth - 3 + j, tile)

    clear_image(seen)
    for tile in range(1, tiles - 1):
        for part in range(3):
            seen[part, span(tile), :] = center[part, span(tile), :]

    @pl.loop(2, depth - 2)
    def _(k):
        def keep(tile, sub, cat):
            new[0, 1 if tile else 0, k] = sub
            new[1, 1 if tile else 0, k] = cat

        image_step(
            k,
            load,
            tiles,
            (0, tiles - 1),
            [rows_low[s, pl.ds(k, 1)] for s in range(2)],
            [rows_high[s, pl.ds(k, 1)] for s in range(2)],
            scales,
            seen,
            keep,
        )

    for copy in copies:
        copy.wait()


def rows_kernel(r_up, r_down, from_low, from_high, up, down):
    depth = from_low.shape[2]
    for plane, r, out in ((depth - 1, r_up, up), (0, r_down, down)):
        for place, edge, source in ((0, 0, from_low.at[:, 1]), (1, ROWS - 1, from_high.at[:, 0])):
            for s in range(2):
                tile = r[s, span(place), :]
                index = lax.broadcasted_iota(jnp.int32, tile.shape, 0)
                row = jnp.broadcast_to((2.0 * RATES[s]) * source[s, plane : plane + 1], tile.shape)
                out[s, span(place), :] = tile + jnp.where(index == edge, row, 0.0)


def rim_kernel(
    values, p_low, p_high, down, up, near, far, rows_low, rows_high, inner,
    ring, known, seen, mid,
):
    depth = rows_low.shape[1]
    rows, columns = inner.shape[1:]
    tiles = rows // ROWS
    scale_sub, scale_cat = across_columns(values[0], columns), across_columns(values[1], columns)
    for side, p, own, inside in ((0, p_low, down, near), (1, p_high, up, far)):
        zero, one, two = (0, 1, 2) if side == 0 else (2, 1, 0)
        outer, beside = (0, 1) if side == 0 else (depth - 1, depth - 2)
        for s in range(2):
            mid[side, s] = inside[s, zero] + RATES[s] * p[s]

        def store_known(tile, sub, cat, side=side, own=own):
            at = span(tile)
            known[side, 0, at, :] = sub + (RATES[0] * RATES[0]) * own[0, at, :]
            known[side, 1, at, :] = cat + (RATES[1] * RATES[1]) * own[1, at, :]

        plane_step(
            lambda s, tile, side=side: mid[side, s, span(tile), :],
            tiles,
            [rows_low[s, outer : outer + 1] for s in range(2)],
            [rows_high[s, outer : outer + 1] for s in range(2)],
            lambda s, tile, inside=inside, one=one: inside[s, one, span(tile), :],
            store_known,
        )

        def store_ring(tile, sub, cat, side=side):
            ring[0, side, span(tile), :] = sub
            ring[1, side, span(tile), :] = cat

        plane_step(
            lambda s, tile, inside=inside, one=one: inside[s, one, span(tile), :],
            tiles,
            [rows_low[s, beside : beside + 1] for s in range(2)],
            [rows_high[s, beside : beside + 1] for s in range(2)],
            lambda s, tile, inside=inside, two=two, side=side: inside[s, two, span(tile), :]
            + mid[side, s, span(tile), :],
            store_ring,
        )

    for tile in range(tiles):
        at = span(tile)
        one, two, clear = composite(ring[0, 0, at, :], ring[1, 0, at, :], scale_sub, scale_cat, 1.0)
        sub = one + clear * inner[0, at, :]
        cat = two + clear * inner[1, at, :]
        clear = clear * inner[2, at, :]
        one, two, clear = composite(ring[0, 1, at, :], ring[1, 1, at, :], scale_sub, scale_cat, clear)
        seen[0, at, :] = sub + one
        seen[1, at, :] = cat + two
        seen[2, at, :] = clear


def partner(index, shift, count):
    return index ^ shift if count & (count - 1) == 0 else (index + shift) % count


def origin(index, shift, count):
    return index ^ shift if count & (count - 1) == 0 else (index + count - shift) % count


def finish(values, known, seen, low, high, tiles, outer, whole, where):
    columns = seen.shape[2]
    scales = across_columns(values[0], columns), across_columns(values[1], columns)
    for place, tile in enumerate(tiles):
        at, to = span(tile), span(place)
        planes = []
        for side, q in enumerate((low, high)):
            for s in range(2):
                value = known[side, s, at, :] + RATES[s] * q[s, to, :]
                outer[s, side, to, :] = value
                planes.append(value)
        one, two, clear = composite(planes[0], planes[1], *scales, 1.0)
        sub = one + clear * seen[0, at, :]
        cat = two + clear * seen[1, at, :]
        clear = clear * seen[2, at, :]
        one, two, clear = composite(planes[2], planes[3], *scales, clear)
        whole[0, where(tile), :] = sub + one
        whole[1, where(tile), :] = cat + two
        whole[2, where(tile), :] = clear


def cut(whole, rows, piece, to, target, count):
    wide = whole.shape[2] // count
    if wide % LANES == 0:
        piece[:, to, :] = whole[:, rows, pl.ds(pl.multiple_of(target * wide, LANES), wide)]
        return
    for other in range(count):

        @pl.when(target == other)
        def _(other=other):
            piece[:, to, :] = whole[:, rows, other * wide : (other + 1) * wide]


def most_kernel(count, values, known, q_low, q_high, seen, piece, outer, whole):
    tiles = seen.shape[1] // ROWS
    finish(values, known, seen, q_low, q_high, range(1, tiles - 1), outer, whole, lambda tile: span(tile - 1))
    everything = pl.ds(0, piece.shape[1])
    cut(whole, everything, piece, everything, partner(lax.axis_index("gz"), count // 2, count), count)


def last_kernel(values, known, r_low, r_high, seen, most, *rest):
    *pieces, outer, whole = rest
    rows = seen.shape[1]
    tiles = rows // ROWS
    count = len(pieces)
    finish(values, known, seen, r_low, r_high, (0, tiles - 1), outer, whole, span)
    inside = pl.ds(ROWS, rows - 2 * ROWS)
    whole[:, inside, :] = most[...]
    me = lax.axis_index("gz")
    for shift, piece in enumerate(pieces):
        target = partner(me, shift, count)
        if piece.shape[1] == rows:
            everything = pl.ds(0, rows)
            cut(whole, everything, piece, everything, target, count)
        else:
            cut(whole, pl.ds(0, ROWS), piece, span(0), target, count)
            cut(whole, pl.ds(rows - ROWS, ROWS), piece, span(1), target, count)


def lanes_of(block, wide):
    return pl.ds(pl.multiple_of(block * wide, LANES), wide)


def foreign_kernel(count, q_up, q_down, up, down):
    wide = q_up.shape[2] // count
    me = lax.axis_index("gz")
    for q, out, target in ((q_up, up, (me + 1) % count), (q_down, down, (me + count - 1) % count)):
        for block in range(count - 1):
            out[:, :, block * wide : (block + 1) * wide] = q[:, :, lanes_of((target + 1 + block) % count, wide)]


def split_kernel(count, m_up, m_down, q_up, q_down, up, down, own_up, own_down):
    outers = m_up.shape[1]
    wide = m_up.shape[2] // count
    rows = own_up.shape[1]
    me = lax.axis_index("gz")
    for m, q, out, own, target in (
        (m_up, q_up, up, own_up, (me + 1) % count),
        (m_down, q_down, down, own_down, (me + count - 1) % count),
    ):
        for block in range(count - 1):
            out[:, :, block * wide : (block + 1) * wide] = m[:, :, lanes_of((target + 1 + block) % count, wide)]
        mine = lanes_of(target, wide)
        own[:, :ROWS, :] = m[:, :ROWS, mine]
        own[:, pl.ds(ROWS, rows - outers), :] = q[:, :, mine]
        own[:, rows - ROWS :, :] = m[:, ROWS:, mine]


def finish_tile(scales, low, high, seen):
    one, two, clear = composite(low[0], low[1], *scales, 1.0)
    sub = one + clear * seen[0]
    cat = two + clear * seen[1]
    clear = clear * seen[2]
    one, two, clear = composite(high[0], high[1], *scales, clear)
    return sub + one, cat + two, clear


def others_kernel(values, known, q_low, q_high, r_low, r_high, seen, *pieces_and_outer):
    *pieces, outer = pieces_and_outer
    rows, columns = seen.shape[1:]
    count = len(pieces) + 1
    wide = columns // count
    tiles = rows // ROWS
    scales = across_columns(values[0], wide), across_columns(values[1], wide)
    me = lax.axis_index("gz")
    for shift, piece in enumerate(pieces, 1):
        owner = partner(me, shift, count)
        there = lanes_of(owner, wide)
        sent = lanes_of((owner + count - me - 1) % count, wide)
        for tile in range(tiles):
            at = span(tile)
            ends = []
            for side, (q, r) in enumerate(((q_low, r_low), (q_high, r_high))):
                got, place = tile_of(q, r, tile, tiles)
                ends.append([known[side, s, at, there] + RATES[s] * got[s, place, sent] for s in range(2)])
                for s in range(2):
                    outer[s, side, at, there] = ends[side][s]
            result = finish_tile(scales, ends[0], ends[1], [seen[part, at, there] for part in range(3)])
            for part in range(3):
                piece[part, at, :] = result[part]


def own_kernel(values, known, o_low, o_high, seen, piece, outer):
    rows, wide = piece.shape[1:]
    scales = across_columns(values[0], wide), across_columns(values[1], wide)
    here = lanes_of(lax.axis_index("gz"), wide)
    for tile in range(rows // ROWS):
        at = span(tile)
        ends = []
        for side, o in enumerate((o_low, o_high)):
            ends.append([known[side, s, at, here] + RATES[s] * o[s, at, :] for s in range(2)])
            for s in range(2):
                outer[s, side, at, :] = ends[side][s]
        result = finish_tile(scales, ends[0], ends[1], [seen[part, at, here] for part in range(3)])
        for part in range(3):
            piece[part, at, :] = result[part]


def put_kernel(count, new, ring, others, own, sub_in, cat_in, sub_out, cat_out, sems):
    del sub_in, cat_in
    depth, rows, columns = sub_out.shape
    wide = columns // count
    planes = pl.ds(2, depth - 4)
    me = lax.axis_index("gz")
    copies = []
    for s, out in enumerate((sub_out, cat_out)):
        targets = []
        for end in range(2):
            targets.append((new.at[s, end, planes], out.at[planes, pl.ds(end * (rows - ROWS), ROWS)]))
        for side in range(2):
            plane = side * (depth - 1)
            targets.append((ring.at[s, side], out.at[1 + side * (depth - 3)]))
            targets.append((own.at[s, side], out.at[plane, :, lanes_of(me, wide)]))
            for shift in range(1, count):
                there = lanes_of(partner(me, shift, count), wide)
                targets.append((others.at[s, side, :, there], out.at[plane, :, there]))
        for source, target in targets:
            copies.append(pltpu.make_async_copy(source, target, sems.at[len(copies)]))
    for copy in copies:
        copy.start()
    for copy in copies:
        copy.wait()


def paint_kernel(values, *pieces_and_rest):
    *pieces, image, slabs = pieces_and_rest
    count = len(pieces)
    me = lax.axis_index("gz")
    for shift, piece in enumerate(pieces):
        slabs[origin(me, shift, count)] = piece[...]
    shade(values, slabs, image, count)


def shade(values, slabs, image, count):
    rows, wide = image.shape[1:]
    for tile in range(rows // ROWS):
        at = span(tile)
        sub, cat, clear = slabs[0, 0, at, :], slabs[0, 1, at, :], slabs[0, 2, at, :]
        for slab in range(1, count):
            sub = sub + clear * slabs[slab, 0, at, :]
            cat = cat + clear * slabs[slab, 1, at, :]
            clear = clear * slabs[slab, 2, at, :]
        for channel in range(3):
            of_sub = across_columns(values[2 + channel * 2], wide)
            of_cat = across_columns(values[3 + channel * 2], wide)
            image[channel, at, :] = of_sub * sub + of_cat * cat
        image[3, at, :] = 1.0 - clear


def shade_kernel(values, half, *pieces_and_rest):
    *pieces, image, slabs = pieces_and_rest
    count = len(pieces)
    rows, _ = image.shape[1:]
    me = lax.axis_index("gz")
    for shift, piece in enumerate(pieces):
        slab = origin(me, shift, count)
        if piece.shape[1] == rows:
            slabs[slab] = piece[...]
        else:
            slabs[slab, :, pl.ds(ROWS, rows - 2 * ROWS), :] = half[...]
            slabs[slab, :, span(0), :] = piece[:, :ROWS]
            slabs[slab, :, pl.ds(rows - ROWS, ROWS), :] = piece[:, ROWS:]
    shade(values, slabs, image, count)


def place_kernel(new, ring, inner, outer, sub_in, cat_in, sub_out, cat_out, sems):
    del sub_in, cat_in
    depth, rows, _ = sub_out.shape
    planes = pl.ds(2, depth - 4)
    copies = []
    for s, out in enumerate((sub_out, cat_out)):
        for end in range(2):
            target = out.at[planes, pl.ds(end * (rows - ROWS), ROWS)]
            copies.append(pltpu.make_async_copy(new.at[s, end, planes], target, sems.at[len(copies)]))
        for side in range(2):
            plane = side * (depth - 1)
            for source, target in (
                (ring.at[s, side], out.at[1 + side * (depth - 3)]),
                (inner.at[s, side], out.at[plane, pl.ds(ROWS, rows - 2 * ROWS)]),
                (outer.at[s, side, span(0)], out.at[plane, span(0)]),
                (outer.at[s, side, span(1)], out.at[plane, pl.ds(rows - ROWS, ROWS)]),
            ):
                copies.append(pltpu.make_async_copy(source, target, sems.at[len(copies)]))
    for copy in copies:
        copy.start()
    for copy in copies:
        copy.wait()


def call(kernel, flops, room, **kwargs):
    return pl.pallas_call(
        kernel,
        cost_estimate=pl.CostEstimate(flops=flops, bytes_accessed=1 << 16, transcendentals=0),
        compiler_params=pltpu.CompilerParams(vmem_limit_bytes=room << 20),
        **kwargs,
    )


def body(substrate, catalyst, extinction, emission):
    depth, rows, columns = substrate.shape
    count = lax.axis_size("gz")
    wide = columns // count
    share = OPTICAL / (depth * count)
    middle = rows - 2 * ROWS

    def ring(size, shift):
        return [(i, (i + shift) % size) for i in range(size)]

    def shifted(x, axis, shift):
        return lax.ppermute(x, axis, ring(lax.axis_size(axis), shift))

    up, down = call(
        planes_kernel,
        1 << 20,
        2,
        name="planes",
        out_shape=(f32(2, rows, columns),) * 2,
        in_specs=[HBM, HBM],
        out_specs=(VMEM,) * 2,
        scratch_shapes=[pltpu.SemaphoreType.DMA((4,))],
    )(hbm(substrate), hbm(catalyst))
    p_low = shifted(up, "gz", 1)
    p_high = shifted(down, "gz", -1)

    own_low, own_high, q_up, q_down, r_up, r_down = call(
        prepare_kernel,
        1 << 22,
        2,
        name="prepare",
        out_shape=(f32(2, 2, depth, columns),) * 2 + (f32(2, middle, columns),) * 2 + (f32(2, 2 * ROWS, columns),) * 2,
        in_specs=[VMEM] * 2,
        out_specs=(VMEM,) * 6,
    )(substrate, catalyst)
    from_low = shifted(own_high, "gx", 1)
    from_high = shifted(own_low, "gx", -1)
    split = wide % LANES == 0
    foreign = columns - wide
    if split:
        q_sent = call(
            functools.partial(foreign_kernel, count),
            1 << 18,
            2,
            name="foreign",
            out_shape=(f32(2, middle, foreign),) * 2,
            in_specs=[VMEM] * 2,
            out_specs=(VMEM,) * 2,
        )(q_up, q_down)
    else:
        q_sent = (q_up, q_down)
    q_low = shifted(q_sent[0], "gz", 1)
    q_high = shifted(q_sent[1], "gz", -1)

    mid, values = call(
        functools.partial(first_kernel, share),
        1 << 24,
        2,
        name="first",
        out_shape=(f32(2, depth, rows, columns), f32(8, ROWS, LANES)),
        in_specs=[HBM, HBM, VMEM, VMEM],
        out_specs=(VMEM, VMEM),
        scratch_shapes=[
            pltpu.SMEM((2,), jnp.float32),
            pltpu.SMEM((2, 3), jnp.float32),
            pltpu.SemaphoreType.DMA((2,)),
        ],
    )(hbm(extinction), hbm(emission.T), substrate, catalyst)
    done, center = call(
        center_kernel,
        1 << 24,
        2,
        name="center",
        out_shape=(f32(2, depth, middle, columns), f32(3, rows, columns)),
        in_specs=[VMEM, VMEM],
        out_specs=(VMEM, VMEM),
    )(values, mid)

    m_up, m_down = call(
        rows_kernel,
        1 << 18,
        2,
        name="rows",
        out_shape=(f32(2, 2 * ROWS, columns),) * 2,
        in_specs=[VMEM] * 4,
        out_specs=(VMEM,) * 2,
    )(r_up, r_down, from_low, from_high)
    if split:
        m_up, m_down, o_up, o_down = call(
            functools.partial(split_kernel, count),
            1 << 18,
            2,
            name="split",
            out_shape=(f32(2, 2 * ROWS, foreign),) * 2 + (f32(2, rows, wide),) * 2,
            in_specs=[VMEM] * 4,
            out_specs=(VMEM,) * 4,
        )(m_up, m_down, q_up, q_down)
        o_low = shifted(o_up, "gz", 1)
        o_high = shifted(o_down, "gz", -1)
    r_low = shifted(m_up, "gz", 1)
    r_high = shifted(m_down, "gz", -1)

    sub_part, cat_part, new, inner, near, far, rows_low, rows_high = call(
        second_kernel,
        1 << 25,
        4,
        name="second",
        out_shape=(
            f32(depth, rows, columns),
            f32(depth, rows, columns),
            f32(2, 2, depth, ROWS, columns),
            f32(3, rows, columns),
            f32(2, 3, rows, columns),
            f32(2, 3, rows, columns),
            f32(2, depth, columns),
            f32(2, depth, columns),
        ),
        in_specs=[VMEM] * 12,
        out_specs=(HBM, HBM) + (VMEM,) * 6,
        scratch_shapes=[
            pltpu.VMEM((2, depth, ROWS, columns), jnp.float32),
            pltpu.VMEM((2, depth, ROWS, columns), jnp.float32),
            pltpu.SemaphoreType.DMA((2,)),
        ],
    )(values, mid, q_up, q_down, r_up, r_down, from_low, from_high, own_low, own_high, center, done)

    p_low, p_high, inner = lax.optimization_barrier((p_low, p_high, inner))
    ring_planes, known, seen = call(
        rim_kernel,
        1 << 23,
        4,
        name="rim",
        out_shape=(f32(2, 2, rows, columns), f32(2, 2, rows, columns), f32(3, rows, columns)),
        in_specs=[VMEM] * 10,
        out_specs=(VMEM,) * 3,
        scratch_shapes=[pltpu.VMEM((2, 2, rows, columns), jnp.float32)],
    )(values, p_low, p_high, down, up, near, far, rows_low, rows_high, inner)

    def paired(piece, shift):
        return lax.ppermute(piece, "gz", [(i, int(partner(i, shift, count))) for i in range(count)])

    if split:
        *pieces, others = call(
            others_kernel,
            1 << 22,
            2,
            name="others",
            out_shape=(f32(3, rows, wide),) * (count - 1) + (f32(2, 2, rows, columns),),
            in_specs=[VMEM] * 7,
            out_specs=(VMEM,) * count,
        )(values, known, q_low, q_high, r_low, r_high, seen)
        received = [None] * count
        half = count // 2
        for shift in [i for i in range(count - 1, 0, -1) if i != half] + [half]:
            received[shift] = paired(pieces[shift - 1], shift)
        received[0], own = call(
            own_kernel,
            1 << 20,
            2,
            name="own",
            out_shape=(f32(3, rows, wide), f32(2, 2, rows, wide)),
            in_specs=[VMEM] * 5,
            out_specs=(VMEM,) * 2,
        )(values, known, o_low, o_high, seen)
        sub_final, cat_final = call(
            functools.partial(put_kernel, count),
            1 << 22,
            2,
            name="put",
            out_shape=(f32(depth, rows, columns), f32(depth, rows, columns)),
            in_specs=[VMEM, VMEM, VMEM, VMEM, HBM, HBM],
            out_specs=(HBM, HBM),
            input_output_aliases={4: 0, 5: 1},
            scratch_shapes=[pltpu.SemaphoreType.DMA((4 * (count + 2),))],
        )(new, ring_planes, others, own, sub_part, cat_part)
        image = call(
            paint_kernel,
            1 << 20,
            4,
            name="paint",
            out_shape=f32(4, rows, wide),
            in_specs=[VMEM] * (1 + count),
            out_specs=VMEM,
            scratch_shapes=[pltpu.VMEM((count, 3, rows, wide), jnp.float32)],
        )(values, *received)
        return sub_final, cat_final, image

    half = count // 2
    half_piece, inner_rows, most = call(
        functools.partial(most_kernel, count),
        1 << 22,
        2,
        name="most",
        out_shape=(f32(3, middle, wide), f32(2, 2, middle, columns), f32(3, middle, columns)),
        in_specs=[VMEM] * 5,
        out_specs=(VMEM,) * 3,
    )(values, known, q_low, q_high, seen)

    half_piece = paired(half_piece, half)

    *pieces, outer_rows = call(
        last_kernel,
        1 << 22,
        4,
        name="last",
        out_shape=tuple(f32(3, 2 * ROWS if shift == half else rows, wide) for shift in range(count))
        + (f32(2, 2, 2 * ROWS, columns),),
        in_specs=[VMEM] * 6,
        out_specs=(VMEM,) * (count + 1),
        scratch_shapes=[pltpu.VMEM((3, rows, columns), jnp.float32)],
    )(values, known, r_low, r_high, seen, most)

    received = [pieces[0]] * count
    for shift in range(count - 1, 0, -1):
        received[shift] = paired(pieces[shift], shift)

    sub_final, cat_final = call(
        place_kernel,
        1 << 22,
        2,
        name="place",
        out_shape=(f32(depth, rows, columns), f32(depth, rows, columns)),
        in_specs=[VMEM, VMEM, VMEM, VMEM, HBM, HBM],
        out_specs=(HBM, HBM),
        input_output_aliases={4: 0, 5: 1},
        scratch_shapes=[pltpu.SemaphoreType.DMA((20,))],
    )(new, ring_planes, inner_rows, outer_rows, sub_part, cat_part)

    image = call(
        shade_kernel,
        1 << 20,
        4,
        name="shade",
        out_shape=f32(4, rows, wide),
        in_specs=[VMEM] * (2 + count),
        out_specs=VMEM,
        scratch_shapes=[pltpu.VMEM((count, 3, rows, wide), jnp.float32)],
    )(values, half_piece, *received)
    return sub_final, cat_final, image


def solution(mesh):
    placed = (P("gz", "gx", None), P("gz", "gx", None), P(), P())

    return jax.shard_map(
        body,
        mesh=mesh,
        in_specs=placed,
        out_specs=(P("gz", "gx", None), P("gz", "gx", None), P(None, "gx", "gz")),
        check_vma=False,
    )
```

```python
import functools

import jax
import jax.numpy as jnp
from jax import lax
from jax.experimental import pallas as pl
from jax.experimental.pallas import tpu as pltpu
from jax.sharding import PartitionSpec as P


RATES = (0.16, 0.08)
FEED = 0.037
KILL = 0.06
OPTICAL = 4.0
ROWS, LANES = 8, 128

HBM = pl.BlockSpec(memory_space=pltpu.HBM)
VMEM = pl.BlockSpec(memory_space=pltpu.VMEM)
SMEM = pl.BlockSpec(memory_space=pltpu.SMEM)


def f32(*shape):
    return jax.ShapeDtypeStruct(shape, jnp.float32)


def hbm(x):
    return pltpu.with_memory_space_constraint(x, pltpu.HBM)


def lanes(x):
    return pltpu.roll(x, 1, axis=x.ndim - 1) + pltpu.roll(x, x.shape[-1] - 1, axis=x.ndim - 1)


def react(sub, cat, around_sub, around_cat):
    growth = sub * cat * cat
    sub_new = (1.0 - 6.0 * RATES[0] - FEED) * sub + RATES[0] * around_sub - growth + FEED
    cat_new = (1.0 - 6.0 * RATES[1] - FEED - KILL) * cat + RATES[1] * around_cat + growth
    return sub_new, cat_new


def plane_step(load, tiles, low_rows, high_rows, across, store, only=None):
    for tile in range(tiles) if only is None else only:
        sums, olds = [], []
        for s in range(2):
            old = load(s, tile)
            index = lax.broadcasted_iota(jnp.int32, old.shape, 0)
            above = load(s, tile - 1)[ROWS - 1 :] if tile else low_rows and low_rows[s]
            below = load(s, tile + 1)[:1] if tile < tiles - 1 else high_rows and high_rows[s]
            above = 0.0 if above is None else jnp.broadcast_to(above, old.shape)
            below = 0.0 if below is None else jnp.broadcast_to(below, old.shape)
            up = jnp.where(index == 0, above, pltpu.roll(old, 1, axis=0))
            down = jnp.where(index == ROWS - 1, below, pltpu.roll(old, ROWS - 1, axis=0))
            sums.append(lanes(old) + (up + down) + across(s, tile))
            olds.append(old)
        store(tile, *react(olds[0], olds[1], sums[0], sums[1]))


def span(tile):
    return pl.ds(tile * ROWS, ROWS)


def across_columns(tile, columns):
    return tile[:, :columns] if columns <= LANES else jnp.concatenate([tile] * (columns // LANES), axis=1)


def tile_of(inner, outer, tile, tiles):
    if 0 < tile < tiles - 1:
        return inner, span(tile - 1)
    return outer, span(1 if tile else 0)


def planes_kernel(sub, cat, up, down, sems):
    depth = sub.shape[0]
    copies = []
    for out, plane in ((up, depth - 1), (down, 0)):
        for s, field in enumerate((sub, cat)):
            copies.append(pltpu.make_async_copy(field.at[plane], out.at[s], sems.at[len(copies)]))
    for copy in copies:
        copy.start()
    for copy in copies:
        copy.wait()


def prepare_kernel(sub, cat, low, high, q_up, q_down, r_up, r_down):
    depth, rows, _ = sub.shape
    tiles = rows // ROWS
    fields = (sub, cat)
    for s, field in enumerate(fields):
        for plane in range(depth):
            for row in range(2):
                low[s, row, plane : plane + 1] = field[plane, row : row + 1]
                high[s, row, plane : plane + 1] = field[plane, rows - 2 + row : rows - 1 + row]
    for outer, inner, q, r in ((depth - 1, depth - 2, q_up, r_up), (0, 1, q_down, r_down)):

        def store(tile, sub_new, cat_new, q=q, r=r):
            out, at = tile_of(q, r, tile, tiles)
            out[0, at, :] = sub_new
            out[1, at, :] = cat_new

        plane_step(
            lambda s, tile, outer=outer: fields[s][outer, span(tile), :],
            rows // ROWS,
            None,
            None,
            lambda s, tile, inner=inner: fields[s][inner, span(tile), :],
            store,
        )


def composite(sub, cat, scale_sub, scale_cat, clear):
    keep = jnp.exp(-(scale_sub * sub + scale_cat * cat))
    weight = clear * (1.0 - keep)
    return weight * sub, weight * cat, clear * keep


def first_kernel(share, scale_hbm, emission_hbm, sub, cat, mid, values, scale, emission, sems):
    depth, rows, _ = sub.shape
    old = (sub, cat)
    copies = [
        pltpu.make_async_copy(scale_hbm, scale, sems.at[0]),
        pltpu.make_async_copy(emission_hbm, emission, sems.at[1]),
    ]
    for copy in copies:
        copy.start()

    @pl.loop(1, depth - 1)
    def _(k):
        def store(tile, sub_new, cat_new):
            mid[0, k, span(tile), :] = sub_new
            mid[1, k, span(tile), :] = cat_new

        plane_step(
            lambda s, tile: old[s][k, span(tile), :],
            rows // ROWS,
            None,
            None,
            lambda s, tile: old[s][k - 1, span(tile), :] + old[s][k + 1, span(tile), :],
            store,
        )

    for copy in copies:
        copy.wait()
    shape = values.shape[1:]
    for s in range(2):
        values[s] = jnp.full(shape, scale[s] * share, jnp.float32)
        for channel in range(3):
            values[2 + channel * 2 + s] = jnp.full(shape, emission[s, channel], jnp.float32)


def image_step(k, load, tiles, only, low_rows, high_rows, scales, seen, keep):
    def store(tile, sub, cat):
        at = span(tile)
        keep(tile, sub, cat)
        one, two, clear = composite(sub, cat, *scales, seen[2, at, :])
        seen[0, at, :] += one
        seen[1, at, :] += two
        seen[2, at, :] = clear

    plane_step(
        lambda s, tile: load(s, k, tile),
        tiles,
        low_rows,
        high_rows,
        lambda s, tile: load(s, k - 1, tile) + load(s, k + 1, tile),
        store,
        only,
    )


def clear_image(seen):
    seen[0] = jnp.zeros(seen.shape[1:], jnp.float32)
    seen[1] = jnp.zeros(seen.shape[1:], jnp.float32)
    seen[2] = jnp.ones(seen.shape[1:], jnp.float32)


def center_kernel(values, mid, new, seen):
    depth, rows, columns = mid.shape[1:]
    tiles = rows // ROWS
    scales = across_columns(values[0], columns), across_columns(values[1], columns)
    clear_image(seen)

    @pl.loop(2, depth - 2)
    def _(k):
        def keep(tile, sub, cat):
            new[0, k, span(tile - 1), :] = sub
            new[1, k, span(tile - 1), :] = cat

        image_step(
            k, lambda s, k, tile: mid[s, k, span(tile), :], tiles, range(1, tiles - 1), None, None, scales, seen, keep
        )


def second_kernel(
    values, mid, q_up, q_down, r_up, r_down, from_low, from_high, own_low, own_high, center, done,
    sub_out, cat_out, new, seen, near, far, rows_low, rows_high,
    heads, tails, sems,
):
    depth, rows, columns = sub_out.shape
    tiles = rows // ROWS
    scales = across_columns(values[0], columns), across_columns(values[1], columns)
    planes = pl.ds(2, depth - 4)
    copies = [
        pltpu.make_async_copy(done.at[s, planes], out.at[planes, pl.ds(ROWS, rows - 2 * ROWS)], sems.at[s])
        for s, out in enumerate((sub_out, cat_out))
    ]
    for copy in copies:
        copy.start()

    which = lax.broadcasted_iota(jnp.int32, (depth, columns), 0)
    for got, at, own, at_own, out in (
        (from_low, 1, own_low, 0, rows_low),
        (from_high, 0, own_high, 1, rows_high),
    ):
        sums, olds = [], []
        for s in range(2):
            here = got[s, at]
            ahead = jnp.where(which == 0, 0.0, pltpu.roll(here, 1, axis=0))
            behind = jnp.where(which == depth - 1, 0.0, pltpu.roll(here, depth - 1, axis=0))
            sums.append(lanes(here) + (got[s, 1 - at] + own[s, at_own]) + (ahead + behind))
            olds.append(here)
        sub, cat = react(olds[0], olds[1], sums[0], sums[1])
        out[0] = sub
        out[1] = cat

    index = lax.broadcasted_iota(jnp.int32, (ROWS, columns), 0)

    def with_low(s, k, tile):
        row = jnp.broadcast_to(from_low[s, 1, pl.ds(k, 1)], tile.shape)
        return tile + jnp.where(index == 0, RATES[s] * row, 0.0)

    def with_high(s, k, tile):
        row = jnp.broadcast_to(from_high[s, 0, pl.ds(k, 1)], tile.shape)
        return tile + jnp.where(index == ROWS - 1, RATES[s] * row, 0.0)

    @pl.loop(1, depth - 1)
    def _(k):
        for s in range(2):
            heads[s, k] = with_low(s, k, mid[s, k, span(0), :])
            tails[s, k] = with_high(s, k, mid[s, k, span(tiles - 1), :])

    def load(s, k, tile):
        if tile == 0:
            return heads[s, k]
        if tile == tiles - 1:
            return tails[s, k]
        return mid[s, k, span(tile), :]

    for s in range(2):
        for tile in range(tiles):
            down, at = tile_of(q_down, r_down, tile, tiles)
            up, at = tile_of(q_up, r_up, tile, tiles)
            first, last = down[s, at, :], up[s, at, :]
            if tile == 0:
                first, last = with_low(s, 0, first), with_low(s, depth - 1, last)
            if tile == tiles - 1:
                first, last = with_high(s, 0, first), with_high(s, depth - 1, last)
            near[s, 0, span(tile), :] = first
            far[s, 2, span(tile), :] = last
            for j in range(2):
                near[s, 1 + j, span(tile), :] = load(s, 1 + j, tile)
                far[s, j, span(tile), :] = load(s, depth - 3 + j, tile)

    clear_image(seen)
    for tile in range(1, tiles - 1):
        for part in range(3):
            seen[part, span(tile), :] = center[part, span(tile), :]

    @pl.loop(2, depth - 2)
    def _(k):
        def keep(tile, sub, cat):
            new[0, 1 if tile else 0, k] = sub
            new[1, 1 if tile else 0, k] = cat

        image_step(
            k,
            load,
            tiles,
            (0, tiles - 1),
            [rows_low[s, pl.ds(k, 1)] for s in range(2)],
            [rows_high[s, pl.ds(k, 1)] for s in range(2)],
            scales,
            seen,
            keep,
        )

    for copy in copies:
        copy.wait()


def rows_kernel(r_up, r_down, from_low, from_high, up, down):
    depth = from_low.shape[2]
    for plane, r, out in ((depth - 1, r_up, up), (0, r_down, down)):
        for place, edge, source in ((0, 0, from_low.at[:, 1]), (1, ROWS - 1, from_high.at[:, 0])):
            for s in range(2):
                tile = r[s, span(place), :]
                index = lax.broadcasted_iota(jnp.int32, tile.shape, 0)
                row = jnp.broadcast_to((2.0 * RATES[s]) * source[s, plane : plane + 1], tile.shape)
                out[s, span(place), :] = tile + jnp.where(index == edge, row, 0.0)


def rim_kernel(
    values, p_low, p_high, down, up, near, far, rows_low, rows_high, inner,
    ring, known, seen, mid,
):
    depth = rows_low.shape[1]
    rows, columns = inner.shape[1:]
    tiles = rows // ROWS
    scale_sub, scale_cat = across_columns(values[0], columns), across_columns(values[1], columns)
    for side, p, own, inside in ((0, p_low, down, near), (1, p_high, up, far)):
        zero, one, two = (0, 1, 2) if side == 0 else (2, 1, 0)
        outer, beside = (0, 1) if side == 0 else (depth - 1, depth - 2)
        for s in range(2):
            mid[side, s] = inside[s, zero] + RATES[s] * p[s]

        def store_known(tile, sub, cat, side=side, own=own):
            at = span(tile)
            known[side, 0, at, :] = sub + (RATES[0] * RATES[0]) * own[0, at, :]
            known[side, 1, at, :] = cat + (RATES[1] * RATES[1]) * own[1, at, :]

        plane_step(
            lambda s, tile, side=side: mid[side, s, span(tile), :],
            tiles,
            [rows_low[s, outer : outer + 1] for s in range(2)],
            [rows_high[s, outer : outer + 1] for s in range(2)],
            lambda s, tile, inside=inside, one=one: inside[s, one, span(tile), :],
            store_known,
        )

        def store_ring(tile, sub, cat, side=side):
            ring[0, side, span(tile), :] = sub
            ring[1, side, span(tile), :] = cat

        plane_step(
            lambda s, tile, inside=inside, one=one: inside[s, one, span(tile), :],
            tiles,
            [rows_low[s, beside : beside + 1] for s in range(2)],
            [rows_high[s, beside : beside + 1] for s in range(2)],
            lambda s, tile, inside=inside, two=two, side=side: inside[s, two, span(tile), :]
            + mid[side, s, span(tile), :],
            store_ring,
        )

    for tile in range(tiles):
        at = span(tile)
        one, two, clear = composite(ring[0, 0, at, :], ring[1, 0, at, :], scale_sub, scale_cat, 1.0)
        sub = one + clear * inner[0, at, :]
        cat = two + clear * inner[1, at, :]
        clear = clear * inner[2, at, :]
        one, two, clear = composite(ring[0, 1, at, :], ring[1, 1, at, :], scale_sub, scale_cat, clear)
        seen[0, at, :] = sub + one
        seen[1, at, :] = cat + two
        seen[2, at, :] = clear


def partner(index, shift, count):
    return index ^ shift if count & (count - 1) == 0 else (index + shift) % count


def origin(index, shift, count):
    return index ^ shift if count & (count - 1) == 0 else (index + count - shift) % count


def finish(values, known, seen, low, high, tiles, outer, whole, where):
    columns = seen.shape[2]
    scales = across_columns(values[0], columns), across_columns(values[1], columns)
    for place, tile in enumerate(tiles):
        at, to = span(tile), span(place)
        planes = []
        for side, q in enumerate((low, high)):
            for s in range(2):
                value = known[side, s, at, :] + RATES[s] * q[s, to, :]
                outer[s, side, to, :] = value
                planes.append(value)
        one, two, clear = composite(planes[0], planes[1], *scales, 1.0)
        sub = one + clear * seen[0, at, :]
        cat = two + clear * seen[1, at, :]
        clear = clear * seen[2, at, :]
        one, two, clear = composite(planes[2], planes[3], *scales, clear)
        whole[0, where(tile), :] = sub + one
        whole[1, where(tile), :] = cat + two
        whole[2, where(tile), :] = clear


def cut(whole, rows, piece, to, target, count):
    wide = whole.shape[2] // count
    if wide % LANES == 0:
        piece[:, to, :] = whole[:, rows, pl.ds(pl.multiple_of(target * wide, LANES), wide)]
        return
    for other in range(count):

        @pl.when(target == other)
        def _(other=other):
            piece[:, to, :] = whole[:, rows, other * wide : (other + 1) * wide]


def most_kernel(count, values, known, q_low, q_high, seen, piece, outer, whole):
    tiles = seen.shape[1] // ROWS
    finish(values, known, seen, q_low, q_high, range(1, tiles - 1), outer, whole, lambda tile: span(tile - 1))
    everything = pl.ds(0, piece.shape[1])
    cut(whole, everything, piece, everything, partner(lax.axis_index("gz"), count // 2, count), count)


def last_kernel(values, known, r_low, r_high, seen, most, *rest):
    *pieces, outer, whole = rest
    rows = seen.shape[1]
    tiles = rows // ROWS
    count = len(pieces)
    finish(values, known, seen, r_low, r_high, (0, tiles - 1), outer, whole, span)
    inside = pl.ds(ROWS, rows - 2 * ROWS)
    whole[:, inside, :] = most[...]
    me = lax.axis_index("gz")
    for shift, piece in enumerate(pieces):
        target = partner(me, shift, count)
        if piece.shape[1] == rows:
            everything = pl.ds(0, rows)
            cut(whole, everything, piece, everything, target, count)
        else:
            cut(whole, pl.ds(0, ROWS), piece, span(0), target, count)
            cut(whole, pl.ds(rows - ROWS, ROWS), piece, span(1), target, count)


def lanes_of(block, wide):
    return pl.ds(pl.multiple_of(block * wide, LANES), wide)


def foreign_kernel(count, q_up, q_down, up, down):
    wide = q_up.shape[2] // count
    me = lax.axis_index("gz")
    for q, out, target in ((q_up, up, (me + 1) % count), (q_down, down, (me + count - 1) % count)):
        for block in range(count - 1):
            out[:, :, block * wide : (block + 1) * wide] = q[:, :, lanes_of((target + 1 + block) % count, wide)]


def split_kernel(count, m_up, m_down, q_up, q_down, up, down, own_up, own_down):
    outers = m_up.shape[1]
    wide = m_up.shape[2] // count
    rows = own_up.shape[1]
    me = lax.axis_index("gz")
    for m, q, out, own, target in (
        (m_up, q_up, up, own_up, (me + 1) % count),
        (m_down, q_down, down, own_down, (me + count - 1) % count),
    ):
        for block in range(count - 1):
            out[:, :, block * wide : (block + 1) * wide] = m[:, :, lanes_of((target + 1 + block) % count, wide)]
        mine = lanes_of(target, wide)
        own[:, :ROWS, :] = m[:, :ROWS, mine]
        own[:, pl.ds(ROWS, rows - outers), :] = q[:, :, mine]
        own[:, rows - ROWS :, :] = m[:, ROWS:, mine]


def finish_tile(scales, low, high, seen):
    one, two, clear = composite(low[0], low[1], *scales, 1.0)
    sub = one + clear * seen[0]
    cat = two + clear * seen[1]
    clear = clear * seen[2]
    one, two, clear = composite(high[0], high[1], *scales, clear)
    return sub + one, cat + two, clear


def others_kernel(values, known, q_low, q_high, r_low, r_high, seen, *pieces_and_outer):
    *pieces, outer = pieces_and_outer
    rows, columns = seen.shape[1:]
    count = len(pieces) + 1
    wide = columns // count
    tiles = rows // ROWS
    scales = across_columns(values[0], wide), across_columns(values[1], wide)
    me = lax.axis_index("gz")
    for shift, piece in enumerate(pieces, 1):
        owner = partner(me, shift, count)
        there = lanes_of(owner, wide)
        sent = lanes_of((owner + count - me - 1) % count, wide)
        for tile in range(tiles):
            at = span(tile)
            ends = []
            for side, (q, r) in enumerate(((q_low, r_low), (q_high, r_high))):
                got, place = tile_of(q, r, tile, tiles)
                ends.append([known[side, s, at, there] + RATES[s] * got[s, place, sent] for s in range(2)])
                for s in range(2):
                    outer[s, side, at, there] = ends[side][s]
            result = finish_tile(scales, ends[0], ends[1], [seen[part, at, there] for part in range(3)])
            for part in range(3):
                piece[part, at, :] = result[part]


def own_kernel(values, known, o_low, o_high, seen, piece, outer):
    rows, wide = piece.shape[1:]
    scales = across_columns(values[0], wide), across_columns(values[1], wide)
    here = lanes_of(lax.axis_index("gz"), wide)
    for tile in range(rows // ROWS):
        at = span(tile)
        ends = []
        for side, o in enumerate((o_low, o_high)):
            ends.append([known[side, s, at, here] + RATES[s] * o[s, at, :] for s in range(2)])
            for s in range(2):
                outer[s, side, at, :] = ends[side][s]
        result = finish_tile(scales, ends[0], ends[1], [seen[part, at, here] for part in range(3)])
        for part in range(3):
            piece[part, at, :] = result[part]


def put_kernel(count, new, ring, others, own, sub_in, cat_in, sub_out, cat_out, sems):
    del sub_in, cat_in
    depth, rows, columns = sub_out.shape
    wide = columns // count
    planes = pl.ds(2, depth - 4)
    me = lax.axis_index("gz")
    copies = []
    for s, out in enumerate((sub_out, cat_out)):
        targets = []
        for end in range(2):
            targets.append((new.at[s, end, planes], out.at[planes, pl.ds(end * (rows - ROWS), ROWS)]))
        for side in range(2):
            plane = side * (depth - 1)
            targets.append((ring.at[s, side], out.at[1 + side * (depth - 3)]))
            targets.append((own.at[s, side], out.at[plane, :, lanes_of(me, wide)]))
            for shift in range(1, count):
                there = lanes_of(partner(me, shift, count), wide)
                targets.append((others.at[s, side, :, there], out.at[plane, :, there]))
        for source, target in targets:
            copies.append(pltpu.make_async_copy(source, target, sems.at[len(copies)]))
    for copy in copies:
        copy.start()
    for copy in copies:
        copy.wait()


def paint_kernel(values, *pieces_and_rest):
    *pieces, out, slabs, image, sems = pieces_and_rest
    count = len(pieces)
    me = lax.axis_index("gz")
    for shift, piece in enumerate(pieces):
        slabs[origin(me, shift, count)] = piece[...]
    shade(values, slabs, out, image, sems, count)


def shade(values, slabs, out, image, sems, count):
    rows, wide = image.shape[1:]
    copies = []
    for tile in range(rows // ROWS):
        at = span(tile)
        sub, cat, clear = slabs[0, 0, at, :], slabs[0, 1, at, :], slabs[0, 2, at, :]
        for slab in range(1, count):
            sub = sub + clear * slabs[slab, 0, at, :]
            cat = cat + clear * slabs[slab, 1, at, :]
            clear = clear * slabs[slab, 2, at, :]
        for channel in range(3):
            of_sub = across_columns(values[2 + channel * 2], wide)
            of_cat = across_columns(values[3 + channel * 2], wide)
            image[channel, at, :] = of_sub * sub + of_cat * cat
        image[3, at, :] = 1.0 - clear
        copies.append(pltpu.make_async_copy(image.at[:, at], out.at[:, at], sems.at[tile]))
        copies[-1].start()
    for copy in copies:
        copy.wait()


def shade_kernel(values, half, *pieces_and_rest):
    *pieces, out, slabs, image, sems = pieces_and_rest
    count = len(pieces)
    rows, _ = image.shape[1:]
    me = lax.axis_index("gz")
    for shift, piece in enumerate(pieces):
        slab = origin(me, shift, count)
        if piece.shape[1] == rows:
            slabs[slab] = piece[...]
        else:
            slabs[slab, :, pl.ds(ROWS, rows - 2 * ROWS), :] = half[...]
            slabs[slab, :, span(0), :] = piece[:, :ROWS]
            slabs[slab, :, pl.ds(rows - ROWS, ROWS), :] = piece[:, ROWS:]
    shade(values, slabs, out, image, sems, count)


def place_kernel(new, ring, inner, outer, sub_in, cat_in, sub_out, cat_out, sems):
    del sub_in, cat_in
    depth, rows, _ = sub_out.shape
    planes = pl.ds(2, depth - 4)
    copies = []
    for s, out in enumerate((sub_out, cat_out)):
        for end in range(2):
            target = out.at[planes, pl.ds(end * (rows - ROWS), ROWS)]
            copies.append(pltpu.make_async_copy(new.at[s, end, planes], target, sems.at[len(copies)]))
        for side in range(2):
            plane = side * (depth - 1)
            for source, target in (
                (ring.at[s, side], out.at[1 + side * (depth - 3)]),
                (inner.at[s, side], out.at[plane, pl.ds(ROWS, rows - 2 * ROWS)]),
                (outer.at[s, side, span(0)], out.at[plane, span(0)]),
                (outer.at[s, side, span(1)], out.at[plane, pl.ds(rows - ROWS, ROWS)]),
            ):
                copies.append(pltpu.make_async_copy(source, target, sems.at[len(copies)]))
    for copy in copies:
        copy.start()
    for copy in copies:
        copy.wait()


def call(kernel, flops, room, **kwargs):
    return pl.pallas_call(
        kernel,
        cost_estimate=pl.CostEstimate(flops=flops, bytes_accessed=1 << 16, transcendentals=0),
        compiler_params=pltpu.CompilerParams(vmem_limit_bytes=room << 20),
        **kwargs,
    )


def body(substrate, catalyst, extinction, emission):
    depth, rows, columns = substrate.shape
    count = lax.axis_size("gz")
    wide = columns // count
    share = OPTICAL / (depth * count)
    middle = rows - 2 * ROWS

    def ring(size, shift):
        return [(i, (i + shift) % size) for i in range(size)]

    def shifted(x, axis, shift):
        return lax.ppermute(x, axis, ring(lax.axis_size(axis), shift))

    up, down = call(
        planes_kernel,
        1 << 20,
        2,
        name="planes",
        out_shape=(f32(2, rows, columns),) * 2,
        in_specs=[HBM, HBM],
        out_specs=(VMEM,) * 2,
        scratch_shapes=[pltpu.SemaphoreType.DMA((4,))],
    )(hbm(substrate), hbm(catalyst))
    p_low = shifted(up, "gz", 1)
    p_high = shifted(down, "gz", -1)

    own_low, own_high, q_up, q_down, r_up, r_down = call(
        prepare_kernel,
        1 << 22,
        2,
        name="prepare",
        out_shape=(f32(2, 2, depth, columns),) * 2 + (f32(2, middle, columns),) * 2 + (f32(2, 2 * ROWS, columns),) * 2,
        in_specs=[VMEM] * 2,
        out_specs=(VMEM,) * 6,
    )(substrate, catalyst)
    from_low = shifted(own_high, "gx", 1)
    from_high = shifted(own_low, "gx", -1)
    split = wide % LANES == 0
    foreign = columns - wide
    if split:
        q_sent = call(
            functools.partial(foreign_kernel, count),
            1 << 18,
            2,
            name="foreign",
            out_shape=(f32(2, middle, foreign),) * 2,
            in_specs=[VMEM] * 2,
            out_specs=(VMEM,) * 2,
        )(q_up, q_down)
    else:
        q_sent = (q_up, q_down)
    q_low = shifted(q_sent[0], "gz", 1)
    q_high = shifted(q_sent[1], "gz", -1)

    mid, values = call(
        functools.partial(first_kernel, share),
        1 << 24,
        2,
        name="first",
        out_shape=(f32(2, depth, rows, columns), f32(8, ROWS, LANES)),
        in_specs=[HBM, HBM, VMEM, VMEM],
        out_specs=(VMEM, VMEM),
        scratch_shapes=[
            pltpu.SMEM((2,), jnp.float32),
            pltpu.SMEM((2, 3), jnp.float32),
            pltpu.SemaphoreType.DMA((2,)),
        ],
    )(hbm(extinction), hbm(emission.T), substrate, catalyst)
    done, center = call(
        center_kernel,
        1 << 24,
        2,
        name="center",
        out_shape=(f32(2, depth, middle, columns), f32(3, rows, columns)),
        in_specs=[VMEM, VMEM],
        out_specs=(VMEM, VMEM),
    )(values, mid)

    m_up, m_down = call(
        rows_kernel,
        1 << 18,
        2,
        name="rows",
        out_shape=(f32(2, 2 * ROWS, columns),) * 2,
        in_specs=[VMEM] * 4,
        out_specs=(VMEM,) * 2,
    )(r_up, r_down, from_low, from_high)
    if split:
        m_up, m_down, o_up, o_down = call(
            functools.partial(split_kernel, count),
            1 << 18,
            2,
            name="split",
            out_shape=(f32(2, 2 * ROWS, foreign),) * 2 + (f32(2, rows, wide),) * 2,
            in_specs=[VMEM] * 4,
            out_specs=(VMEM,) * 4,
        )(m_up, m_down, q_up, q_down)
        o_low = shifted(o_up, "gz", 1)
        o_high = shifted(o_down, "gz", -1)
    r_low = shifted(m_up, "gz", 1)
    r_high = shifted(m_down, "gz", -1)

    sub_part, cat_part, new, inner, near, far, rows_low, rows_high = call(
        second_kernel,
        1 << 25,
        4,
        name="second",
        out_shape=(
            f32(depth, rows, columns),
            f32(depth, rows, columns),
            f32(2, 2, depth, ROWS, columns),
            f32(3, rows, columns),
            f32(2, 3, rows, columns),
            f32(2, 3, rows, columns),
            f32(2, depth, columns),
            f32(2, depth, columns),
        ),
        in_specs=[VMEM] * 12,
        out_specs=(HBM, HBM) + (VMEM,) * 6,
        scratch_shapes=[
            pltpu.VMEM((2, depth, ROWS, columns), jnp.float32),
            pltpu.VMEM((2, depth, ROWS, columns), jnp.float32),
            pltpu.SemaphoreType.DMA((2,)),
        ],
    )(values, mid, q_up, q_down, r_up, r_down, from_low, from_high, own_low, own_high, center, done)

    p_low, p_high, inner = lax.optimization_barrier((p_low, p_high, inner))
    ring_planes, known, seen = call(
        rim_kernel,
        1 << 23,
        4,
        name="rim",
        out_shape=(f32(2, 2, rows, columns), f32(2, 2, rows, columns), f32(3, rows, columns)),
        in_specs=[VMEM] * 10,
        out_specs=(VMEM,) * 3,
        scratch_shapes=[pltpu.VMEM((2, 2, rows, columns), jnp.float32)],
    )(values, p_low, p_high, down, up, near, far, rows_low, rows_high, inner)

    def paired(piece, shift):
        return lax.ppermute(piece, "gz", [(i, int(partner(i, shift, count))) for i in range(count)])

    if split:
        *pieces, others = call(
            others_kernel,
            1 << 22,
            2,
            name="others",
            out_shape=(f32(3, rows, wide),) * (count - 1) + (f32(2, 2, rows, columns),),
            in_specs=[VMEM] * 7,
            out_specs=(VMEM,) * count,
        )(values, known, q_low, q_high, r_low, r_high, seen)
        received = [None] * count
        half = count // 2
        for shift in [i for i in range(count - 1, 0, -1) if i != half] + [half]:
            received[shift] = paired(pieces[shift - 1], shift)
        received[0], own = call(
            own_kernel,
            1 << 20,
            2,
            name="own",
            out_shape=(f32(3, rows, wide), f32(2, 2, rows, wide)),
            in_specs=[VMEM] * 5,
            out_specs=(VMEM,) * 2,
        )(values, known, o_low, o_high, seen)
        sub_final, cat_final = call(
            functools.partial(put_kernel, count),
            1 << 22,
            2,
            name="put",
            out_shape=(f32(depth, rows, columns), f32(depth, rows, columns)),
            in_specs=[VMEM, VMEM, VMEM, VMEM, HBM, HBM],
            out_specs=(HBM, HBM),
            input_output_aliases={4: 0, 5: 1},
            scratch_shapes=[pltpu.SemaphoreType.DMA((4 * (count + 2),))],
        )(new, ring_planes, others, own, sub_part, cat_part)
        image = call(
            paint_kernel,
            1 << 20,
            4,
            name="paint",
            out_shape=f32(4, rows, wide),
            in_specs=[VMEM] * (1 + count),
            out_specs=HBM,
            scratch_shapes=[
                pltpu.VMEM((count, 3, rows, wide), jnp.float32),
                pltpu.VMEM((4, rows, wide), jnp.float32),
                pltpu.SemaphoreType.DMA((rows // ROWS,)),
            ],
        )(values, *received)
        return sub_final, cat_final, image

    half = count // 2
    half_piece, inner_rows, most = call(
        functools.partial(most_kernel, count),
        1 << 22,
        2,
        name="most",
        out_shape=(f32(3, middle, wide), f32(2, 2, middle, columns), f32(3, middle, columns)),
        in_specs=[VMEM] * 5,
        out_specs=(VMEM,) * 3,
    )(values, known, q_low, q_high, seen)

    half_piece = paired(half_piece, half)

    *pieces, outer_rows = call(
        last_kernel,
        1 << 22,
        4,
        name="last",
        out_shape=tuple(f32(3, 2 * ROWS if shift == half else rows, wide) for shift in range(count))
        + (f32(2, 2, 2 * ROWS, columns),),
        in_specs=[VMEM] * 6,
        out_specs=(VMEM,) * (count + 1),
        scratch_shapes=[pltpu.VMEM((3, rows, columns), jnp.float32)],
    )(values, known, r_low, r_high, seen, most)

    received = [pieces[0]] * count
    for shift in range(count - 1, 0, -1):
        received[shift] = paired(pieces[shift], shift)

    sub_final, cat_final = call(
        place_kernel,
        1 << 22,
        2,
        name="place",
        out_shape=(f32(depth, rows, columns), f32(depth, rows, columns)),
        in_specs=[VMEM, VMEM, VMEM, VMEM, HBM, HBM],
        out_specs=(HBM, HBM),
        input_output_aliases={4: 0, 5: 1},
        scratch_shapes=[pltpu.SemaphoreType.DMA((20,))],
    )(new, ring_planes, inner_rows, outer_rows, sub_part, cat_part)

    image = call(
        shade_kernel,
        1 << 20,
        4,
        name="shade",
        out_shape=f32(4, rows, wide),
        in_specs=[VMEM] * (2 + count),
        out_specs=HBM,
        scratch_shapes=[
            pltpu.VMEM((count, 3, rows, wide), jnp.float32),
            pltpu.VMEM((4, rows, wide), jnp.float32),
            pltpu.SemaphoreType.DMA((rows // ROWS,)),
        ],
    )(values, half_piece, *received)
    return sub_final, cat_final, image


def solution(mesh):
    placed = (P("gz", "gx", None), P("gz", "gx", None), P(), P())

    return jax.shard_map(
        body,
        mesh=mesh,
        in_specs=placed,
        out_specs=(P("gz", "gx", None), P("gz", "gx", None), P(None, "gx", "gz")),
        check_vma=False,
    )
```
